128 devices in a mesh: blk: 16 (over y, z), tm: 8 (over x, core).
Axes of the slice: x: 4, y: 4, z: 4, core: 2. Of those that a mesh axis runs over, the one named last changes fastest.
Arguments:
- solution: float32 [512, 128, 1024], P('blk', 'tm'), may hold values from -6 to 6
- residual: float32 [512, 128, 1024], P('blk', 'tm'), may hold values from -12 to 12
- direction: float32 [512, 128, 1024], P('blk', 'tm'), may hold values from -6 to 6
- noise_var: float32 [512, 128, 1024], P('blk', 'tm'), may hold values from 0.5 to 2
- legendre: bfloat16 [512, 512, 512], P('blk', 'tm'), may hold values from -0.25 to 0.25
- temporal: float32 [512, 128, 128], P('tm'), may hold values from -3 to 3.5, as said below
- order_table: int32 [512], replicated, may hold values from 0 to 511, as said below
Outputs:
- solution_new: float32 [512, 128, 1024], P('blk', 'tm')
- residual_new: float32 [512, 128, 1024], P('blk', 'tm')
- direction_new: float32 [512, 128, 1024], P('blk', 'tm')
The draws below stay inside these ranges and needn't reach their ends.
Inputs may be any that keep to these rules, and one draw needn't show every extreme that they name: `order_table`: each value 0 to 511 appears once. In each aligned block of 32 entries, entry 16 + k equals 511 minus entry k, so each block holds pairs of orders m and 511 - m. `temporal`: each matrix is symmetric and positive definite.
All inputs are finite; a program needn't handle non-finite values.
Results may differ from the reference program's by a relative error of at most 0.0048.
Values may be sent and summed in bfloat16 or wider, within the bound.
A program may use at most 192 MiB of HBM per device.

```python
import math
import jax
import jax.numpy as jnp
from jax import lax

LAT = 512
LON = 1024
DEGREES = 512
TIME = 128
ORD_DEV = 32


def draw_residual(key, part):
    cycles = jnp.arange(LAT, dtype=jnp.int32).astype(jnp.float32)
    scaling_factor = 1.0 + 2.0 * cycles / (LAT - 1)
    values = jnp.clip(jax.random.normal(key, (LAT, TIME, LON), jnp.float32), -4.0, 4.0)
    return values * scaling_factor[:, None, None]


def draw_temporal(key, part):
    limit = math.sqrt(3.0)
    factors = jax.random.uniform(jax.random.fold_in(key, 11), (DEGREES, TIME, TIME), jnp.float32, -limit, limit) / math.sqrt(TIME)
    gram = jnp.einsum('ltk,luk->ltu', factors, factors)
    return gram + 0.5 * jnp.eye(TIME, dtype=jnp.float32)[None, :, :]


def draw_order_table(key, part):
    pairs = jax.random.permutation(jax.random.fold_in(key, 7), DEGREES // 2).astype(jnp.int32)
    pairs = pairs.reshape(DEGREES // ORD_DEV, ORD_DEV // 2)
    return jnp.concatenate([pairs, DEGREES - 1 - pairs], axis=1).reshape(DEGREES).astype(jnp.int32)


def block_levels(own_key, extent, cuts, least, top_value):
    gain = 1.0
    for position, parts in cuts:
        steps = jax.random.uniform(jax.random.fold_in(jax.random.fold_in(own_key, 6), position), (parts,), jnp.float32, least / len(cuts), top_value / len(cuts))
        gain = gain * jnp.repeat(jnp.exp(steps), extent[position] // parts).reshape((-1,) + (1,) * (len(extent) - 1 - position))
    return gain


def bell_draw(stream_key, dims, deviation, most, shards=(), held_as=jnp.bfloat16):
    values = deviation * jax.random.normal(stream_key, dims, jnp.float32)
    if shards:
        values = values * block_levels(stream_key, dims, shards, -0.22, 0.18)
    return jnp.clip(values, -most, most).astype(held_as)


def setup_inputs(seed: int = 0) -> dict:
    arg_keys = jax.random.split(jax.random.key(seed), 8)
    return {
        "solution": bell_draw(arg_keys[0], (LAT, TIME, LON), 1.0, 6.0, ((0, 16), (1, 8)), jnp.float32),
        "residual": draw_residual(jax.random.fold_in(arg_keys[7], 71), 0),
        "direction": bell_draw(arg_keys[2], (LAT, TIME, LON), 1.0, 6.0, ((0, 16), (1, 8)), jnp.float32),
        "noise_var": jnp.clip(jnp.exp(math.log(2.0) - 1.3862944 * jax.random.uniform(arg_keys[3], (LAT, TIME, LON), jnp.float32) ** block_levels(arg_keys[3], (LAT, TIME, LON), ((0, 16), (1, 8)), -0.2, 0.2)), 0.5, 2.0),
        "legendre": bell_draw(arg_keys[4], (DEGREES, DEGREES, LAT), LAT ** -0.5, 0.25, ((0, 16), (1, 8))),
        "temporal": draw_temporal(jax.random.fold_in(arg_keys[7], 71), 0),
        "order_table": draw_order_table(jax.random.fold_in(arg_keys[7], 71), 0),
    }


def trig_table(orders, length):
    points = jnp.arange(length, dtype=jnp.int32)
    phases = points[:, None] * orders.astype(jnp.int32)[None, :] % length
    angles = phases.astype(jnp.float32) * (2.0 * math.pi / length)
    scaling_factor = 1.0 / math.sqrt(length / 2.0)
    stacked = jnp.stack([jnp.cos(angles), jnp.sin(angles)], axis=-1) * scaling_factor
    return stacked.reshape(length, 2 * orders.shape[0])

def reference(solution, residual, direction, noise_var, legendre, temporal, order_table):
    lookup_table = trig_table(order_table, LON)
    spectra = jnp.dot(direction.reshape(LAT * TIME, LON), lookup_table, precision=lax.Precision.HIGHEST).astype(jnp.bfloat16)
    spectra = spectra.reshape(LAT, TIME, DEGREES, 2).transpose(2, 0, 1, 3).reshape(DEGREES, LAT, TIME * 2)
    degrees = jnp.arange(DEGREES, dtype=jnp.int32)

    def per_order(items):
        rows, order, values = items
        mask_applied = jnp.where((degrees >= order)[:, None], rows, jnp.zeros_like(rows))
        coeffs = jnp.dot(mask_applied, values, preferred_element_type=jnp.float32).reshape(DEGREES, TIME, 2)
        mixed = jnp.einsum('ltu,luc->ltc', temporal, coeffs, precision=lax.Precision.HIGHEST).astype(jnp.bfloat16)
        return jnp.dot(mask_applied.T, mixed.reshape(DEGREES, TIME * 2), preferred_element_type=jnp.float32)
    grids = lax.map(per_order, (legendre, order_table, spectra))
    grids = grids.reshape(DEGREES, LAT, TIME, 2).transpose(1, 2, 0, 3).reshape(LAT * TIME, 2 * DEGREES)
    harmonic_synthesis = jnp.dot(grids, lookup_table.T, precision=lax.Precision.HIGHEST).reshape(LAT, TIME, LON)
    product = harmonic_synthesis + noise_var * direction
    norm_now = jnp.sum(residual * residual)
    curvature = jnp.sum(direction * product)
    step_size = norm_now / curvature
    solution_new = solution + step_size * direction
    residual_new = residual - step_size * product
    norm_next = jnp.sum(residual_new * residual_new)
    direction_new = residual_new + norm_next / norm_now * direction
    return (solution_new, residual_new, direction_new)
```

```python
import math

import jax
import jax.numpy as jnp
from jax import lax
from jax.sharding import Mesh
from jax.sharding import PartitionSpec as P

BLK = ("blk_0", "blk_1")
TM = ("tm_0", "tm_1")
BLK_TM = ("blk_0", "blk_1", "tm_0", "tm_1")


def trig_table(orders, length):
    points = jnp.arange(128, dtype=jnp.int32)
    step = 2.0 * math.pi / length
    scale = 1.0 / math.sqrt(length / 2.0)
    fine = ((orders[:, None] * points[None, :]) % length).astype(jnp.float32) * step
    cos_fine, sin_fine = jnp.cos(fine) * scale, jnp.sin(fine) * scale
    coarse = jnp.arange(length // 128, dtype=jnp.int32) * 128
    shift = ((orders[:, None] * coarse[None, :]) % length).astype(jnp.float32) * step
    cos_shift, sin_shift = jnp.cos(shift), jnp.sin(shift)
    cos_parts, sin_parts = [], []
    for q in range(length // 128):
        a, b = cos_shift[:, q : q + 1], sin_shift[:, q : q + 1]
        cos_parts.append((cos_fine * a - sin_fine * b).astype(jnp.bfloat16))
        sin_parts.append((sin_fine * a + cos_fine * b).astype(jnp.bfloat16))
    return jnp.concatenate(cos_parts, axis=1), jnp.concatenate(sin_parts, axis=1)


def body(solution, residual, direction, noise_var, legendre, temporal, order_table):
    per_device, deg_dev, lat_all = legendre.shape
    lat_dev, time_dev, longitude = direction.shape
    blocks = lat_all // lat_dev
    cos_table, sin_table = trig_table(order_table, longitude)
    table = jnp.stack(
        [
            cos_table.reshape(blocks, per_device, longitude),
            sin_table.reshape(blocks, per_device, longitude),
        ],
        axis=1,
    )
    own_orders = lax.dynamic_slice_in_dim(order_table, lax.axis_index(BLK) * per_device, per_device)
    own_degrees = lax.axis_index(TM) * deg_dev + jnp.arange(deg_dev, dtype=jnp.int32)
    keep_mask = own_degrees[None, :, None] >= own_orders[:, None, None]
    masked = jnp.where(keep_mask, legendre, jnp.zeros_like(legendre))
    flat = table.reshape(-1, longitude)
    spectra = jnp.einsum(
        "kj,atj->kta",
        flat,
        direction.astype(jnp.bfloat16),
        preferred_element_type=jnp.float32,
    ).astype(jnp.bfloat16)
    cycles = lax.all_to_all(
        spectra.reshape(blocks, 2 * per_device * time_dev * lat_dev),
        BLK,
        split_axis=0,
        concat_axis=0,
        tiled=True,
    )
    cycles = cycles.reshape(blocks, 2, per_device, time_dev, lat_dev)
    cycles = cycles.transpose(2, 1, 3, 0, 4).reshape(per_device, 2, time_dev, lat_all)
    cycles = lax.all_gather(cycles, TM, axis=2, tiled=True)
    coeffs = jnp.einsum(
        "icta,ila->lict", cycles, masked, preferred_element_type=jnp.float32
    ).astype(jnp.bfloat16)
    mixed = jnp.einsum(
        "lict,ltu->licu",
        coeffs,
        temporal.astype(jnp.bfloat16),
        preferred_element_type=jnp.float32,
    ).astype(jnp.bfloat16)
    terms = jnp.einsum(
        "ila,licu->icua", masked, mixed, preferred_element_type=jnp.float32
    ).astype(jnp.bfloat16)
    terms = lax.psum_scatter(terms, TM, scatter_dimension=2, tiled=True)
    terms = terms.reshape(per_device, 2, time_dev, blocks, lat_dev).transpose(3, 1, 0, 2, 4)
    entries = lax.all_to_all(
        terms.reshape(blocks, -1), BLK, split_axis=0, concat_axis=0, tiled=True
    )
    entries = entries.reshape(blocks * 2 * per_device, time_dev, lat_dev)
    synthesis = jnp.einsum("kta,kj->atj", entries, flat, preferred_element_type=jnp.float32)
    product = synthesis + noise_var * direction
    sums = jnp.stack(
        [
            jnp.sum(residual * residual),
            jnp.sum(direction * product),
            jnp.sum(residual * product),
            jnp.sum(product * product),
        ]
    )
    norm_now, curvature, cross, square = lax.psum(sums, BLK_TM)
    step_size = norm_now / curvature
    norm_next = norm_now - 2.0 * step_size * cross + step_size * step_size * square
    residual_new = residual - step_size * product
    return (
        solution + step_size * direction,
        residual_new,
        residual_new + norm_next / norm_now * direction,
    )


def solution(mesh):
    torus = Mesh(mesh.devices.reshape(4, 4, 4, 2), ("blk_0", "blk_1", "tm_0", "tm_1"))
    return jax.shard_map(
        body,
        mesh=torus,
        in_specs=(
            P(BLK, TM, None),
            P(BLK, TM, None),
            P(BLK, TM, None),
            P(BLK, TM, None),
            P(BLK, TM, None),
            P(TM, None, None),
            P(),
        ),
        out_specs=(P(BLK, TM, None), P(BLK, TM, None), P(BLK, TM, None)),
        check_vma=False,
    )
```

```python
import math

import jax
import jax.numpy as jnp
from jax import lax
from jax.experimental import pallas as pl
from jax.experimental.pallas import tpu as pltpu
from jax.sharding import Mesh
from jax.sharding import PartitionSpec as P

BLK = ("blk_0", "blk_1")
TM = ("tm_0", "tm_1")
BLK_TM = ("blk_0", "blk_1", "tm_0", "tm_1")
BF = jnp.bfloat16
F32 = jnp.float32
MESH = pl.DeviceIdType.MESH
GROUPS = 4
ORD = 8
VM = pl.BlockSpec(memory_space=pltpu.VMEM)


def unit_circle(phase):
    quadrant = (phase + 128) // 256
    x = (phase - quadrant * 256).astype(F32) * (2.0 * math.pi / 1024)
    x2 = x * x
    s = x * (1.0 + x2 * (-1.0 / 6 + x2 * (1.0 / 120 + x2 * (-1.0 / 5040 + x2 / 362880))))
    c = 1.0 + x2 * (-0.5 + x2 * (1.0 / 24 + x2 * (-1.0 / 720 + x2 / 40320)))
    odd = quadrant % 2 == 1
    cos = jnp.where(odd, s, c)
    sin = jnp.where(odd, c, s)
    cos = jnp.where((quadrant == 1) | (quadrant == 2), -cos, cos)
    sin = jnp.where((quadrant == 2) | (quadrant == 3), -sin, sin)
    return cos, sin


def table_dft_kernel(orders, direction, table, spectra, rows, split):
    lat, time = 32, 16
    lane = lax.broadcasted_iota(jnp.int32, (ORD, 128), 1)
    scale = 1.0 / math.sqrt(512.0)

    for q in range(8):
        split[q * 512 : (q + 1) * 512, :] = direction[:, q * 128 : (q + 1) * 128]

    def gather(t, _):
        for q in range(8):
            rows[pl.ds(pl.multiple_of(t * lat, lat), lat), q * 128 : (q + 1) * 128] = split[
                pl.ds(q * 512 + t, lat, stride=time), :
            ].astype(BF)
        return 0

    lax.fori_loop(0, time, gather, 0)

    def fill(n, _):
        m = orders[pl.ds(pl.multiple_of(n * ORD, ORD), ORD), :]
        cos, sin = unit_circle((m * lane) % 1024)
        turn_c, turn_s = unit_circle((m * 128) % 1024)
        cos, sin = cos * scale, sin * scale
        for q in range(8):
            table[pl.ds(pl.multiple_of(n * 16, 16), 16), q * 128 : (q + 1) * 128] = (
                jnp.concatenate([cos, sin], axis=0).astype(BF)
            )
            cos, sin = cos * turn_c - sin * turn_s, sin * turn_c + cos * turn_s
        return 0

    lax.fori_loop(0, 64, fill, 0)

    def transform(n, _):
        part = lax.dot_general(
            table[pl.ds(pl.multiple_of(n * 256, 256), 256), :],
            rows[...],
            (((1,), (1,)), ((), ())),
            preferred_element_type=F32,
        )
        spectra[pl.ds(n * 4, 4)] = part.astype(BF).reshape(4, GROUPS, 2 * ORD, 512)
        return 0

    lax.fori_loop(0, 4, transform, 0)


def table_dft(orders, direction):
    return pl.pallas_call(
        table_dft_kernel,
        out_shape=(
            jax.ShapeDtypeStruct((1024, 1024), BF),
            jax.ShapeDtypeStruct((16, GROUPS, 2 * ORD, 512), BF),
        ),
        in_specs=[VM, VM],
        out_specs=(VM, VM),
        scratch_shapes=[pltpu.VMEM((512, 1024), BF), pltpu.VMEM((4096, 128), F32)],
        compiler_params=pltpu.CompilerParams(vmem_limit_bytes=40 * 1024 * 1024),
        name="table_dft",
    )(orders, direction)


def lane_swap():
    row = lax.broadcasted_iota(jnp.int32, (512, 512), 0)
    col = lax.broadcasted_iota(jnp.int32, (512, 512), 1)
    moved = (row // 32 % 4) * 128 + (row // 128) * 32 + row % 32
    return (col == moved).astype(F32).astype(BF)


def front_kernel(spectra, full, recv, mid, perm, a2a_send, a2a_recv, own_send, fwd_send, peer_send,
                 line_recv, far_recv, peer_recv):
    y, z = lax.axis_index("blk_0"), lax.axis_index("blk_1")
    x, core = lax.axis_index("tm_0"), lax.axis_index("tm_1")
    me = y * 4 + z
    right, left, far = (x + 1) % 4, (x + 3) % 4, (x + 2) % 4
    barrier = pltpu.get_barrier_semaphore()

    def greet(k, _):
        pl.semaphore_signal(
            barrier, inc=1, device_id={"blk_0": (y + k // 4) % 4, "blk_1": (z + k % 4) % 4},
            device_id_type=MESH,
        )
        return 0

    lax.fori_loop(1, 16, greet, 0)
    pl.semaphore_signal(barrier, inc=1, device_id={"tm_0": right}, device_id_type=MESH)
    pl.semaphore_signal(barrier, inc=1, device_id={"tm_0": left}, device_id_type=MESH)
    pl.semaphore_signal(barrier, inc=1, device_id={"tm_1": 1 - core}, device_id_type=MESH)
    perm[...] = lane_swap()
    pl.semaphore_wait(barrier, 18)

    def block_copy(g, k):
        ty, tz = (y + k // 4) % 4, (z + k % 4) % 4
        return pltpu.make_async_remote_copy(
            src_ref=spectra.at[ty * 4 + tz, g], dst_ref=recv.at[g, me],
            send_sem=a2a_send.at[g, k], recv_sem=a2a_recv.at[g, k],
            device_id={"blk_0": ty, "blk_1": tz}, device_id_type=MESH,
        )

    def send_block(n, _):
        block_copy(n // 15, n % 15 + 1).start()
        return 0

    lax.fori_loop(0, GROUPS * 15, send_block, 0)
    for g in range(GROUPS):
        recv[g, pl.ds(me, 1)] = spectra[pl.ds(me, 1), g]

    def part(g, plane, who, first, count):
        return full.at[pl.ds(g * ORD + first, count), :, pl.ds(pl.multiple_of((plane * 2 + who) * 16, 16), 16), :]

    def line_copy(g, way):
        ref = part(g, x, core, 0, ORD)
        return pltpu.make_async_remote_copy(
            src_ref=ref, dst_ref=ref, send_sem=own_send.at[g, way], recv_sem=line_recv.at[g, way],
            device_id={"tm_0": right if way == 0 else left}, device_id_type=MESH,
        )

    def far_copy(g, way):
        ref = part(g, left if way == 0 else right, core, way * (ORD // 2), ORD // 2)
        return pltpu.make_async_remote_copy(
            src_ref=ref, dst_ref=ref, send_sem=fwd_send.at[g, way], recv_sem=far_recv.at[g, way],
            device_id={"tm_0": right if way == 0 else left}, device_id_type=MESH,
        )

    def peer_copy(g, slot):
        plane, first, count = (
            (x, 0, ORD), (left, 0, ORD), (right, 0, ORD), (far, 0, ORD // 2), (far, ORD // 2, ORD // 2)
        )[slot]
        ref = part(g, plane, core, first, count)
        return pltpu.make_async_remote_copy(
            src_ref=ref, dst_ref=ref, send_sem=peer_send.at[g, slot], recv_sem=peer_recv.at[g, slot],
            device_id={"tm_1": 1 - core}, device_id_type=MESH,
        )

    def regroup(g):
        rows = []
        for sq in range(4):
            for tq in range(4):
                rows.append(jnp.concatenate(
                    [recv[g, sq * 4 + s, :, tq * 128 : (tq + 1) * 128] for s in range(4)], axis=1))
        moved = jnp.dot(jnp.concatenate(rows, axis=0), perm[...], preferred_element_type=F32)
        for sq in range(4):
            for tq in range(4):
                n = (sq * 4 + tq) * 16
                for t in range(4):
                    m = sq * 256 + (tq * 4 + t) * 16
                    mid[m : m + 16, :] = moved[n : n + 16, t * 128 : (t + 1) * 128]
        for c in range(2):
            for i in range(ORD):
                for sq in range(4):
                    full[g * ORD + i, c, pl.ds(pl.multiple_of((x * 2 + core) * 16, 16), 16),
                         sq * 128 : (sq + 1) * 128] = (
                        mid[pl.ds(sq * 256 + c * ORD + i, 16, stride=16), :].astype(BF))

    for g in range(GROUPS + 2):
        if g < GROUPS:
            def arrive(k, _):
                block_copy(g, k).wait_recv()
                return 0

            lax.fori_loop(1, 16, arrive, 0)
            regroup(g)
            line_copy(g, 0).start()
            line_copy(g, 1).start()
            peer_copy(g, 0).start()
        if 1 <= g <= GROUPS:
            line_copy(g - 1, 0).wait_recv()
            far_copy(g - 1, 0).start()
            peer_copy(g - 1, 1).start()
            line_copy(g - 1, 1).wait_recv()
            far_copy(g - 1, 1).start()
            peer_copy(g - 1, 2).start()
        if g >= 2:
            far_copy(g - 2, 0).wait_recv()
            peer_copy(g - 2, 3).start()
            far_copy(g - 2, 1).wait_recv()
            peer_copy(g - 2, 4).start()
    for g in range(GROUPS):
        for slot in range(5):
            peer_copy(g, slot).wait_recv()
    for g in range(GROUPS):
        for slot in range(5):
            peer_copy(g, slot).wait_send()
        for way in range(2):
            line_copy(g, way).wait_send()
            far_copy(g, way).wait_send()

    def sent(n, _):
        block_copy(n // 15, n % 15 + 1).wait_send()
        return 0

    lax.fori_loop(0, GROUPS * 15, sent, 0)


def front(spectra):
    dma = pltpu.SemaphoreType.DMA
    return pl.pallas_call(
        front_kernel,
        out_shape=jax.ShapeDtypeStruct((32, 2, 128, 512), BF),
        in_specs=[VM],
        out_specs=VM,
        scratch_shapes=[
            pltpu.VMEM((GROUPS, 16, 2 * ORD, 512), BF),
            pltpu.VMEM((1024, 128), F32),
            pltpu.VMEM((512, 512), BF),
            dma((GROUPS, 16)), dma((GROUPS, 16)),
            dma((GROUPS, 2)), dma((GROUPS, 2)), dma((GROUPS, 5)),
            dma((GROUPS, 2)), dma((GROUPS, 2)), dma((GROUPS, 5)),
        ],
        compiler_params=pltpu.CompilerParams(
            collective_id=0, has_side_effects=True, vmem_limit_bytes=40 * 1024 * 1024),
        name="front",
    )(spectra)


def order_groups(order_table):
    pairs = order_table.reshape(16, 2, 16)[:, 0]
    low = jnp.minimum(pairs, 511 - pairs)
    both = jnp.stack([low, 511 - low], axis=1).reshape(16, 2, 2, ORD)
    return jnp.broadcast_to(both.reshape(512, 1), (512, 128))


def back_kernel(part, out, acc, far_in, fin_in, blocks, mid, perm, peer_send, peer_recv, far_send,
                far_recv, line_send, line_recv, a2a_send, a2a_recv):
    y, z = lax.axis_index("blk_0"), lax.axis_index("blk_1")
    x, core = lax.axis_index("tm_0"), lax.axis_index("tm_1")
    me = y * 4 + z
    right, left, far = (x + 1) % 4, (x + 3) % 4, (x + 2) % 4
    half = ORD // 2
    barrier = pltpu.get_barrier_semaphore()

    def greet(k, _):
        pl.semaphore_signal(
            barrier, inc=1, device_id={"blk_0": (y + k // 4) % 4, "blk_1": (z + k % 4) % 4},
            device_id_type=MESH,
        )
        return 0

    lax.fori_loop(1, 16, greet, 0)
    pl.semaphore_signal(barrier, inc=1, device_id={"tm_0": right}, device_id_type=MESH)
    pl.semaphore_signal(barrier, inc=1, device_id={"tm_0": left}, device_id_type=MESH)
    pl.semaphore_signal(barrier, inc=1, device_id={"tm_1": 1 - core}, device_id_type=MESH)
    perm[...] = lane_swap()
    pl.semaphore_wait(barrier, 18)
    planes = (far, right, left, x)

    def hours(plane, who):
        return pl.ds(pl.multiple_of((plane * 2 + who) * 16, 16), 16)

    def peer_copy(g, n):
        return pltpu.make_async_remote_copy(
            src_ref=part.at[pl.ds(g * ORD, ORD), :, hours(planes[n], 1 - core), :],
            dst_ref=acc.at[g, n],
            send_sem=peer_send.at[g, n], recv_sem=peer_recv.at[g, n],
            device_id={"tm_1": 1 - core}, device_id_type=MESH,
        )

    def far_copy(g, way):
        return pltpu.make_async_remote_copy(
            src_ref=acc.at[g, 0, pl.ds(way * half, half)], dst_ref=far_in.at[g, way],
            send_sem=far_send.at[g, way], recv_sem=far_recv.at[g, way],
            device_id={"tm_0": right if way == 0 else left}, device_id_type=MESH,
        )

    def line_copy(g, way):
        return pltpu.make_async_remote_copy(
            src_ref=acc.at[g, 1 + way], dst_ref=fin_in.at[g, way],
            send_sem=line_send.at[g, way], recv_sem=line_recv.at[g, way],
            device_id={"tm_0": right if way == 0 else left}, device_id_type=MESH,
        )

    def block_copy(g, k):
        ty, tz = (y + k // 4) % 4, (z + k % 4) % 4
        return pltpu.make_async_remote_copy(
            src_ref=blocks.at[g, ty * 4 + tz], dst_ref=out.at[me, g],
            send_sem=a2a_send.at[g, k], recv_sem=a2a_recv.at[g, k],
            device_id={"blk_0": ty, "blk_1": tz}, device_id_type=MESH,
        )

    def add_own(g, n):
        def step(i, _):
            own = part[g * ORD + i, :, hours(planes[n], core), :]
            acc[g, n, i] = (acc[g, n, i].astype(F32) + own.astype(F32)).astype(BF)
            return 0

        lax.fori_loop(0, ORD, step, 0)

    def add_far(g, way):
        def step(i, _):
            acc[g, 1 + way, way * half + i] = (
                acc[g, 1 + way, way * half + i].astype(F32) + far_in[g, way, i].astype(F32)
            ).astype(BF)
            return 0

        lax.fori_loop(0, half, step, 0)

    def regroup(g):
        for i in range(ORD):
            for c in range(2):
                total = (acc[g, 3, i, c].astype(F32) + fin_in[g, 0, i, c].astype(F32)
                         + fin_in[g, 1, i, c].astype(F32))
                for sq in range(4):
                    mid[pl.ds(sq * 256 + c * ORD + i, 16, stride=16), :] = (
                        total[:, sq * 128 : (sq + 1) * 128])
        rows = []
        for sq in range(4):
            for tq in range(4):
                m = sq * 256 + tq * 64
                rows.append(jnp.concatenate(
                    [mid[m + t * 16 : m + (t + 1) * 16, :].astype(BF) for t in range(4)], axis=1))
        moved = jnp.dot(
            jnp.concatenate(rows, axis=0), perm[...], preferred_element_type=F32).astype(BF)
        for sq in range(4):
            for tq in range(4):
                n = (sq * 4 + tq) * 16
                for s in range(4):
                    blocks[g, sq * 4 + s, :, tq * 128 : (tq + 1) * 128] = (
                        moved[n : n + 16, s * 128 : (s + 1) * 128])

    for g in range(GROUPS):
        for n in range(4):
            peer_copy(g, n).start()
    for g in range(GROUPS + 2):
        if g < GROUPS:
            for n in range(4):
                peer_copy(g, n).wait_recv()
                add_own(g, n)
                if n == 0:
                    far_copy(g, 0).start()
                    far_copy(g, 1).start()
        if 1 <= g <= GROUPS:
            for way in range(2):
                far_copy(g - 1, way).wait_recv()
                add_far(g - 1, way)
                line_copy(g - 1, way).start()
        if g >= 2:
            line_copy(g - 2, 0).wait_recv()
            line_copy(g - 2, 1).wait_recv()
            regroup(g - 2)

            def send_block(k, _):
                block_copy(g - 2, k).start()
                return 0

            lax.fori_loop(1, 16, send_block, 0)
            out[pl.ds(me, 1), g - 2] = blocks[g - 2, pl.ds(me, 1)]
    for g in range(GROUPS):
        for n in range(4):
            peer_copy(g, n).wait_send()
        for way in range(2):
            far_copy(g, way).wait_send()
            line_copy(g, way).wait_send()

    def finish(n, _):
        block_copy(n // 15, n % 15 + 1).wait_recv()
        block_copy(n // 15, n % 15 + 1).wait_send()
        return 0

    lax.fori_loop(0, GROUPS * 15, finish, 0)


def back(part):
    dma = pltpu.SemaphoreType.DMA
    return pl.pallas_call(
        back_kernel,
        out_shape=jax.ShapeDtypeStruct((16, GROUPS, 2 * ORD, 512), BF),
        in_specs=[VM],
        out_specs=VM,
        scratch_shapes=[
            pltpu.VMEM((GROUPS, 4, ORD, 2, 16, 512), BF),
            pltpu.VMEM((GROUPS, 2, ORD // 2, 2, 16, 512), BF),
            pltpu.VMEM((GROUPS, 2, ORD, 2, 16, 512), BF),
            pltpu.VMEM((GROUPS, 16, 2 * ORD, 512), BF),
            pltpu.VMEM((1024, 128), F32),
            pltpu.VMEM((512, 512), BF),
            dma((GROUPS, 4)), dma((GROUPS, 4)), dma((GROUPS, 2)), dma((GROUPS, 2)),
            dma((GROUPS, 2)), dma((GROUPS, 2)), dma((GROUPS, 16)), dma((GROUPS, 16)),
        ],
        compiler_params=pltpu.CompilerParams(
            collective_id=1, has_side_effects=True, vmem_limit_bytes=48 * 1024 * 1024),
        name="back",
    )(part)


def product_kernel(entries, table, residual, direction, noise, product, sums, split, stage, line,
                   plane, line_send, line_recv, plane_send, plane_recv):
    y, z = lax.axis_index("blk_0"), lax.axis_index("blk_1")
    x, core = lax.axis_index("tm_0"), lax.axis_index("tm_1")
    row, col = y * 4 + z, x * 2 + core

    def in_line(k):
        return {"tm_0": (x + k // 2) % 4, "tm_1": (core + k) % 2}

    def in_plane(k):
        return {"blk_0": (y + k // 4) % 4, "blk_1": (z + k % 4) % 4}

    barrier = pltpu.get_barrier_semaphore()

    def greet_line(k, _):
        pl.semaphore_signal(barrier, inc=1, device_id=in_line(k), device_id_type=MESH)
        return 0

    def greet_plane(k, _):
        pl.semaphore_signal(barrier, inc=1, device_id=in_plane(k), device_id_type=MESH)
        return 0

    lax.fori_loop(1, 8, greet_line, 0)
    lax.fori_loop(1, 16, greet_plane, 0)

    def synthesis(n, _):
        cols = entries[:, pl.ds(pl.multiple_of(n * 128, 128), 128)]
        block = lax.dot_general(cols, table[...], (((0,), (0,)), ((), ())), preferred_element_type=F32)
        for t in range(4):
            for q in range(8):
                split[pl.ds(q * 512 + n * 4 + t, 32, stride=16), :] = (
                    block[t * 32 : (t + 1) * 32, q * 128 : (q + 1) * 128])
        return 0

    lax.fori_loop(0, 4, synthesis, 0)

    def combine(n, totals):
        rows = pl.ds(pl.multiple_of(n * 8, 8), 8)
        nn, dp, rp, pp = totals
        for q in range(8):
            cols = slice(q * 128, (q + 1) * 128)
            d, r = direction[rows, cols], residual[rows, cols]
            p = split[pl.ds(pl.multiple_of(q * 512 + n * 8, 8), 8), :] + noise[rows, cols] * d
            product[rows, cols] = p
            nn, dp, rp, pp = nn + r * r, dp + d * p, rp + r * p, pp + p * p
        return nn, dp, rp, pp

    zero = jnp.zeros((8, 128), F32)
    totals = lax.fori_loop(0, 64, combine, (zero, zero, zero, zero))
    for k in range(4):
        stage[0, 2 * k : 2 * k + 2, :] = jnp.broadcast_to(
            jnp.sum(totals[k], axis=0, keepdims=True), (2, 128))
    pl.semaphore_wait(barrier, 22)

    def line_copy(k):
        return pltpu.make_async_remote_copy(
            src_ref=stage.at[0], dst_ref=line.at[col], send_sem=line_send.at[k],
            recv_sem=line_recv.at[k], device_id=in_line(k), device_id_type=MESH)

    def plane_copy(k):
        return pltpu.make_async_remote_copy(
            src_ref=stage.at[1], dst_ref=plane.at[row], send_sem=plane_send.at[k],
            recv_sem=plane_recv.at[k], device_id=in_plane(k), device_id_type=MESH)

    for k in range(1, 8):
        line_copy(k).start()
    line[pl.ds(col, 1)] = stage[0:1]
    for k in range(1, 8):
        line_copy(k).wait_recv()
    stage[1] = jnp.sum(line[...], axis=0)
    for k in range(1, 16):
        plane_copy(k).start()
    plane[pl.ds(row, 1)] = stage[1:2]
    for k in range(1, 16):
        plane_copy(k).wait_recv()
    sums[...] = jnp.sum(plane[...], axis=0)
    for k in range(1, 8):
        line_copy(k).wait_send()
    for k in range(1, 16):
        plane_copy(k).wait_send()


def product_sums(entries, table, residual, direction, noise):
    dma = pltpu.SemaphoreType.DMA
    return pl.pallas_call(
        product_kernel,
        out_shape=(jax.ShapeDtypeStruct((512, 1024), F32), jax.ShapeDtypeStruct((8, 128), F32)),
        in_specs=[VM] * 5,
        out_specs=(VM, VM),
        scratch_shapes=[
            pltpu.VMEM((4096, 128), F32),
            pltpu.VMEM((2, 8, 128), F32),
            pltpu.VMEM((8, 8, 128), F32),
            pltpu.VMEM((16, 8, 128), F32),
            dma((8,)), dma((8,)), dma((16,)), dma((16,)),
        ],
        compiler_params=pltpu.CompilerParams(
            collective_id=2, has_side_effects=True, vmem_limit_bytes=48 * 1024 * 1024),
        name="product_sums",
    )(entries, table, residual, direction, noise)


def update_kernel(sums, solution, residual, direction, product, solution_new, residual_new,
                  direction_new):
    def total(k):
        return jnp.sum(sums[2 * k : 2 * k + 1, :], axis=1, keepdims=True)

    norm_now, curvature, cross, square = total(0), total(1), total(2), total(3)
    step = norm_now / curvature
    norm_next = norm_now - 2.0 * step * cross + step * step * square
    ratio = norm_next / norm_now
    d = direction[...]
    r = residual[...] - step * product[...]
    solution_new[...] = solution[...] + step * d
    residual_new[...] = r
    direction_new[...] = r + ratio * d


def update(sums, solution, residual, direction, product):
    block = pl.BlockSpec((64, 1024), lambda n: (n, 0))
    shape = jax.ShapeDtypeStruct((512, 1024), F32)
    return pl.pallas_call(
        update_kernel,
        grid=(8,),
        out_shape=(shape, shape, shape),
        in_specs=[pl.BlockSpec((8, 128), lambda n: (0, 0))] + [block] * 4,
        out_specs=(block, block, block),
        name="update",
    )(sums, solution, residual, direction, product)


def body(solution, residual, direction, noise_var, legendre, temporal, order_table):
    per_device, deg_dev, lat_all = legendre.shape
    shape = direction.shape
    flat = lambda v: v.reshape(512, 1024)
    groups = order_groups(order_table)
    table, spectra = table_dft(groups, flat(direction))
    cycles = front(spectra)
    own = lax.dynamic_slice_in_dim(order_table, lax.axis_index(BLK) * per_device, per_device)
    degrees = lax.axis_index(TM) * deg_dev + jnp.arange(deg_dev, dtype=jnp.int32)
    low_first = (own[:16] < 256)[:, None, None]
    first, second = legendre[:16], legendre[16:]
    low = jnp.minimum(own[:16], 511 - own[:16])
    orders = jnp.concatenate([low, 511 - low])
    swapped = jnp.concatenate(
        [jnp.where(low_first, first, second), jnp.where(low_first, second, first)], axis=0)
    masked = jnp.where(degrees[None, :, None] >= orders[:, None, None], swapped, jnp.zeros_like(swapped))
    coeffs = jnp.einsum(
        "icta,ila->lict", cycles, masked, preferred_element_type=F32).astype(BF)
    mixed = jnp.einsum(
        "lict,ltu->licu", coeffs, temporal.astype(BF), preferred_element_type=F32).astype(BF)
    terms = jnp.einsum("ila,licu->icua", masked, mixed, preferred_element_type=F32).astype(BF)
    entries = back(terms).reshape(1024, 512)
    product, sums = product_sums(entries, table, flat(residual), flat(direction), flat(noise_var))
    outs = update(sums, flat(solution), flat(residual), flat(direction), product)
    return tuple(o.reshape(shape) for o in outs)


def solution(mesh):
    torus = Mesh(mesh.devices.reshape(4, 4, 4, 2), ("blk_0", "blk_1", "tm_0", "tm_1"))
    return jax.shard_map(
        body,
        mesh=torus,
        in_specs=(
            P(BLK, TM, None),
            P(BLK, TM, None),
            P(BLK, TM, None),
            P(BLK, TM, None),
            P(BLK, TM, None),
            P(TM, None, None),
            P(),
        ),
        out_specs=(P(BLK, TM, None), P(BLK, TM, None), P(BLK, TM, None)),
        check_vma=False,
    )
```

```python
import math

import jax
import jax.numpy as jnp
from jax import lax
from jax.experimental import pallas as pl
from jax.experimental.pallas import tpu as pltpu
from jax.sharding import Mesh
from jax.sharding import PartitionSpec as P

BLK = ("blk_0", "blk_1")
TM = ("tm_0", "tm_1")
BLK_TM = ("blk_0", "blk_1", "tm_0", "tm_1")
BF = jnp.bfloat16
F32 = jnp.float32
MESH = pl.DeviceIdType.MESH
GROUPS = 4
ORD = 8
VM = pl.BlockSpec(memory_space=pltpu.VMEM)


def unit_circle(phase):
    quadrant = (phase + 128) // 256
    x = (phase - quadrant * 256).astype(F32) * (2.0 * math.pi / 1024)
    x2 = x * x
    s = x * (1.0 + x2 * (-1.0 / 6 + x2 * (1.0 / 120 + x2 * (-1.0 / 5040 + x2 / 362880))))
    c = 1.0 + x2 * (-0.5 + x2 * (1.0 / 24 + x2 * (-1.0 / 720 + x2 / 40320)))
    odd = quadrant % 2 == 1
    cos = jnp.where(odd, s, c)
    sin = jnp.where(odd, c, s)
    cos = jnp.where((quadrant == 1) | (quadrant == 2), -cos, cos)
    sin = jnp.where((quadrant == 2) | (quadrant == 3), -sin, sin)
    return cos, sin


def table_dft_kernel(orders, direction, table, spectra, rows, split):
    lat, time = 32, 16
    lane = lax.broadcasted_iota(jnp.int32, (ORD, 128), 1)
    scale = 1.0 / math.sqrt(512.0)

    for q in range(8):
        split[q * 512 : (q + 1) * 512, :] = direction[:, q * 128 : (q + 1) * 128]

    def gather(t, _):
        for q in range(8):
            rows[pl.ds(pl.multiple_of(t * lat, lat), lat), q * 128 : (q + 1) * 128] = split[
                pl.ds(q * 512 + t, lat, stride=time), :
            ].astype(BF)
        return 0

    lax.fori_loop(0, time, gather, 0)

    def fill(n, _):
        m = orders[pl.ds(pl.multiple_of(n * ORD, ORD), ORD), :]
        cos, sin = unit_circle((m * lane) % 1024)
        turn_c, turn_s = unit_circle((m * 128) % 1024)
        cos, sin = cos * scale, sin * scale
        for q in range(8):
            table[pl.ds(pl.multiple_of(n * 16, 16), 16), q * 128 : (q + 1) * 128] = (
                jnp.concatenate([cos, sin], axis=0).astype(BF)
            )
            cos, sin = cos * turn_c - sin * turn_s, sin * turn_c + cos * turn_s
        return 0

    lax.fori_loop(0, 64, fill, 0)

    def transform(n, _):
        part = lax.dot_general(
            table[pl.ds(pl.multiple_of(n * 256, 256), 256), :],
            rows[...],
            (((1,), (1,)), ((), ())),
            preferred_element_type=F32,
        )
        spectra[pl.ds(n * 4, 4)] = part.astype(BF).reshape(4, GROUPS, 2 * ORD, 512)
        return 0

    lax.fori_loop(0, 4, transform, 0)


def table_dft(orders, direction):
    return pl.pallas_call(
        table_dft_kernel,
        out_shape=(
            jax.ShapeDtypeStruct((1024, 1024), BF),
            jax.ShapeDtypeStruct((16, GROUPS, 2 * ORD, 512), BF),
        ),
        in_specs=[VM, VM],
        out_specs=(VM, VM),
        scratch_shapes=[pltpu.VMEM((512, 1024), BF), pltpu.VMEM((4096, 128), F32)],
        compiler_params=pltpu.CompilerParams(vmem_limit_bytes=40 * 1024 * 1024),
        name="table_dft",
    )(orders, direction)


def lane_swap():
    row = lax.broadcasted_iota(jnp.int32, (512, 512), 0)
    col = lax.broadcasted_iota(jnp.int32, (512, 512), 1)
    moved = (row // 32 % 4) * 128 + (row // 128) * 32 + row % 32
    return (col == moved).astype(F32).astype(BF)


def order_groups(order_table):
    pairs = order_table.reshape(16, 2, 16)[:, 0]
    low = jnp.minimum(pairs, 511 - pairs)
    swap = jnp.where(pairs == low, 0, 1024)
    both = jnp.stack([low + swap, 511 - low + swap], axis=1).reshape(512, 1)
    return jnp.broadcast_to(both, (512, 128))


def core_kernel(spectra, orders, legendre, temporal, out, full, part, leg, recv, blocks, mid, perm,
                coef, mixed, acc, far_in, fin_in, in_send, in_recv, own_send, fwd_send, dup_send,
                own_recv, fwd_recv, dup_recv, pair_send, pair_recv, far_send, far_recv, line_send,
                line_recv, out_send, out_recv):
    y, z = lax.axis_index("blk_0"), lax.axis_index("blk_1")
    x, core = lax.axis_index("tm_0"), lax.axis_index("tm_1")
    me = y * 4 + z
    right, left, far = (x + 1) % 4, (x + 3) % 4, (x + 2) % 4
    half = ORD // 2
    barrier = pltpu.get_barrier_semaphore()

    def greet(k, _):
        pl.semaphore_signal(
            barrier, inc=1, device_id={"blk_0": (y + k // 4) % 4, "blk_1": (z + k % 4) % 4},
            device_id_type=MESH,
        )
        return 0

    lax.fori_loop(1, 16, greet, 0)
    pl.semaphore_signal(barrier, inc=1, device_id={"tm_0": right}, device_id_type=MESH)
    pl.semaphore_signal(barrier, inc=1, device_id={"tm_0": left}, device_id_type=MESH)
    pl.semaphore_signal(barrier, inc=1, device_id={"tm_1": 1 - core}, device_id_type=MESH)
    pl.semaphore_wait(barrier, 18)
    side = ({"tm_0": right}, {"tm_0": left})
    peer = {"tm_1": 1 - core}

    def remote(src, dst, send, recv_sem, device):
        return pltpu.make_async_remote_copy(
            src_ref=src, dst_ref=dst, send_sem=send, recv_sem=recv_sem, device_id=device,
            device_id_type=MESH)

    def in_copy(g, k):
        ty, tz = (y + k // 4) % 4, (z + k % 4) % 4
        return remote(spectra.at[ty * 4 + tz, g], recv.at[g, me], in_send.at[g, k],
                      in_recv.at[g, k], {"blk_0": ty, "blk_1": tz})

    def out_copy(g, k):
        ty, tz = (y + k // 4) % 4, (z + k % 4) % 4
        return remote(blocks.at[g, ty * 4 + tz], out.at[me, g], out_send.at[g, k],
                      out_recv.at[g, k], {"blk_0": ty, "blk_1": tz})

    def hours(plane, who):
        return pl.ds(pl.multiple_of((plane * 2 + who) * 16, 16), 16)

    def piece(g, plane, first, count):
        return full.at[pl.ds(g * ORD + first, count), :, hours(plane, core), :]

    def own_copy(g, way):
        ref = piece(g, x, 0, ORD)
        return remote(ref, ref, own_send.at[g, way], own_recv.at[g, way], side[way])

    def fwd_copy(g, way):
        ref = piece(g, left if way == 0 else right, way * half, half)
        return remote(ref, ref, fwd_send.at[g, way], fwd_recv.at[g, way], side[way])

    def dup_copy(g, slot):
        plane, first, count = (
            (x, 0, ORD), (left, 0, ORD), (right, 0, ORD), (far, 0, half), (far, half, half))[slot]
        ref = piece(g, plane, first, count)
        return remote(ref, ref, dup_send.at[g, slot], dup_recv.at[g, slot], peer)

    planes = (far, right, left, x)

    def pair_copy(g, n):
        return remote(part.at[pl.ds(g * ORD, ORD), :, hours(planes[n], 1 - core), :], acc.at[g, n],
                      pair_send.at[g, n], pair_recv.at[g, n], peer)

    def far_copy(g, way):
        return remote(acc.at[g, 0, pl.ds(way * half, half)], far_in.at[g, way],
                      far_send.at[g, way], far_recv.at[g, way], side[way])

    def line_copy(g, way):
        return remote(acc.at[g, 1 + way], fin_in.at[g, way], line_send.at[g, way],
                      line_recv.at[g, way], side[way])

    def arrive(g):
        def wait(k, _):
            in_copy(g, k).wait_recv()
            return 0

        lax.fori_loop(1, 16, wait, 0)
        rows = []
        for sq in range(4):
            for tq in range(4):
                rows.append(jnp.concatenate(
                    [recv[g, sq * 4 + s, :, tq * 128 : (tq + 1) * 128] for s in range(4)], axis=1))
        moved = jnp.dot(jnp.concatenate(rows, axis=0), perm[...], preferred_element_type=F32)
        for sq in range(4):
            for tq in range(4):
                n = (sq * 4 + tq) * 16
                for t in range(4):
                    m = sq * 256 + (tq * 4 + t) * 16
                    mid[m : m + 16, :] = moved[n : n + 16, t * 128 : (t + 1) * 128]
        for c in range(2):
            for i in range(ORD):
                for sq in range(4):
                    full[g * ORD + i, c, hours(x, core), sq * 128 : (sq + 1) * 128] = (
                        mid[pl.ds(sq * 256 + c * ORD + i, 16, stride=16), :].astype(BF))
        own_copy(g, 0).start()
        own_copy(g, 1).start()
        dup_copy(g, 0).start()

    def forward(g):
        for way in range(2):
            own_copy(g, way).wait_recv()
            fwd_copy(g, way).start()
            dup_copy(g, 1 + way).start()

    def forward_far(g):
        for way in range(2):
            fwd_copy(g, way).wait_recv()
            dup_copy(g, 3 + way).start()

    def middle(g):
        for slot in range(5):
            dup_copy(g, slot).wait_recv()

        def analyse(i, _):
            value = lax.dot_general(
                leg[g * ORD + i], full[g * ORD + i].reshape(256, 512), (((1,), (1,)), ((), ())),
                preferred_element_type=F32)
            row = pl.multiple_of(i * 64, 64)
            coef[pl.ds(row, 64), :] = value[:, :128]
            coef[pl.ds(ORD * 64 + row, 64), :] = value[:, 128:]
            return 0

        lax.fori_loop(0, ORD, analyse, 0, unroll=2)

        def mix(n, _):
            for k in range(16):
                l = n * 16 + k
                rows = jnp.concatenate(
                    [coef[pl.ds(c * ORD * 64 + l, ORD, stride=64), :] for c in range(2)], axis=0)
                mixed[pl.ds(pl.multiple_of(l * 16, 16), 16), :] = jnp.dot(
                    rows.astype(BF), temporal[l].astype(BF), preferred_element_type=F32)
            return 0

        lax.fori_loop(0, 4, mix, 0)

        def synthesise(i, _):
            rows = jnp.concatenate(
                [mixed[pl.ds(c * ORD + i, 64, stride=16), :] for c in range(2)], axis=1)
            value = lax.dot_general(
                rows.astype(BF), leg[g * ORD + i], (((0,), (0,)), ((), ())),
                preferred_element_type=F32)
            part[g * ORD + i] = value.astype(BF).reshape(2, 128, 512)
            return 0

        lax.fori_loop(0, ORD, synthesise, 0, unroll=2)
        for n in range(4):
            pair_copy(g, n).start()

    def add_pair(g):
        for n in range(4):
            pair_copy(g, n).wait_recv()

            def step(i, _):
                own = part[g * ORD + i, :, hours(planes[n], core), :]
                acc[g, n, i] = (acc[g, n, i].astype(F32) + own.astype(F32)).astype(BF)
                return 0

            lax.fori_loop(0, ORD, step, 0)
            if n == 0:
                far_copy(g, 0).start()
                far_copy(g, 1).start()

    def add_far(g):
        for way in range(2):
            far_copy(g, way).wait_recv()

            def step(i, _):
                acc[g, 1 + way, way * half + i] = (
                    acc[g, 1 + way, way * half + i].astype(F32) + far_in[g, way, i].astype(F32)
                ).astype(BF)
                return 0

            lax.fori_loop(0, half, step, 0)
            line_copy(g, way).start()

    def depart(g):
        line_copy(g, 0).wait_recv()
        line_copy(g, 1).wait_recv()
        for i in range(ORD):
            for c in range(2):
                total = (acc[g, 3, i, c].astype(F32) + fin_in[g, 0, i, c].astype(F32)
                         + fin_in[g, 1, i, c].astype(F32))
                for sq in range(4):
                    mid[pl.ds(sq * 256 + c * ORD + i, 16, stride=16), :] = (
                        total[:, sq * 128 : (sq + 1) * 128])
        rows = []
        for sq in range(4):
            for tq in range(4):
                m = sq * 256 + tq * 64
                rows.append(jnp.concatenate(
                    [mid[m + t * 16 : m + (t + 1) * 16, :].astype(BF) for t in range(4)], axis=1))
        moved = jnp.dot(
            jnp.concatenate(rows, axis=0), perm[...], preferred_element_type=F32).astype(BF)
        for sq in range(4):
            for tq in range(4):
                n = (sq * 4 + tq) * 16
                for s in range(4):
                    blocks[g, sq * 4 + s, :, tq * 128 : (tq + 1) * 128] = (
                        moved[n : n + 16, s * 128 : (s + 1) * 128])

        def send(k, _):
            out_copy(g, k).start()
            return 0

        lax.fori_loop(1, 16, send, 0)
        out[pl.ds(me, 1), g] = blocks[g, pl.ds(me, 1)]

    def send_in(n, _):
        in_copy(n // 15, n % 15 + 1).start()
        return 0

    lax.fori_loop(0, GROUPS * 15, send_in, 0)
    for g in range(GROUPS):
        recv[g, pl.ds(me, 1)] = spectra[pl.ds(me, 1), g]
    perm[...] = lane_swap()
    degree = (x * 2 + core) * 64 + lax.broadcasted_iota(jnp.int32, (64, 512), 0)

    def mask(k, _):
        both = (legendre[k].astype(F32), legendre[16 + k].astype(F32))
        for h in range(2):
            entry = jnp.concatenate([orders[pl.ds(me * 32 + h * 16 + k, 1), :]] * 4, axis=1)
            entry = jnp.broadcast_to(entry, (64, 512))
            row = jnp.where(entry >= 1024, both[1 - h], both[h])
            leg[h * 16 + k] = jnp.where(degree >= entry % 1024, row, 0.0).astype(BF)
        return 0

    lax.fori_loop(0, 16, mask, 0)
    arrive(0)
    arrive(1)
    forward(0)
    arrive(2)
    forward(1)
    forward_far(0)
    arrive(3)
    middle(0)
    forward(2)
    forward_far(1)
    add_pair(0)
    middle(1)
    forward(3)
    add_pair(1)
    forward_far(2)
    middle(2)
    add_far(0)
    add_pair(2)
    forward_far(3)
    middle(3)
    add_far(1)
    add_pair(3)
    depart(0)
    add_far(2)
    depart(1)
    add_far(3)
    depart(2)
    depart(3)
    for g in range(GROUPS):
        for slot in range(5):
            dup_copy(g, slot).wait_send()
        for n in range(4):
            pair_copy(g, n).wait_send()
        for way in range(2):
            own_copy(g, way).wait_send()
            fwd_copy(g, way).wait_send()
            far_copy(g, way).wait_send()
            line_copy(g, way).wait_send()

    def finish(n, _):
        in_copy(n // 15, n % 15 + 1).wait_send()
        out_copy(n // 15, n % 15 + 1).wait_recv()
        out_copy(n // 15, n % 15 + 1).wait_send()
        return 0

    lax.fori_loop(0, GROUPS * 15, finish, 0)


def core_stage(spectra, orders, legendre, temporal):
    dma = pltpu.SemaphoreType.DMA
    two, four, five, blk = dma((GROUPS, 2)), dma((GROUPS, 4)), dma((GROUPS, 5)), dma((GROUPS, 16))
    return pl.pallas_call(
        core_kernel,
        out_shape=jax.ShapeDtypeStruct((16, GROUPS, 2 * ORD, 512), BF),
        in_specs=[VM] * 4,
        out_specs=VM,
        scratch_shapes=[
            pltpu.VMEM((32, 2, 128, 512), BF),
            pltpu.VMEM((32, 2, 128, 512), BF),
            pltpu.VMEM((32, 64, 512), BF),
            pltpu.VMEM((GROUPS, 16, 2 * ORD, 512), BF),
            pltpu.VMEM((GROUPS, 16, 2 * ORD, 512), BF),
            pltpu.VMEM((1024, 128), F32),
            pltpu.VMEM((512, 512), BF),
            pltpu.VMEM((2 * ORD * 64, 128), F32),
            pltpu.VMEM((2 * ORD * 64, 128), F32),
            pltpu.VMEM((GROUPS, 4, ORD, 2, 16, 512), BF),
            pltpu.VMEM((GROUPS, 2, ORD // 2, 2, 16, 512), BF),
            pltpu.VMEM((GROUPS, 2, ORD, 2, 16, 512), BF),
            blk, blk, two, two, five, two, two, five, four, four, two, two, two, two, blk, blk,
        ],
        compiler_params=pltpu.CompilerParams(
            collective_id=0, has_side_effects=True, vmem_limit_bytes=48 * 1024 * 1024),
        name="core_stage",
    )(spectra, orders, legendre, temporal)


def product_kernel(entries, table, residual, direction, noise, product, sums, split, stage, line,
                   plane, line_send, line_recv, plane_send, plane_recv):
    y, z = lax.axis_index("blk_0"), lax.axis_index("blk_1")
    x, core = lax.axis_index("tm_0"), lax.axis_index("tm_1")
    row, col = y * 4 + z, x * 2 + core

    def in_line(k):
        return {"tm_0": (x + k // 2) % 4, "tm_1": (core + k) % 2}

    def in_plane(k):
        return {"blk_0": (y + k // 4) % 4, "blk_1": (z + k % 4) % 4}

    barrier = pltpu.get_barrier_semaphore()

    def greet_line(k, _):
        pl.semaphore_signal(barrier, inc=1, device_id=in_line(k), device_id_type=MESH)
        return 0

    def greet_plane(k, _):
        pl.semaphore_signal(barrier, inc=1, device_id=in_plane(k), device_id_type=MESH)
        return 0

    lax.fori_loop(1, 8, greet_line, 0)
    lax.fori_loop(1, 16, greet_plane, 0)

    def synthesis(n, _):
        cols = entries[:, pl.ds(pl.multiple_of(n * 128, 128), 128)]
        block = lax.dot_general(cols, table[...], (((0,), (0,)), ((), ())), preferred_element_type=F32)
        for t in range(4):
            for q in range(8):
                split[pl.ds(q * 512 + n * 4 + t, 32, stride=16), :] = (
                    block[t * 32 : (t + 1) * 32, q * 128 : (q + 1) * 128])
        return 0

    lax.fori_loop(0, 4, synthesis, 0)

    def combine(n, totals):
        rows = pl.ds(pl.multiple_of(n * 8, 8), 8)
        nn, dp, rp, pp = totals
        for q in range(8):
            cols = slice(q * 128, (q + 1) * 128)
            d, r = direction[rows, cols], residual[rows, cols]
            p = split[pl.ds(pl.multiple_of(q * 512 + n * 8, 8), 8), :] + noise[rows, cols] * d
            product[rows, cols] = p
            nn, dp, rp, pp = nn + r * r, dp + d * p, rp + r * p, pp + p * p
        return nn, dp, rp, pp

    zero = jnp.zeros((8, 128), F32)
    totals = lax.fori_loop(0, 64, combine, (zero, zero, zero, zero))
    for k in range(4):
        stage[0, 2 * k : 2 * k + 2, :] = jnp.broadcast_to(
            jnp.sum(totals[k], axis=0, keepdims=True), (2, 128))
    pl.semaphore_wait(barrier, 22)

    def line_copy(k):
        return pltpu.make_async_remote_copy(
            src_ref=stage.at[0], dst_ref=line.at[col], send_sem=line_send.at[k],
            recv_sem=line_recv.at[k], device_id=in_line(k), device_id_type=MESH)

    def plane_copy(k):
        return pltpu.make_async_remote_copy(
            src_ref=stage.at[1], dst_ref=plane.at[row], send_sem=plane_send.at[k],
            recv_sem=plane_recv.at[k], device_id=in_plane(k), device_id_type=MESH)

    for k in range(1, 8):
        line_copy(k).start()
    line[pl.ds(col, 1)] = stage[0:1]
    for k in range(1, 8):
        line_copy(k).wait_recv()
    stage[1] = jnp.sum(line[...], axis=0)
    for k in range(1, 16):
        plane_copy(k).start()
    plane[pl.ds(row, 1)] = stage[1:2]
    for k in range(1, 16):
        plane_copy(k).wait_recv()
    sums[...] = jnp.sum(plane[...], axis=0)
    for k in range(1, 8):
        line_copy(k).wait_send()
    for k in range(1, 16):
        plane_copy(k).wait_send()


def product_sums(entries, table, residual, direction, noise):
    dma = pltpu.SemaphoreType.DMA
    return pl.pallas_call(
        product_kernel,
        out_shape=(jax.ShapeDtypeStruct((512, 1024), F32), jax.ShapeDtypeStruct((8, 128), F32)),
        in_specs=[VM] * 5,
        out_specs=(VM, VM),
        scratch_shapes=[
            pltpu.VMEM((4096, 128), F32),
            pltpu.VMEM((2, 8, 128), F32),
            pltpu.VMEM((8, 8, 128), F32),
            pltpu.VMEM((16, 8, 128), F32),
            dma((8,)), dma((8,)), dma((16,)), dma((16,)),
        ],
        compiler_params=pltpu.CompilerParams(
            collective_id=2, has_side_effects=True, vmem_limit_bytes=48 * 1024 * 1024),
        name="product_sums",
    )(entries, table, residual, direction, noise)


def update_kernel(sums, solution, residual, direction, product, solution_new, residual_new,
                  direction_new, stage, sems):
    def total(k):
        return jnp.sum(sums[2 * k : 2 * k + 1, :], axis=1, keepdims=True)

    norm_now, curvature, cross, square = total(0), total(1), total(2), total(3)
    step = norm_now / curvature
    norm_next = norm_now - 2.0 * step * cross + step * step * square
    ratio = norm_next / norm_now
    outs = (solution_new, residual_new, direction_new)

    def copy(n, k):
        rows = pl.ds(pl.multiple_of(n * 64, 64), 64)
        return pltpu.make_async_copy(stage.at[k, rows, :], outs[k].at[rows, :], sems.at[n, k])

    def block(n, _):
        rows = pl.ds(pl.multiple_of(n * 64, 64), 64)
        d = direction[rows, :]
        r = residual[rows, :] - step * product[rows, :]
        stage[0, rows, :] = solution[rows, :] + step * d
        stage[1, rows, :] = r
        stage[2, rows, :] = r + ratio * d
        for k in range(3):
            copy(n, k).start()
        return 0

    lax.fori_loop(0, 8, block, 0)

    def drain(n, _):
        for k in range(3):
            copy(n, k).wait()
        return 0

    lax.fori_loop(0, 8, drain, 0)


def update(sums, solution, residual, direction, product):
    shape = jax.ShapeDtypeStruct((512, 1024), F32)
    hbm = pl.BlockSpec(memory_space=pl.ANY)
    return pl.pallas_call(
        update_kernel,
        out_shape=(shape, shape, shape),
        in_specs=[VM] * 5,
        out_specs=(hbm, hbm, hbm),
        scratch_shapes=[pltpu.VMEM((3, 512, 1024), F32), pltpu.SemaphoreType.DMA((8, 3))],
        compiler_params=pltpu.CompilerParams(vmem_limit_bytes=24 * 1024 * 1024),
        name="update",
    )(sums, solution, residual, direction, product)


def body(solution, residual, direction, noise_var, legendre, temporal, order_table):
    shape = direction.shape
    flat = lambda v: v.reshape(512, 1024)
    orders = order_groups(order_table)
    table, spectra = table_dft(orders, flat(direction))
    entries = core_stage(spectra, orders, legendre, temporal).reshape(1024, 512)
    product, sums = product_sums(entries, table, flat(residual), flat(direction), flat(noise_var))
    outs = update(sums, flat(solution), flat(residual), flat(direction), product)
    return tuple(o.reshape(shape) for o in outs)


def solution(mesh):
    torus = Mesh(mesh.devices.reshape(4, 4, 4, 2), ("blk_0", "blk_1", "tm_0", "tm_1"))
    return jax.shard_map(
        body,
        mesh=torus,
        in_specs=(
            P(BLK, TM, None),
            P(BLK, TM, None),
            P(BLK, TM, None),
            P(BLK, TM, None),
            P(BLK, TM, None),
            P(TM, None, None),
            P(),
        ),
        out_specs=(P(BLK, TM, None), P(BLK, TM, None), P(BLK, TM, None)),
        check_vma=False,
    )
```

```python
import math

import jax
import jax.numpy as jnp
from jax import lax
from jax.experimental import pallas as pl
from jax.experimental.pallas import tpu as pltpu
from jax.sharding import Mesh
from jax.sharding import PartitionSpec as P

BLK = ("blk_0", "blk_1")
TM = ("tm_0", "tm_1")
BLK_TM = ("blk_0", "blk_1", "tm_0", "tm_1")
BF = jnp.bfloat16
F32 = jnp.float32
MESH = pl.DeviceIdType.MESH
GROUPS = 4
ORD = 8
VM = pl.BlockSpec(memory_space=pltpu.VMEM)


def unit_circle(phase):
    quadrant = (phase + 128) // 256
    x = (phase - quadrant * 256).astype(F32) * (2.0 * math.pi / 1024)
    x2 = x * x
    s = x * (1.0 + x2 * (-1.0 / 6 + x2 * (1.0 / 120 + x2 * (-1.0 / 5040 + x2 / 362880))))
    c = 1.0 + x2 * (-0.5 + x2 * (1.0 / 24 + x2 * (-1.0 / 720 + x2 / 40320)))
    odd = quadrant % 2 == 1
    cos = jnp.where(odd, s, c)
    sin = jnp.where(odd, c, s)
    cos = jnp.where((quadrant == 1) | (quadrant == 2), -cos, cos)
    sin = jnp.where((quadrant == 2) | (quadrant == 3), -sin, sin)
    return cos, sin


def lane_swap():
    row = lax.broadcasted_iota(jnp.int32, (512, 512), 0)
    col = lax.broadcasted_iota(jnp.int32, (512, 512), 1)
    moved = (row // 32 % 4) * 128 + (row // 128) * 32 + row % 32
    return (col == moved).astype(F32).astype(BF)


def step_kernel(orders, direction_in, residual_in, noise_in, legendre_in, temporal_in, product, sums,
                direction, residual, noise, legendre, temporal, load, split, rows, table, spectra,
                full, part, leg, recv, blocks, mid, perm, coef, mixed, acc, far_in, fin_in, out, synth,
                stage, line, plane, in_send, in_recv, own_send, fwd_send, dup_send,
                own_recv, fwd_recv, dup_recv, pair_send, pair_recv, far_send, far_recv, line_send,
                line_recv, out_send, out_recv, sum_send, sum_recv, all_send, all_recv):
    loads = [
        pltpu.make_async_copy(src, dst, load.at[n])
        for n, (src, dst) in enumerate((
            (direction_in, direction), (legendre_in, legendre), (temporal_in, temporal),
            (residual_in, residual), (noise_in, noise)))
    ]
    for copy in loads:
        copy.start()
    y, z = lax.axis_index("blk_0"), lax.axis_index("blk_1")
    x, core = lax.axis_index("tm_0"), lax.axis_index("tm_1")
    me = y * 4 + z
    right, left, far = (x + 1) % 4, (x + 3) % 4, (x + 2) % 4
    half = ORD // 2
    barrier = pltpu.get_barrier_semaphore()

    def greet(k, _):
        pl.semaphore_signal(
            barrier, inc=1, device_id={"blk_0": (y + k // 4) % 4, "blk_1": (z + k % 4) % 4},
            device_id_type=MESH,
        )
        return 0

    lax.fori_loop(1, 16, greet, 0)

    def in_line(k):
        return {"tm_0": (x + k // 2) % 4, "tm_1": (core + k) % 2}

    def greet_line(k, _):
        pl.semaphore_signal(barrier, inc=1, device_id=in_line(k), device_id_type=MESH)
        return 0

    lax.fori_loop(1, 8, greet_line, 0)
    side = ({"tm_0": right}, {"tm_0": left})
    peer = {"tm_1": 1 - core}

    def remote(src, dst, send, recv_sem, device):
        return pltpu.make_async_remote_copy(
            src_ref=src, dst_ref=dst, send_sem=send, recv_sem=recv_sem, device_id=device,
            device_id_type=MESH)

    def in_copy(g, k):
        ty, tz = (y + k // 4) % 4, (z + k % 4) % 4
        return remote(spectra.at[g, ty * 4 + tz], recv.at[g, me], in_send.at[g, k],
                      in_recv.at[g, k], {"blk_0": ty, "blk_1": tz})

    def out_copy(g, k):
        ty, tz = (y + k // 4) % 4, (z + k % 4) % 4
        return remote(blocks.at[g, ty * 4 + tz], out.at[g, me], out_send.at[g, k],
                      out_recv.at[g, k], {"blk_0": ty, "blk_1": tz})

    def hours(plane, who):
        return pl.ds(pl.multiple_of((plane * 2 + who) * 16, 16), 16)

    def piece(g, plane, first, count):
        return full.at[pl.ds(g * ORD + first, count), :, hours(plane, core), :]

    def own_copy(g, way):
        ref = piece(g, x, 0, ORD)
        return remote(ref, ref, own_send.at[g, way], own_recv.at[g, way], side[way])

    def fwd_copy(g, way):
        ref = piece(g, left if way == 0 else right, way * half, half)
        return remote(ref, ref, fwd_send.at[g, way], fwd_recv.at[g, way], side[way])

    def dup_copy(g, slot):
        plane, first, count = (
            (x, 0, ORD), (left, 0, ORD), (right, 0, ORD), (far, 0, half), (far, half, half))[slot]
        ref = piece(g, plane, first, count)
        return remote(ref, ref, dup_send.at[g, slot], dup_recv.at[g, slot], peer)

    planes = (far, right, left, x)

    def pair_copy(g, n):
        return remote(part.at[pl.ds(g * ORD, ORD), :, hours(planes[n], 1 - core), :], acc.at[g, n],
                      pair_send.at[g, n], pair_recv.at[g, n], peer)

    def far_copy(g, way):
        return remote(acc.at[g, 0, pl.ds(way * half, half)], far_in.at[g, way],
                      far_send.at[g, way], far_recv.at[g, way], side[way])

    def line_copy(g, way):
        return remote(acc.at[g, 1 + way], fin_in.at[g, way], line_send.at[g, way],
                      line_recv.at[g, way], side[way])

    def arrive(g):
        def wait(k, _):
            in_copy(g, k).wait_recv()
            return 0

        lax.fori_loop(1, 16, wait, 0)
        rows = []
        for sq in range(4):
            for tq in range(4):
                rows.append(jnp.concatenate(
                    [recv[g, sq * 4 + s, :, tq * 128 : (tq + 1) * 128] for s in range(4)], axis=1))
        moved = jnp.dot(jnp.concatenate(rows, axis=0), perm[...], preferred_element_type=F32)
        for sq in range(4):
            for tq in range(4):
                n = (sq * 4 + tq) * 16
                for t in range(4):
                    m = sq * 256 + (tq * 4 + t) * 16
                    mid[m : m + 16, :] = moved[n : n + 16, t * 128 : (t + 1) * 128]
        for c in range(2):
            for i in range(ORD):
                for sq in range(4):
                    full[g * ORD + i, c, hours(x, core), sq * 128 : (sq + 1) * 128] = (
                        mid[pl.ds(sq * 256 + c * ORD + i, 16, stride=16), :].astype(BF))
        own_copy(g, 0).start()
        own_copy(g, 1).start()
        dup_copy(g, 0).start()

    def forward(g):
        for way in range(2):
            own_copy(g, way).wait_recv()
            fwd_copy(g, way).start()
            dup_copy(g, 1 + way).start()

    def forward_far(g):
        for way in range(2):
            fwd_copy(g, way).wait_recv()
            dup_copy(g, 3 + way).start()

    def middle(g):
        for slot in range(5):
            dup_copy(g, slot).wait_recv()

        def analyse(i, _):
            value = lax.dot_general(
                leg[g * ORD + i], full[g * ORD + i].reshape(256, 512), (((1,), (1,)), ((), ())),
                preferred_element_type=F32)
            row = pl.multiple_of(i * 64, 64)
            coef[pl.ds(row, 64), :] = value[:, :128]
            coef[pl.ds(ORD * 64 + row, 64), :] = value[:, 128:]
            return 0

        lax.fori_loop(0, ORD, analyse, 0, unroll=2)

        def mix(n, _):
            for k in range(16):
                l = n * 16 + k
                rows = jnp.concatenate(
                    [coef[pl.ds(c * ORD * 64 + l, ORD, stride=64), :] for c in range(2)], axis=0)
                mixed[pl.ds(pl.multiple_of(l * 16, 16), 16), :] = jnp.dot(
                    rows.astype(BF), temporal[l].astype(BF), preferred_element_type=F32)
            return 0

        lax.fori_loop(0, 4, mix, 0)

        def synthesise(i, _):
            rows = jnp.concatenate(
                [mixed[pl.ds(c * ORD + i, 64, stride=16), :] for c in range(2)], axis=1)
            value = lax.dot_general(
                rows.astype(BF), leg[g * ORD + i], (((0,), (0,)), ((), ())),
                preferred_element_type=F32)
            part[g * ORD + i] = value.astype(BF).reshape(2, 128, 512)
            return 0

        lax.fori_loop(0, ORD, synthesise, 0, unroll=2)
        for n in range(4):
            pair_copy(g, n).start()

    def add_pair(g):
        for n in range(4):
            pair_copy(g, n).wait_recv()

            def step(i, _):
                own = part[g * ORD + i, :, hours(planes[n], core), :]
                acc[g, n, i] = (acc[g, n, i].astype(F32) + own.astype(F32)).astype(BF)
                return 0

            lax.fori_loop(0, ORD, step, 0)
            if n == 0:
                far_copy(g, 0).start()
                far_copy(g, 1).start()

    def add_far(g):
        for way in range(2):
            far_copy(g, way).wait_recv()

            def step(i, _):
                acc[g, 1 + way, way * half + i] = (
                    acc[g, 1 + way, way * half + i].astype(F32) + far_in[g, way, i].astype(F32)
                ).astype(BF)
                return 0

            lax.fori_loop(0, half, step, 0)
            line_copy(g, way).start()

    def depart(g):
        line_copy(g, 0).wait_recv()
        line_copy(g, 1).wait_recv()
        for i in range(ORD):
            for c in range(2):
                total = (acc[g, 3, i, c].astype(F32) + fin_in[g, 0, i, c].astype(F32)
                         + fin_in[g, 1, i, c].astype(F32))
                for sq in range(4):
                    mid[pl.ds(sq * 256 + c * ORD + i, 16, stride=16), :] = (
                        total[:, sq * 128 : (sq + 1) * 128])
        rows = []
        for sq in range(4):
            for tq in range(4):
                m = sq * 256 + tq * 64
                rows.append(jnp.concatenate(
                    [mid[m + t * 16 : m + (t + 1) * 16, :].astype(BF) for t in range(4)], axis=1))
        moved = jnp.dot(
            jnp.concatenate(rows, axis=0), perm[...], preferred_element_type=F32).astype(BF)
        for sq in range(4):
            for tq in range(4):
                n = (sq * 4 + tq) * 16
                for s in range(4):
                    blocks[g, sq * 4 + s, :, tq * 128 : (tq + 1) * 128] = (
                        moved[n : n + 16, s * 128 : (s + 1) * 128])

        def send(k, _):
            out_copy(g, k).start()
            return 0

        lax.fori_loop(1, 16, send, 0)
        out[g, pl.ds(me, 1)] = blocks[g, pl.ds(me, 1)]

    def sum_copy(k):
        return remote(stage.at[0], line.at[x * 2 + core], sum_send.at[k], sum_recv.at[k], in_line(k))

    def all_copy(k):
        return remote(stage.at[1], plane.at[me], all_send.at[k], all_recv.at[k],
                      {"blk_0": (y + k // 4) % 4, "blk_1": (z + k % 4) % 4})

    def order_rows(block, odd):
        sub = lax.broadcasted_iota(jnp.int32, (ORD, 128), 0)
        value = jnp.zeros((ORD, 128), jnp.int32)
        for i in range(ORD):
            value = jnp.where(sub == i, orders[block * 32 + odd * ORD + i], value)
        low = jnp.minimum(value, 511 - value)
        return low + jnp.where(value == low, 0, 1024)

    loads[0].wait()
    lat, time = 32, 16
    for q in range(8):
        split[q * 512 : (q + 1) * 512, :] = direction[:, q * 128 : (q + 1) * 128]

    def gather(t, _):
        for q in range(8):
            rows[pl.ds(pl.multiple_of(t * lat, lat), lat), q * 128 : (q + 1) * 128] = split[
                pl.ds(q * 512 + t, lat, stride=time), :
            ].astype(BF)
        return 0

    lax.fori_loop(0, time, gather, 0, unroll=2)
    lane = lax.broadcasted_iota(jnp.int32, (4 * ORD, 128), 1)
    scale = 1.0 / math.sqrt(512.0)
    for g in range(GROUPS):
        def fill(n, _):
            m = jnp.concatenate([order_rows(n * 4 + k, g % 2) for k in range(4)], axis=0) % 1024
            m = m if g < 2 else 511 - m
            cos, sin = unit_circle((m * lane) % 1024)
            turn_c, turn_s = unit_circle((m * 128) % 1024)
            cos, sin = cos * scale, sin * scale
            for q in range(8):
                both = jnp.concatenate(
                    [v[k * ORD : (k + 1) * ORD] for k in range(4) for v in (cos, sin)], axis=0)
                table[pl.ds(pl.multiple_of(g * 256 + n * 64, 64), 64), q * 128 : (q + 1) * 128] = (
                    both.astype(BF))
                cos, sin = cos * turn_c - sin * turn_s, sin * turn_c + cos * turn_s
            return 0

        lax.fori_loop(0, 4, fill, 0)
        spectra[g] = lax.dot_general(
            table[g * 256 : (g + 1) * 256, :], rows[...], (((1,), (1,)), ((), ())),
            preferred_element_type=F32).astype(BF).reshape(16, 2 * ORD, 512)
        if g == 0:
            pl.semaphore_wait(barrier, 22)

        def send_in(k, _):
            in_copy(g, k).start()
            return 0

        lax.fori_loop(1, 16, send_in, 0)
        recv[g, pl.ds(me, 1)] = spectra[g, pl.ds(me, 1)]
    perm[...] = lane_swap()
    arrive(0)
    degree = (x * 2 + core) * 64 + lax.broadcasted_iota(jnp.int32, (64, 512), 0)
    loads[1].wait()
    loads[2].wait()
    for odd in range(2):
        entry_rows = order_rows(me, odd)
        for k in range(ORD):
            n = odd * ORD + k
            first, second = legendre[n].astype(F32), legendre[16 + n].astype(F32)
            entry = jnp.broadcast_to(
                jnp.concatenate([entry_rows[k : k + 1, :]] * 4, axis=1), (64, 512))
            swap, low = entry >= 1024, entry % 1024
            leg[n] = jnp.where(degree >= low, jnp.where(swap, second, first), 0.0).astype(BF)
            leg[16 + n] = jnp.where(degree >= 511 - low, jnp.where(swap, first, second), 0.0).astype(BF)
    arrive(1)
    forward(0)
    arrive(2)
    forward(1)
    forward_far(0)
    arrive(3)
    middle(0)
    forward(2)
    forward_far(1)
    add_pair(0)
    middle(1)
    forward(3)
    add_pair(1)
    forward_far(2)
    middle(2)
    add_far(0)
    add_pair(2)
    forward_far(3)
    middle(3)
    add_far(1)
    add_pair(3)
    depart(0)
    add_far(2)
    depart(1)
    add_far(3)
    depart(2)

    def arrived(g):
        def wait(k, _):
            out_copy(g, k).wait_recv()
            return 0

        lax.fori_loop(1, 16, wait, 0)

    def transform(first, count, n):
        cols = pl.ds(pl.multiple_of(n * 128, 128), 128)
        value = out[first : first + count, :, :, cols].reshape(count * 256, 128)
        return lax.dot_general(
            value, table[first * 256 : (first + count) * 256, :], (((0,), (0,)), ((), ())),
            preferred_element_type=F32)

    arrived(0)
    arrived(1)

    def partial(n, _):
        synth[pl.ds(pl.multiple_of(n * 128, 128), 128), :] = transform(0, 2, n)
        return 0

    lax.fori_loop(0, 4, partial, 0)
    depart(3)
    arrived(2)

    def partial2(n, _):
        synth[pl.ds(pl.multiple_of(n * 128, 128), 128), :] += transform(2, 1, n)
        return 0

    lax.fori_loop(0, 4, partial2, 0)
    loads[3].wait()
    loads[4].wait()
    arrived(3)

    def synthesis(n, _):
        block = synth[pl.ds(pl.multiple_of(n * 128, 128), 128), :] + transform(3, 1, n)
        for t in range(4):
            for q in range(8):
                split[pl.ds(q * 512 + n * 4 + t, 32, stride=16), :] = (
                    block[t * 32 : (t + 1) * 32, q * 128 : (q + 1) * 128])
        return 0

    lax.fori_loop(0, 4, synthesis, 0)

    def combine(n, totals):
        r8 = pl.ds(pl.multiple_of(n * 8, 8), 8)
        nn, dp, rp, pp = totals
        for q in range(8):
            cols = slice(q * 128, (q + 1) * 128)
            d, r = direction[r8, cols], residual[r8, cols]
            p = split[pl.ds(pl.multiple_of(q * 512 + n * 8, 8), 8), :] + noise[r8, cols] * d
            product[r8, cols] = p
            nn, dp, rp, pp = nn + r * r, dp + d * p, rp + r * p, pp + p * p
        return nn, dp, rp, pp

    zero = jnp.zeros((8, 128), F32)
    totals = lax.fori_loop(0, 64, combine, (zero, zero, zero, zero), unroll=2)
    for k in range(4):
        stage[0, 2 * k : 2 * k + 2, :] = jnp.broadcast_to(
            jnp.sum(totals[k], axis=0, keepdims=True), (2, 128))
    for k in range(1, 8):
        sum_copy(k).start()
    line[pl.ds(x * 2 + core, 1)] = stage[0:1]
    for k in range(1, 8):
        sum_copy(k).wait_recv()
    stage[1] = jnp.sum(line[...], axis=0)
    for k in range(1, 16):
        all_copy(k).start()
    plane[pl.ds(me, 1)] = stage[1:2]
    for k in range(1, 16):
        all_copy(k).wait_recv()
    sums[...] = jnp.sum(plane[...], axis=0)
    for k in range(1, 8):
        sum_copy(k).wait_send()
    for k in range(1, 16):
        all_copy(k).wait_send()
    for g in range(GROUPS):
        for slot in range(5):
            dup_copy(g, slot).wait_send()
        for n in range(4):
            pair_copy(g, n).wait_send()
        for way in range(2):
            own_copy(g, way).wait_send()
            fwd_copy(g, way).wait_send()
            far_copy(g, way).wait_send()
            line_copy(g, way).wait_send()

    def finish(n, _):
        in_copy(n // 15, n % 15 + 1).wait_send()
        out_copy(n // 15, n % 15 + 1).wait_send()
        return 0

    lax.fori_loop(0, GROUPS * 15, finish, 0)


def step_stage(orders, direction, residual, noise, legendre, temporal):
    dma = pltpu.SemaphoreType.DMA
    two, four, five, blk = dma((GROUPS, 2)), dma((GROUPS, 4)), dma((GROUPS, 5)), dma((GROUPS, 16))
    grid = pltpu.VMEM((512, 1024), F32)
    hbm = pl.BlockSpec(memory_space=pl.ANY)
    return pl.pallas_call(
        step_kernel,
        out_shape=(jax.ShapeDtypeStruct((512, 1024), F32), jax.ShapeDtypeStruct((8, 128), F32)),
        in_specs=[pl.BlockSpec(memory_space=pltpu.SMEM)] + [hbm] * 5,
        out_specs=(VM, VM),
        scratch_shapes=[
            grid, grid, grid,
            pltpu.VMEM((32, 64, 512), BF),
            pltpu.VMEM((64, 128, 128), F32),
            dma((5,)),
            pltpu.VMEM((4096, 128), F32),
            pltpu.VMEM((512, 1024), BF),
            pltpu.VMEM((1024, 1024), BF),
            pltpu.VMEM((GROUPS, 16, 2 * ORD, 512), BF),
            pltpu.VMEM((32, 2, 128, 512), BF),
            pltpu.VMEM((32, 2, 128, 512), BF),
            pltpu.VMEM((32, 64, 512), BF),
            pltpu.VMEM((GROUPS, 16, 2 * ORD, 512), BF),
            pltpu.VMEM((GROUPS, 16, 2 * ORD, 512), BF),
            pltpu.VMEM((1024, 128), F32),
            pltpu.VMEM((512, 512), BF),
            pltpu.VMEM((2 * ORD * 64, 128), F32),
            pltpu.VMEM((2 * ORD * 64, 128), F32),
            pltpu.VMEM((GROUPS, 4, ORD, 2, 16, 512), BF),
            pltpu.VMEM((GROUPS, 2, ORD // 2, 2, 16, 512), BF),
            pltpu.VMEM((GROUPS, 2, ORD, 2, 16, 512), BF),
            pltpu.VMEM((GROUPS, 16, 2 * ORD, 512), BF),
            grid,
            pltpu.VMEM((2, 8, 128), F32),
            pltpu.VMEM((8, 8, 128), F32),
            pltpu.VMEM((16, 8, 128), F32),
            blk, blk, two, two, five, two, two, five, four, four, two, two, two, two, blk, blk,
            dma((8,)), dma((8,)), dma((16,)), dma((16,)),
        ],
        compiler_params=pltpu.CompilerParams(
            collective_id=0, has_side_effects=True, vmem_limit_bytes=54 * 1024 * 1024),
        name="step_stage",
    )(orders, direction, residual, noise, legendre, temporal)


def update_kernel(sums, solution, residual, direction, product, solution_new, residual_new,
                  direction_new, stage, sems):
    def total(k):
        return jnp.sum(sums[2 * k : 2 * k + 1, :], axis=1, keepdims=True)

    norm_now, curvature, cross, square = total(0), total(1), total(2), total(3)
    step = norm_now / curvature
    norm_next = norm_now - 2.0 * step * cross + step * step * square
    ratio = norm_next / norm_now
    outs = (solution_new, residual_new, direction_new)

    def copy(n, k):
        rows = pl.ds(pl.multiple_of(n * 64, 64), 64)
        return pltpu.make_async_copy(stage.at[k, rows, :], outs[k].at[rows, :], sems.at[n, k])

    def block(n, _):
        rows = pl.ds(pl.multiple_of(n * 64, 64), 64)
        d = direction[rows, :]
        r = residual[rows, :] - step * product[rows, :]
        stage[0, rows, :] = solution[rows, :] + step * d
        stage[1, rows, :] = r
        stage[2, rows, :] = r + ratio * d
        for k in range(3):
            copy(n, k).start()
        return 0

    lax.fori_loop(0, 8, block, 0)

    def drain(n, _):
        for k in range(3):
            copy(n, k).wait()
        return 0

    lax.fori_loop(0, 8, drain, 0)


def update(sums, solution, residual, direction, product):
    shape = jax.ShapeDtypeStruct((512, 1024), F32)
    hbm = pl.BlockSpec(memory_space=pl.ANY)
    return pl.pallas_call(
        update_kernel,
        out_shape=(shape, shape, shape),
        in_specs=[VM] * 5,
        out_specs=(hbm, hbm, hbm),
        scratch_shapes=[pltpu.VMEM((3, 512, 1024), F32), pltpu.SemaphoreType.DMA((8, 3))],
        compiler_params=pltpu.CompilerParams(vmem_limit_bytes=24 * 1024 * 1024),
        name="update",
    )(sums, solution, residual, direction, product)


def body(solution, residual, direction, noise_var, legendre, temporal, order_table):
    shape = direction.shape
    flat = lambda v: v.reshape(512, 1024)
    product, sums = step_stage(
        order_table, flat(direction), flat(residual), flat(noise_var), legendre, temporal)
    outs = update(sums, flat(solution), flat(residual), flat(direction), product)
    return tuple(o.reshape(shape) for o in outs)


def solution(mesh):
    torus = Mesh(mesh.devices.reshape(4, 4, 4, 2), ("blk_0", "blk_1", "tm_0", "tm_1"))
    return jax.shard_map(
        body,
        mesh=torus,
        in_specs=(
            P(BLK, TM, None),
            P(BLK, TM, None),
            P(BLK, TM, None),
            P(BLK, TM, None),
            P(BLK, TM, None),
            P(TM, None, None),
            P(),
        ),
        out_specs=(P(BLK, TM, None), P(BLK, TM, None), P(BLK, TM, None)),
        check_vma=False,
    )
```

```python
import math

import jax
import jax.numpy as jnp
from jax import lax
from jax.experimental import pallas as pl
from jax.experimental.pallas import tpu as pltpu
from jax.sharding import Mesh
from jax.sharding import PartitionSpec as P

BLK = ("blk_0", "blk_1")
TM = ("tm_0", "tm_1")
BLK_TM = ("blk_0", "blk_1", "tm_0", "tm_1")
BF = jnp.bfloat16
F32 = jnp.float32
MESH = pl.DeviceIdType.MESH
GROUPS = 4
ORD = 8
FIRST = (4, 5, 6, 0)
VM = pl.BlockSpec(memory_space=pltpu.VMEM)


def unit_circle(phase):
    quadrant = (phase + 128) // 256
    x = (phase - quadrant * 256).astype(F32) * (2.0 * math.pi / 1024)
    x2 = x * x
    s = x * (1.0 + x2 * (-1.0 / 6 + x2 * (1.0 / 120 + x2 * (-1.0 / 5040 + x2 / 362880))))
    c = 1.0 + x2 * (-0.5 + x2 * (1.0 / 24 + x2 * (-1.0 / 720 + x2 / 40320)))
    odd = quadrant % 2 == 1
    cos = jnp.where(odd, s, c)
    sin = jnp.where(odd, c, s)
    cos = jnp.where((quadrant == 1) | (quadrant == 2), -cos, cos)
    sin = jnp.where((quadrant == 2) | (quadrant == 3), -sin, sin)
    return cos, sin


def lane_swap():
    row = lax.broadcasted_iota(jnp.int32, (512, 512), 0)
    col = lax.broadcasted_iota(jnp.int32, (512, 512), 1)
    moved = (row // 32 % 4) * 128 + (row // 128) * 32 + row % 32
    return (col == moved).astype(F32).astype(BF)


def step_kernel(orders, direction_in, residual_in, solution_in, noise_in, legendre_in, temporal_in,
                product, sums, direction, residual, solution, noise, legendre, temporal, load, split,
                rows, table, spectra, ring, full, part, leg, recv, blocks, mid, perm, coef, mixed, acc,
                far_in, fin_in, last_far, last_fin, last, out, synth, stage, line, plane, in_send, in_recv, own_send, fwd_send, dup_send,
                own_recv, fwd_recv, dup_recv, pair_send, pair_recv, far_send, far_recv, line_send,
                line_recv, out_send, out_recv, sum_send, sum_recv, all_send, all_recv):
    loads = [
        pltpu.make_async_copy(src, dst, load.at[n])
        for n, (src, dst) in enumerate((
            (direction_in, direction), (legendre_in, legendre), (temporal_in, temporal),
            (residual_in, residual), (noise_in, noise), (solution_in, solution)))
    ]
    for copy in loads:
        copy.start()
    y, z = lax.axis_index("blk_0"), lax.axis_index("blk_1")
    x, core = lax.axis_index("tm_0"), lax.axis_index("tm_1")
    me = y * 4 + z
    right, left, far = (x + 1) % 4, (x + 3) % 4, (x + 2) % 4
    half = ORD // 2
    barrier = pltpu.get_barrier_semaphore()

    def greet(k, _):
        pl.semaphore_signal(
            barrier, inc=1, device_id={"blk_0": (y + k // 4) % 4, "blk_1": (z + k % 4) % 4},
            device_id_type=MESH,
        )
        return 0

    lax.fori_loop(1, 16, greet, 0)

    def in_line(k):
        return {"tm_0": (x + k // 2) % 4, "tm_1": (core + k) % 2}

    def greet_line(k, _):
        pl.semaphore_signal(barrier, inc=1, device_id=in_line(k), device_id_type=MESH)
        return 0

    lax.fori_loop(1, 8, greet_line, 0)
    side = ({"tm_0": right}, {"tm_0": left})
    peer = {"tm_1": 1 - core}

    def remote(src, dst, send, recv_sem, device):
        return pltpu.make_async_remote_copy(
            src_ref=src, dst_ref=dst, send_sem=send, recv_sem=recv_sem, device_id=device,
            device_id_type=MESH)

    def in_copy(g, k):
        ty, tz = (y + k // 4) % 4, (z + k % 4) % 4
        return remote(spectra.at[g, ty * 4 + tz], recv.at[g, me], in_send.at[g, k],
                      in_recv.at[g, k], {"blk_0": ty, "blk_1": tz})

    def in_first(slot, k):
        ty, tz = (y + k // 4) % 4, (z + k % 4) % 4
        dest = ty * 4 + tz
        src = spectra.at[0, dest] if slot == 3 else ring.at[slot, dest]
        return remote(src, recv.at[FIRST[slot], me], in_send.at[FIRST[slot], k],
                      in_recv.at[FIRST[slot], k], {"blk_0": ty, "blk_1": tz})

    def ring_copy(way):
        return remote(spectra.at[0], ring.at[way], own_send.at[0, way], own_recv.at[0, way], side[way])

    def ring_forward(way):
        return remote(ring.at[way, pl.ds(way * 8, 8)], ring.at[2, pl.ds(way * 8, 8)],
                      fwd_send.at[0, way], fwd_recv.at[0, way], side[way])

    def dup_first(slot):
        ref = piece(0, (left, right, far, x)[slot], 0, ORD)
        return remote(ref, ref, dup_send.at[0, slot], dup_recv.at[0, slot], peer)

    def out_last(n, k):
        ty, tz = (y + k // 4) % 4, (z + k % 4) % 4
        return remote(blocks.at[3 + n, ty * 4 + tz], last.at[n, me], out_send.at[3 + n, k],
                      out_recv.at[3 + n, k], {"blk_0": ty, "blk_1": tz})

    def last_far_copy(way):
        return remote(last.at[0, pl.ds(way * 8, 8)], last_far.at[way], far_send.at[3, way],
                      far_recv.at[3, way], side[way])

    def last_line_copy(way):
        return remote(last.at[1 + way], last_fin.at[way], line_send.at[3, way],
                      line_recv.at[3, way], side[way])

    def out_copy(g, k):
        ty, tz = (y + k // 4) % 4, (z + k % 4) % 4
        return remote(blocks.at[g, ty * 4 + tz], out.at[g, me], out_send.at[g, k],
                      out_recv.at[g, k], {"blk_0": ty, "blk_1": tz})

    def hours(plane, who):
        return pl.ds(pl.multiple_of((plane * 2 + who) * 16, 16), 16)

    def piece(g, plane, first, count):
        return full.at[pl.ds(g * ORD + first, count), :, hours(plane, core), :]

    def own_copy(g, way):
        ref = piece(g, x, 0, ORD)
        return remote(ref, ref, own_send.at[g, way], own_recv.at[g, way], side[way])

    def fwd_copy(g, way):
        ref = piece(g, left if way == 0 else right, way * half, half)
        return remote(ref, ref, fwd_send.at[g, way], fwd_recv.at[g, way], side[way])

    def dup_copy(g, slot):
        plane, first, count = (
            (x, 0, ORD), (left, 0, ORD), (right, 0, ORD), (far, 0, half), (far, half, half))[slot]
        ref = piece(g, plane, first, count)
        return remote(ref, ref, dup_send.at[g, slot], dup_recv.at[g, slot], peer)

    planes = (far, right, left, x)

    def pair_copy(g, n):
        return remote(part.at[pl.ds(g * ORD, ORD), :, hours(planes[n], 1 - core), :], acc.at[g, n],
                      pair_send.at[g, n], pair_recv.at[g, n], peer)

    def far_copy(g, way):
        return remote(acc.at[g, 0, pl.ds(way * half, half)], far_in.at[g, way],
                      far_send.at[g, way], far_recv.at[g, way], side[way])

    def line_copy(g, way):
        return remote(acc.at[g, 1 + way], fin_in.at[g, way], line_send.at[g, way],
                      line_recv.at[g, way], side[way])

    def regroup_in(n, g, plane_of):
        blocks_in = []
        for sq in range(4):
            for tq in range(4):
                blocks_in.append(jnp.concatenate(
                    [recv[n, sq * 4 + s, :, tq * 128 : (tq + 1) * 128] for s in range(4)], axis=1))
        moved = jnp.dot(jnp.concatenate(blocks_in, axis=0), perm[...], preferred_element_type=F32)
        for sq in range(4):
            for tq in range(4):
                n0 = (sq * 4 + tq) * 16
                for t in range(4):
                    m = sq * 256 + (tq * 4 + t) * 16
                    mid[m : m + 16, :] = moved[n0 : n0 + 16, t * 128 : (t + 1) * 128]
        for c in range(2):
            for i in range(ORD):
                for sq in range(4):
                    full[g * ORD + i, c, hours(plane_of, core), sq * 128 : (sq + 1) * 128] = (
                        mid[pl.ds(sq * 256 + c * ORD + i, 16, stride=16), :].astype(BF))

    def arrive(g):
        def wait(k, _):
            in_copy(g, k).wait_recv()
            return 0

        lax.fori_loop(1, 16, wait, 0)
        regroup_in(g, g, x)
        own_copy(g, 0).start()
        own_copy(g, 1).start()
        dup_copy(g, 0).start()

    def send_first(slot):
        def send(k, _):
            in_first(slot, k).start()
            return 0

        lax.fori_loop(1, 16, send, 0)
        src = spectra if slot == 3 else ring
        recv[FIRST[slot], pl.ds(me, 1)] = src[0 if slot == 3 else slot, pl.ds(me, 1)]

    def arrive_first(slot):
        def wait(k, _):
            in_first(slot, k).wait_recv()
            return 0

        lax.fori_loop(1, 16, wait, 0)
        regroup_in(FIRST[slot], 0, (left, right, far, x)[slot])
        dup_first(slot).start()

    def forward_first():
        for way in range(2):
            ring_copy(way).wait_recv()
            ring_forward(way).start()
        for way in range(2):
            send_first(way)

    def far_first():
        for way in range(2):
            ring_forward(way).wait_recv()
        send_first(2)

    def forward(g):
        for way in range(2):
            own_copy(g, way).wait_recv()
            fwd_copy(g, way).start()
            dup_copy(g, 1 + way).start()

    def forward_far(g):
        for way in range(2):
            fwd_copy(g, way).wait_recv()
            dup_copy(g, 3 + way).start()

    def middle(g):
        if g == 0:
            for slot in range(4):
                dup_first(slot).wait_recv()
        else:
            for slot in range(5):
                dup_copy(g, slot).wait_recv()

        def analyse(i, _):
            value = lax.dot_general(
                leg[g * ORD + i], full[g * ORD + i].reshape(256, 512), (((1,), (1,)), ((), ())),
                preferred_element_type=F32)
            row = pl.multiple_of(i * 64, 64)
            coef[pl.ds(row, 64), :] = value[:, :128]
            coef[pl.ds(ORD * 64 + row, 64), :] = value[:, 128:]
            return 0

        lax.fori_loop(0, ORD, analyse, 0, unroll=2)

        def mix(n, _):
            for k in range(16):
                l = n * 16 + k
                rows = jnp.concatenate(
                    [coef[pl.ds(c * ORD * 64 + l, ORD, stride=64), :] for c in range(2)], axis=0)
                mixed[pl.ds(pl.multiple_of(l * 16, 16), 16), :] = jnp.dot(
                    rows.astype(BF), temporal[l].astype(BF), preferred_element_type=F32)
            return 0

        lax.fori_loop(0, 4, mix, 0)

        def synthesise(i, _):
            rows = jnp.concatenate(
                [mixed[pl.ds(c * ORD + i, 64, stride=16), :] for c in range(2)], axis=1)
            value = lax.dot_general(
                rows.astype(BF), leg[g * ORD + i], (((0,), (0,)), ((), ())),
                preferred_element_type=F32)
            part[g * ORD + i] = value.astype(BF).reshape(2, 128, 512)
            return 0

        lax.fori_loop(0, ORD, synthesise, 0, unroll=2)
        for n in range(4):
            pair_copy(g, n).start()

    def add_pair(g):
        for n in range(4):
            pair_copy(g, n).wait_recv()

            def step(i, _):
                own = part[g * ORD + i, :, hours(planes[n], core), :]
                acc[g, n, i] = (acc[g, n, i].astype(F32) + own.astype(F32)).astype(BF)
                return 0

            lax.fori_loop(0, ORD, step, 0)
            if g == GROUPS - 1:
                regroup_out(3 + n, lambda i, c: acc[g, n, i, c].astype(F32))

                def send(k, _):
                    out_last(n, k).start()
                    return 0

                lax.fori_loop(1, 16, send, 0)
                last[n, pl.ds(me, 1)] = blocks[3 + n, pl.ds(me, 1)]
            elif n == 0:
                far_copy(g, 0).start()
                far_copy(g, 1).start()

    def add_far(g):
        for way in range(2):
            far_copy(g, way).wait_recv()

            def step(i, _):
                acc[g, 1 + way, way * half + i] = (
                    acc[g, 1 + way, way * half + i].astype(F32) + far_in[g, way, i].astype(F32)
                ).astype(BF)
                return 0

            lax.fori_loop(0, half, step, 0)
            line_copy(g, way).start()

    def regroup_out(n, value):
        for i in range(ORD):
            for c in range(2):
                total = value(i, c)
                for sq in range(4):
                    mid[pl.ds(sq * 256 + c * ORD + i, 16, stride=16), :] = (
                        total[:, sq * 128 : (sq + 1) * 128])
        rows_out = []
        for sq in range(4):
            for tq in range(4):
                m = sq * 256 + tq * 64
                rows_out.append(jnp.concatenate(
                    [mid[m + t * 16 : m + (t + 1) * 16, :].astype(BF) for t in range(4)], axis=1))
        moved = jnp.dot(
            jnp.concatenate(rows_out, axis=0), perm[...], preferred_element_type=F32).astype(BF)
        for sq in range(4):
            for tq in range(4):
                n0 = (sq * 4 + tq) * 16
                for s in range(4):
                    blocks[n, sq * 4 + s, :, tq * 128 : (tq + 1) * 128] = (
                        moved[n0 : n0 + 16, s * 128 : (s + 1) * 128])

    def depart(g):
        line_copy(g, 0).wait_recv()
        line_copy(g, 1).wait_recv()
        regroup_out(g, lambda i, c: acc[g, 3, i, c].astype(F32) + fin_in[g, 0, i, c].astype(F32)
                    + fin_in[g, 1, i, c].astype(F32))

        def send(k, _):
            out_copy(g, k).start()
            return 0

        lax.fori_loop(1, 16, send, 0)
        out[g, pl.ds(me, 1)] = blocks[g, pl.ds(me, 1)]

    def last_arrived(n):
        def wait(k, _):
            out_last(n, k).wait_recv()
            return 0

        lax.fori_loop(1, 16, wait, 0)

    def last_add(way):
        last_arrived(1 + way)
        last_far_copy(way).wait_recv()

        def step(j, _):
            last[1 + way, way * 8 + j] = (
                last[1 + way, way * 8 + j].astype(F32) + last_far[way, j].astype(F32)).astype(BF)
            return 0

        lax.fori_loop(0, 8, step, 0)
        last_line_copy(way).start()

    def sum_copy(k):
        return remote(stage.at[0], line.at[x * 2 + core], sum_send.at[k], sum_recv.at[k], in_line(k))

    def all_copy(k):
        return remote(stage.at[1], plane.at[me], all_send.at[k], all_recv.at[k],
                      {"blk_0": (y + k // 4) % 4, "blk_1": (z + k % 4) % 4})

    def order_rows(block, odd):
        sub = lax.broadcasted_iota(jnp.int32, (ORD, 128), 0)
        value = jnp.zeros((ORD, 128), jnp.int32)
        for i in range(ORD):
            value = jnp.where(sub == i, orders[block * 32 + odd * ORD + i], value)
        low = jnp.minimum(value, 511 - value)
        return low + jnp.where(value == low, 0, 1024)

    loads[0].wait()
    lat, time = 32, 16
    for q in range(8):
        split[q * 512 : (q + 1) * 512, :] = direction[:, q * 128 : (q + 1) * 128]

    def gather(t, _):
        for q in range(8):
            rows[pl.ds(pl.multiple_of(t * lat, lat), lat), q * 128 : (q + 1) * 128] = split[
                pl.ds(q * 512 + t, lat, stride=time), :
            ].astype(BF)
        return 0

    lax.fori_loop(0, time, gather, 0, unroll=2)
    lane = lax.broadcasted_iota(jnp.int32, (4 * ORD, 128), 1)
    scale = 1.0 / math.sqrt(512.0)
    for g in range(GROUPS):
        def fill(n, _):
            m = jnp.concatenate([order_rows(n * 4 + k, g % 2) for k in range(4)], axis=0) % 1024
            m = m if g < 2 else 511 - m
            cos, sin = unit_circle((m * lane) % 1024)
            turn_c, turn_s = unit_circle((m * 128) % 1024)
            cos, sin = cos * scale, sin * scale
            for q in range(8):
                both = jnp.concatenate(
                    [v[k * ORD : (k + 1) * ORD] for k in range(4) for v in (cos, sin)], axis=0)
                table[pl.ds(pl.multiple_of(g * 256 + n * 64, 64), 64), q * 128 : (q + 1) * 128] = (
                    both.astype(BF))
                cos, sin = cos * turn_c - sin * turn_s, sin * turn_c + cos * turn_s
            return 0

        lax.fori_loop(0, 4, fill, 0)
        spectra[g] = lax.dot_general(
            table[g * 256 : (g + 1) * 256, :], rows[...], (((1,), (1,)), ((), ())),
            preferred_element_type=F32).astype(BF).reshape(16, 2 * ORD, 512)
        if g == 0:
            pl.semaphore_wait(barrier, 22)

            ring_copy(0).start()
            ring_copy(1).start()
            continue

        def send_in(k, _):
            in_copy(g, k).start()
            return 0

        lax.fori_loop(1, 16, send_in, 0)
        recv[g, pl.ds(me, 1)] = spectra[g, pl.ds(me, 1)]
        if g == 1:
            send_first(3)
    perm[...] = lane_swap()
    arrive(1)
    forward_first()
    arrive(2)
    degree = (x * 2 + core) * 64 + lax.broadcasted_iota(jnp.int32, (64, 512), 0)
    loads[1].wait()
    loads[2].wait()
    for odd in range(2):
        entry_rows = order_rows(me, odd)
        for k in range(ORD):
            n = odd * ORD + k
            first, second = legendre[n].astype(F32), legendre[16 + n].astype(F32)
            entry = jnp.broadcast_to(
                jnp.concatenate([entry_rows[k : k + 1, :]] * 4, axis=1), (64, 512))
            swap, low = entry >= 1024, entry % 1024
            leg[n] = jnp.where(degree >= low, jnp.where(swap, second, first), 0.0).astype(BF)
            leg[16 + n] = jnp.where(degree >= 511 - low, jnp.where(swap, first, second), 0.0).astype(BF)
    far_first()
    arrive_first(3)
    forward(1)
    arrive(3)
    arrive_first(0)
    arrive_first(1)
    arrive_first(2)
    forward_far(1)
    middle(0)
    forward(2)
    add_pair(0)
    middle(1)
    forward(3)
    forward_far(2)
    add_pair(1)
    middle(2)
    forward_far(3)
    add_far(0)
    add_pair(2)
    middle(3)
    add_far(1)
    add_pair(3)
    depart(0)
    add_far(2)
    last_arrived(0)
    last_far_copy(0).start()
    last_far_copy(1).start()
    depart(1)

    def arrived(g):
        def wait(k, _):
            out_copy(g, k).wait_recv()
            return 0

        lax.fori_loop(1, 16, wait, 0)

    def transform(first, count, n):
        cols = pl.ds(pl.multiple_of(n * 128, 128), 128)
        value = out[first : first + count, :, :, cols].reshape(count * 256, 128)
        return lax.dot_general(
            value, table[first * 256 : (first + count) * 256, :], (((0,), (0,)), ((), ())),
            preferred_element_type=F32)

    last_add(0)
    last_add(1)
    depart(2)
    arrived(0)
    arrived(1)

    def partial(n, _):
        synth[pl.ds(pl.multiple_of(n * 128, 128), 128), :] = transform(0, 2, n)
        return 0

    lax.fori_loop(0, 4, partial, 0)
    for n in range(3, 6):
        loads[n].wait()
    last_arrived(3)
    arrived(2)

    def partial2(n, _):
        synth[pl.ds(pl.multiple_of(n * 128, 128), 128), :] += transform(2, 1, n)
        return 0

    lax.fori_loop(0, 4, partial2, 0)
    for way in range(2):
        last_line_copy(way).wait_recv()

    def total(j, _):
        out[3, j] = (last[3, j].astype(F32) + last_fin[0, j].astype(F32)
                     + last_fin[1, j].astype(F32)).astype(BF)
        return 0

    lax.fori_loop(0, 16, total, 0)

    def synthesis(n, _):
        block = synth[pl.ds(pl.multiple_of(n * 128, 128), 128), :] + transform(3, 1, n)
        for t in range(4):
            for q in range(8):
                split[pl.ds(q * 512 + n * 4 + t, 32, stride=16), :] = (
                    block[t * 32 : (t + 1) * 32, q * 128 : (q + 1) * 128])
        return 0

    lax.fori_loop(0, 4, synthesis, 0)

    def combine(n, totals):
        r8 = pl.ds(pl.multiple_of(n * 8, 8), 8)
        nn, dp, rp, pp = totals
        for q in range(8):
            cols = slice(q * 128, (q + 1) * 128)
            d, r = direction[r8, cols], residual[r8, cols]
            p = split[pl.ds(pl.multiple_of(q * 512 + n * 8, 8), 8), :] + noise[r8, cols] * d
            product[r8, cols] = p
            nn, dp, rp, pp = nn + r * r, dp + d * p, rp + r * p, pp + p * p
        return nn, dp, rp, pp

    zero = jnp.zeros((8, 128), F32)
    totals = lax.fori_loop(0, 64, combine, (zero, zero, zero, zero), unroll=2)
    for k in range(4):
        stage[0, 2 * k : 2 * k + 2, :] = jnp.broadcast_to(
            jnp.sum(totals[k], axis=0, keepdims=True), (2, 128))
    for k in range(1, 8):
        sum_copy(k).start()
    line[pl.ds(x * 2 + core, 1)] = stage[0:1]
    for k in range(1, 8):
        sum_copy(k).wait_recv()
    stage[1] = jnp.sum(line[...], axis=0)
    for k in range(1, 16):
        all_copy(k).start()
    plane[pl.ds(me, 1)] = stage[1:2]
    for k in range(1, 16):
        all_copy(k).wait_recv()
    sums[...] = jnp.sum(plane[...], axis=0)
    for k in range(1, 8):
        sum_copy(k).wait_send()
    for k in range(1, 16):
        all_copy(k).wait_send()
    for g in range(GROUPS):
        for n in range(4):
            pair_copy(g, n).wait_send()
        for way in range(2):
            if g == 0:
                ring_copy(way).wait_send()
                ring_forward(way).wait_send()
            else:
                own_copy(g, way).wait_send()
                fwd_copy(g, way).wait_send()
            if g == GROUPS - 1:
                last_far_copy(way).wait_send()
                last_line_copy(way).wait_send()
            else:
                far_copy(g, way).wait_send()
                line_copy(g, way).wait_send()
        for slot in range(4 if g == 0 else 5):
            (dup_first(slot) if g == 0 else dup_copy(g, slot)).wait_send()

    def finish(k, _):
        for g in range(1, GROUPS):
            in_copy(g, k).wait_send()
            out_copy(g - 1, k).wait_send()
        for n in range(4):
            in_first(n, k).wait_send()
            out_last(n, k).wait_send()
        return 0

    lax.fori_loop(1, 16, finish, 0)


def step_stage(orders, direction, residual, solution, noise, legendre, temporal):
    dma = pltpu.SemaphoreType.DMA
    two, four, five, blk = dma((GROUPS, 2)), dma((GROUPS, 4)), dma((GROUPS, 5)), dma((GROUPS + 3, 16))
    grid = pltpu.VMEM((512, 1024), F32)
    hbm = pl.BlockSpec(memory_space=pl.ANY)
    shape = jax.ShapeDtypeStruct((512, 1024), F32)
    return pl.pallas_call(
        step_kernel,
        out_shape=(shape, jax.ShapeDtypeStruct((8, 128), F32), shape, shape, shape),
        in_specs=[pl.BlockSpec(memory_space=pltpu.SMEM)] + [hbm] * 6,
        out_specs=(VM,) * 5,
        scratch_shapes=[
            grid,
            pltpu.VMEM((32, 64, 512), BF),
            pltpu.VMEM((64, 128, 128), F32),
            dma((6,)),
            pltpu.VMEM((4096, 128), F32),
            pltpu.VMEM((512, 1024), BF),
            pltpu.VMEM((1024, 1024), BF),
            pltpu.VMEM((GROUPS, 16, 2 * ORD, 512), BF),
            pltpu.VMEM((3, 16, 2 * ORD, 512), BF),
            pltpu.VMEM((32, 2, 128, 512), BF),
            pltpu.VMEM((32, 2, 128, 512), BF),
            pltpu.VMEM((32, 64, 512), BF),
            pltpu.VMEM((GROUPS + 3, 16, 2 * ORD, 512), BF),
            pltpu.VMEM((GROUPS + 3, 16, 2 * ORD, 512), BF),
            pltpu.VMEM((1024, 128), F32),
            pltpu.VMEM((512, 512), BF),
            pltpu.VMEM((2 * ORD * 64, 128), F32),
            pltpu.VMEM((2 * ORD * 64, 128), F32),
            pltpu.VMEM((GROUPS, 4, ORD, 2, 16, 512), BF),
            pltpu.VMEM((3, 2, ORD // 2, 2, 16, 512), BF),
            pltpu.VMEM((3, 2, ORD, 2, 16, 512), BF),
            pltpu.VMEM((2, 8, 2 * ORD, 512), BF),
            pltpu.VMEM((2, 16, 2 * ORD, 512), BF),
            pltpu.VMEM((4, 16, 2 * ORD, 512), BF),
            pltpu.VMEM((GROUPS, 16, 2 * ORD, 512), BF),
            grid,
            pltpu.VMEM((2, 8, 128), F32),
            pltpu.VMEM((8, 8, 128), F32),
            pltpu.VMEM((16, 8, 128), F32),
            blk, blk, two, two, five, two, two, five, four, four, two, two, two, two, blk, blk,
            dma((8,)), dma((8,)), dma((16,)), dma((16,)),
        ],
        compiler_params=pltpu.CompilerParams(
            collective_id=0, has_side_effects=True, vmem_limit_bytes=58 * 1024 * 1024),
        name="step_stage",
    )(orders, direction, residual, solution, noise, legendre, temporal)


def update_kernel(sums, solution, residual, direction, product, solution_new, residual_new,
                  direction_new, stage, sems):
    def total(k):
        return jnp.sum(sums[2 * k : 2 * k + 1, :], axis=1, keepdims=True)

    norm_now, curvature, cross, square = total(0), total(1), total(2), total(3)
    step = norm_now / curvature
    norm_next = norm_now - 2.0 * step * cross + step * step * square
    ratio = norm_next / norm_now
    outs = (solution_new, residual_new, direction_new)

    def copy(n, k):
        rows = pl.ds(pl.multiple_of(n * 64, 64), 64)
        return pltpu.make_async_copy(stage.at[k, rows, :], outs[k].at[rows, :], sems.at[n, k])

    def block(n, _):
        rows = pl.ds(pl.multiple_of(n * 64, 64), 64)
        d = direction[rows, :]
        r = residual[rows, :] - step * product[rows, :]
        stage[0, rows, :] = solution[rows, :] + step * d
        stage[1, rows, :] = r
        stage[2, rows, :] = r + ratio * d
        for k in range(3):
            copy(n, k).start()
        return 0

    lax.fori_loop(0, 8, block, 0)

    def drain(n, _):
        for k in range(3):
            copy(n, k).wait()
        return 0

    lax.fori_loop(0, 8, drain, 0)


def update(sums, solution, residual, direction, product):
    shape = jax.ShapeDtypeStruct((512, 1024), F32)
    hbm = pl.BlockSpec(memory_space=pl.ANY)
    return pl.pallas_call(
        update_kernel,
        out_shape=(shape, shape, shape),
        in_specs=[VM] * 5,
        out_specs=(hbm, hbm, hbm),
        scratch_shapes=[pltpu.VMEM((3, 512, 1024), F32), pltpu.SemaphoreType.DMA((8, 3))],
        compiler_params=pltpu.CompilerParams(vmem_limit_bytes=24 * 1024 * 1024),
        name="update",
    )(sums, solution, residual, direction, product)


def body(solution, residual, direction, noise_var, legendre, temporal, order_table):
    shape = direction.shape
    flat = lambda v: v.reshape(512, 1024)
    product, sums, direction, residual, solution = step_stage(
        order_table, flat(direction), flat(residual), flat(solution), flat(noise_var), legendre,
        temporal)
    outs = update(sums, solution, residual, direction, product)
    return tuple(o.reshape(shape) for o in outs)


def solution(mesh):
    torus = Mesh(mesh.devices.reshape(4, 4, 4, 2), ("blk_0", "blk_1", "tm_0", "tm_1"))
    return jax.shard_map(
        body,
        mesh=torus,
        in_specs=(
            P(BLK, TM, None),
            P(BLK, TM, None),
            P(BLK, TM, None),
            P(BLK, TM, None),
            P(BLK, TM, None),
            P(TM, None, None),
            P(),
        ),
        out_specs=(P(BLK, TM, None), P(BLK, TM, None), P(BLK, TM, None)),
        check_vma=False,
    )
```

```python
import math

import jax
import jax.numpy as jnp
from jax import lax
from jax.experimental import pallas as pl
from jax.experimental.pallas import tpu as pltpu
from jax.sharding import Mesh
from jax.sharding import PartitionSpec as P

BLK = ("blk_0", "blk_1")
TM = ("tm_0", "tm_1")
BLK_TM = ("blk_0", "blk_1", "tm_0", "tm_1")
BF = jnp.bfloat16
F32 = jnp.float32
MESH = pl.DeviceIdType.MESH
GROUPS = 4
ORD = 8
LAST = 2
SLOT = (0, 1, None, 2)
FIRST = (4, 5, 6, 0)
VM = pl.BlockSpec(memory_space=pltpu.VMEM)


def unit_circle(phase):
    quadrant = (phase + 128) // 256
    x = (phase - quadrant * 256).astype(F32) * (2.0 * math.pi / 1024)
    x2 = x * x
    s = x * (1.0 + x2 * (-1.0 / 6 + x2 * (1.0 / 120 + x2 * (-1.0 / 5040 + x2 / 362880))))
    c = 1.0 + x2 * (-0.5 + x2 * (1.0 / 24 + x2 * (-1.0 / 720 + x2 / 40320)))
    odd = quadrant % 2 == 1
    cos = jnp.where(odd, s, c)
    sin = jnp.where(odd, c, s)
    cos = jnp.where((quadrant == 1) | (quadrant == 2), -cos, cos)
    sin = jnp.where((quadrant == 2) | (quadrant == 3), -sin, sin)
    return cos, sin


def lane_swap():
    row = lax.broadcasted_iota(jnp.int32, (512, 512), 0)
    col = lax.broadcasted_iota(jnp.int32, (512, 512), 1)
    moved = (row // 32 % 4) * 128 + (row // 128) * 32 + row % 32
    return (col == moved).astype(F32).astype(BF)


def step_kernel(orders_in, direction_in, residual_in, solution_in, noise_in, legendre_in, temporal_in,
                product, sums, direction, residual, solution, orders, noise, legendre, temporal, load,
                split, rows, table, spectra, ring, full, leg, recv, blocks, mid, perm, coef, mixed, acc,
                far_in, fin_in, last_far, last_fin, last, out, synth, stage, line, plane, in_send, in_recv, own_send, fwd_send, dup_send,
                own_recv, fwd_recv, dup_recv, pair_send, pair_recv, far_send, far_recv, line_send,
                line_recv, out_send, out_recv, sum_send, sum_recv, all_send, all_recv):
    loads = [
        pltpu.make_async_copy(src, dst, load.at[n])
        for n, (src, dst) in enumerate((
            (direction_in, direction), (legendre_in, legendre), (temporal_in, temporal),
            (residual_in, residual), (noise_in, noise), (solution_in, solution),
            (orders_in, orders)))
    ]
    for copy in loads:
        copy.start()
    y, z = lax.axis_index("blk_0"), lax.axis_index("blk_1")
    x, core = lax.axis_index("tm_0"), lax.axis_index("tm_1")
    me = y * 4 + z
    right, left, far = (x + 1) % 4, (x + 3) % 4, (x + 2) % 4
    half = ORD // 2
    barrier = pltpu.get_barrier_semaphore()

    def greet(k, _):
        pl.semaphore_signal(
            barrier, inc=1, device_id={"blk_0": (y + k // 4) % 4, "blk_1": (z + k % 4) % 4},
            device_id_type=MESH,
        )
        return 0

    lax.fori_loop(1, 16, greet, 0)

    def in_line(k):
        return {"tm_0": (x + k // 2) % 4, "tm_1": (core + k) % 2}

    def greet_line(k, _):
        pl.semaphore_signal(barrier, inc=1, device_id=in_line(k), device_id_type=MESH)
        return 0

    lax.fori_loop(1, 8, greet_line, 0)
    side = ({"tm_0": right}, {"tm_0": left})
    peer = {"tm_1": 1 - core}

    def remote(src, dst, send, recv_sem, device):
        return pltpu.make_async_remote_copy(
            src_ref=src, dst_ref=dst, send_sem=send, recv_sem=recv_sem, device_id=device,
            device_id_type=MESH)

    def in_copy(g, k):
        ty, tz = (y + k // 4) % 4, (z + k % 4) % 4
        return remote(spectra.at[g, ty * 4 + tz], recv.at[g, me], in_send.at[g, k],
                      in_recv.at[g, k], {"blk_0": ty, "blk_1": tz})

    def in_first(slot, k):
        ty, tz = (y + k // 4) % 4, (z + k % 4) % 4
        dest = ty * 4 + tz
        src = spectra.at[0, dest] if slot == 3 else ring.at[slot, dest]
        return remote(src, recv.at[FIRST[slot], me], in_send.at[FIRST[slot], k],
                      in_recv.at[FIRST[slot], k], {"blk_0": ty, "blk_1": tz})

    def ring_copy(way):
        return remote(spectra.at[0], ring.at[way], own_send.at[0, way], own_recv.at[0, way], side[way])

    def ring_forward(way):
        return remote(ring.at[way, pl.ds(way * 8, 8)], ring.at[2, pl.ds(way * 8, 8)],
                      fwd_send.at[0, way], fwd_recv.at[0, way], side[way])

    def dup_first(slot):
        ref = piece(0, (left, right, far, x)[slot], 0, ORD)
        return remote(ref, ref, dup_send.at[0, slot], dup_recv.at[0, slot], peer)

    def out_last(n, k):
        ty, tz = (y + k // 4) % 4, (z + k % 4) % 4
        return remote(blocks.at[3 + n, ty * 4 + tz], last.at[n, me], out_send.at[3 + n, k],
                      out_recv.at[3 + n, k], {"blk_0": ty, "blk_1": tz})

    def last_far_copy(way):
        return remote(last.at[0, pl.ds(way * 8, 8)], last_far.at[way], far_send.at[LAST, way],
                      far_recv.at[LAST, way], side[way])

    def last_line_copy(way):
        return remote(last.at[1 + way], last_fin.at[way], line_send.at[LAST, way],
                      line_recv.at[LAST, way], side[way])

    def out_copy(g, k):
        ty, tz = (y + k // 4) % 4, (z + k % 4) % 4
        return remote(blocks.at[SLOT[g], ty * 4 + tz], out.at[g, me], out_send.at[SLOT[g], k],
                      out_recv.at[SLOT[g], k], {"blk_0": ty, "blk_1": tz})

    def hours(plane, who):
        return pl.ds(pl.multiple_of((plane * 2 + who) * 16, 16), 16)

    def piece(g, plane, first, count):
        return full.at[pl.ds(g * ORD + first, count), :, hours(plane, core), :]

    def own_copy(g, way):
        ref = piece(g, x, 0, ORD)
        return remote(ref, ref, own_send.at[g, way], own_recv.at[g, way], side[way])

    def fwd_copy(g, way):
        ref = piece(g, left if way == 0 else right, way * half, half)
        return remote(ref, ref, fwd_send.at[g, way], fwd_recv.at[g, way], side[way])

    def dup_copy(g, slot):
        plane, first, count = (
            (x, 0, ORD), (left, 0, ORD), (right, 0, ORD), (far, 0, half), (far, half, half))[slot]
        ref = piece(g, plane, first, count)
        return remote(ref, ref, dup_send.at[g, slot], dup_recv.at[g, slot], peer)

    planes = (far, right, left, x)

    def pair_copy(g, n):
        return remote(full.at[pl.ds(g * ORD, ORD), :, hours(planes[n], 1 - core), :], acc.at[g, n],
                      pair_send.at[g, n], pair_recv.at[g, n], peer)

    def far_copy(g, way):
        return remote(acc.at[g, 0, pl.ds(way * half, half)], far_in.at[SLOT[g], way],
                      far_send.at[g, way], far_recv.at[g, way], side[way])

    def line_copy(g, way):
        return remote(acc.at[g, 1 + way], fin_in.at[SLOT[g], way], line_send.at[g, way],
                      line_recv.at[g, way], side[way])

    def regroup_in(n, g, plane_of):
        blocks_in = []
        for sq in range(4):
            for tq in range(4):
                blocks_in.append(jnp.concatenate(
                    [recv[n, sq * 4 + s, :, tq * 128 : (tq + 1) * 128] for s in range(4)], axis=1))
        moved = jnp.dot(jnp.concatenate(blocks_in, axis=0), perm[...], preferred_element_type=F32)
        for sq in range(4):
            for tq in range(4):
                n0 = (sq * 4 + tq) * 16
                for t in range(4):
                    m = sq * 256 + (tq * 4 + t) * 16
                    mid[m : m + 16, :] = moved[n0 : n0 + 16, t * 128 : (t + 1) * 128]
        for c in range(2):
            for i in range(ORD):
                for sq in range(4):
                    full[g * ORD + i, c, hours(plane_of, core), sq * 128 : (sq + 1) * 128] = (
                        mid[pl.ds(sq * 256 + c * ORD + i, 16, stride=16), :].astype(BF))

    def arrive(g):
        def wait(k, _):
            in_copy(g, k).wait_recv()
            return 0

        lax.fori_loop(1, 16, wait, 0)
        regroup_in(g, g, x)
        own_copy(g, 0).start()
        own_copy(g, 1).start()
        dup_copy(g, 0).start()

    def send_first(slot):
        def send(k, _):
            in_first(slot, k).start()
            return 0

        lax.fori_loop(1, 16, send, 0)
        src = spectra if slot == 3 else ring
        recv[FIRST[slot], pl.ds(me, 1)] = src[0 if slot == 3 else slot, pl.ds(me, 1)]

    def arrive_first(slot):
        def wait(k, _):
            in_first(slot, k).wait_recv()
            return 0

        lax.fori_loop(1, 16, wait, 0)
        regroup_in(FIRST[slot], 0, (left, right, far, x)[slot])
        dup_first(slot).start()

    def forward_first():
        for way in range(2):
            ring_copy(way).wait_recv()
            ring_forward(way).start()
        for way in range(2):
            send_first(way)

    def far_first():
        for way in range(2):
            ring_forward(way).wait_recv()
        send_first(2)

    def forward(g):
        for way in range(2):
            own_copy(g, way).wait_recv()
            fwd_copy(g, way).start()
            dup_copy(g, 1 + way).start()

    def forward_far(g):
        for way in range(2):
            fwd_copy(g, way).wait_recv()
            dup_copy(g, 3 + way).start()

    def middle(g):
        if g == 0:
            for slot in range(4):
                dup_first(slot).wait_recv()
        else:
            for slot in range(5):
                dup_copy(g, slot).wait_recv()

        def analyse(i, _):
            value = lax.dot_general(
                leg[g * ORD + i], full[g * ORD + i].reshape(256, 512), (((1,), (1,)), ((), ())),
                preferred_element_type=F32)
            row = pl.multiple_of(i * 64, 64)
            coef[pl.ds(row, 64), :] = value[:, :128]
            coef[pl.ds(ORD * 64 + row, 64), :] = value[:, 128:]
            return 0

        lax.fori_loop(0, ORD, analyse, 0, unroll=2)

        for slot in range(4 if g == 0 else 5):
            (dup_first(slot) if g == 0 else dup_copy(g, slot)).wait_send()
        if g > 0:
            for way in range(2):
                own_copy(g, way).wait_send()
                fwd_copy(g, way).wait_send()

        def mix(n, _):
            for k in range(16):
                l = n * 16 + k
                rows = jnp.concatenate(
                    [coef[pl.ds(c * ORD * 64 + l, ORD, stride=64), :] for c in range(2)], axis=0)
                mixed[pl.ds(pl.multiple_of(l * 16, 16), 16), :] = jnp.dot(
                    rows.astype(BF), temporal[l].astype(BF), preferred_element_type=F32)
            return 0

        lax.fori_loop(0, 4, mix, 0)

        def synthesise(i, _):
            rows = jnp.concatenate(
                [mixed[pl.ds(c * ORD + i, 64, stride=16), :] for c in range(2)], axis=1)
            value = lax.dot_general(
                rows.astype(BF), leg[g * ORD + i], (((0,), (0,)), ((), ())),
                preferred_element_type=F32)
            full[g * ORD + i] = value.astype(BF).reshape(2, 128, 512)
            return 0

        lax.fori_loop(0, ORD, synthesise, 0, unroll=2)
        for n in range(4):
            pair_copy(g, n).start()

    def add_pair(g):
        for n in range(4):
            pair_copy(g, n).wait_recv()

            def step(i, _):
                own = full[g * ORD + i, :, hours(planes[n], core), :]
                acc[g, n, i] = (acc[g, n, i].astype(F32) + own.astype(F32)).astype(BF)
                return 0

            lax.fori_loop(0, ORD, step, 0)
            if g == LAST:
                regroup_out(3 + n, lambda i, c: acc[g, n, i, c].astype(F32))

                def send(k, _):
                    out_last(n, k).start()
                    return 0

                lax.fori_loop(1, 16, send, 0)
                last[n, pl.ds(me, 1)] = blocks[3 + n, pl.ds(me, 1)]
            elif n == 0:
                far_copy(g, 0).start()
                far_copy(g, 1).start()

    def add_far(g):
        for way in range(2):
            far_copy(g, way).wait_recv()

            def step(i, _):
                acc[g, 1 + way, way * half + i] = (
                    acc[g, 1 + way, way * half + i].astype(F32) + far_in[SLOT[g], way, i].astype(F32)
                ).astype(BF)
                return 0

            lax.fori_loop(0, half, step, 0)
            line_copy(g, way).start()

    def regroup_out(n, value):
        for i in range(ORD):
            for c in range(2):
                total = value(i, c)
                for sq in range(4):
                    mid[pl.ds(sq * 256 + c * ORD + i, 16, stride=16), :] = (
                        total[:, sq * 128 : (sq + 1) * 128])
        rows_out = []
        for sq in range(4):
            for tq in range(4):
                m = sq * 256 + tq * 64
                rows_out.append(jnp.concatenate(
                    [mid[m + t * 16 : m + (t + 1) * 16, :].astype(BF) for t in range(4)], axis=1))
        moved = jnp.dot(
            jnp.concatenate(rows_out, axis=0), perm[...], preferred_element_type=F32).astype(BF)
        for sq in range(4):
            for tq in range(4):
                n0 = (sq * 4 + tq) * 16
                for s in range(4):
                    blocks[n, sq * 4 + s, :, tq * 128 : (tq + 1) * 128] = (
                        moved[n0 : n0 + 16, s * 128 : (s + 1) * 128])

    def depart(g):
        line_copy(g, 0).wait_recv()
        line_copy(g, 1).wait_recv()
        regroup_out(SLOT[g], lambda i, c: acc[g, 3, i, c].astype(F32)
                    + fin_in[SLOT[g], 0, i, c].astype(F32) + fin_in[SLOT[g], 1, i, c].astype(F32))

        def send(k, _):
            out_copy(g, k).start()
            return 0

        lax.fori_loop(1, 16, send, 0)
        out[g, pl.ds(me, 1)] = blocks[SLOT[g], pl.ds(me, 1)]

    def last_arrived(n):
        def wait(k, _):
            out_last(n, k).wait_recv()
            return 0

        lax.fori_loop(1, 16, wait, 0)

    def last_add(way):
        last_arrived(1 + way)
        last_far_copy(way).wait_recv()

        def step(j, _):
            last[1 + way, way * 8 + j] = (
                last[1 + way, way * 8 + j].astype(F32) + last_far[way, j].astype(F32)).astype(BF)
            return 0

        lax.fori_loop(0, 8, step, 0)
        last_line_copy(way).start()

    def sum_copy(k):
        return remote(stage.at[0], line.at[x * 2 + core], sum_send.at[k], sum_recv.at[k], in_line(k))

    def all_copy(k):
        return remote(stage.at[1], plane.at[me], all_send.at[k], all_recv.at[k],
                      {"blk_0": (y + k // 4) % 4, "blk_1": (z + k % 4) % 4})

    def order_rows(block, odd):
        sub = lax.broadcasted_iota(jnp.int32, (ORD, 128), 0)
        value = jnp.zeros((ORD, 128), jnp.int32)
        for i in range(ORD):
            value = jnp.where(sub == i, orders[block * 32 + odd * ORD + i], value)
        low = jnp.minimum(value, 511 - value)
        return low + jnp.where(value == low, 0, 1024)

    loads[6].wait()
    lane = lax.broadcasted_iota(jnp.int32, (4 * ORD, 128), 1)
    scale = 1.0 / math.sqrt(512.0)

    def fill_group(g):
        def fill(n, _):
            m = jnp.concatenate([order_rows(n * 4 + k, g % 2) for k in range(4)], axis=0) % 1024
            m = m if g < 2 else 511 - m
            cos, sin = unit_circle((m * lane) % 1024)
            turn_c, turn_s = unit_circle((m * 128) % 1024)
            cos, sin = cos * scale, sin * scale
            for q in range(8):
                both = jnp.concatenate(
                    [v[k * ORD : (k + 1) * ORD] for k in range(4) for v in (cos, sin)], axis=0)
                table[pl.ds(pl.multiple_of(g * 256 + n * 64, 64), 64), q * 128 : (q + 1) * 128] = (
                    both.astype(BF))
                cos, sin = cos * turn_c - sin * turn_s, sin * turn_c + cos * turn_s
            return 0

        lax.fori_loop(0, 4, fill, 0)

    def send_in(g):
        def send(k, _):
            in_copy(g, k).start()
            return 0

        lax.fori_loop(1, 16, send, 0)
        recv[g, pl.ds(me, 1)] = spectra[g, pl.ds(me, 1)]

    fill_group(0)
    fill_group(1)
    loads[0].wait()
    lat, time = 32, 16
    for q in range(8):
        split[q * 512 : (q + 1) * 512, :] = direction[:, q * 128 : (q + 1) * 128]

    def gather(t, _):
        for q in range(8):
            rows[pl.ds(pl.multiple_of(t * lat, lat), lat), q * 128 : (q + 1) * 128] = split[
                pl.ds(q * 512 + t, lat, stride=time), :
            ].astype(BF)
        return 0

    lax.fori_loop(0, time, gather, 0, unroll=2)
    for g in range(GROUPS):
        if g >= 2:
            fill_group(g)
        spectra[g] = lax.dot_general(
            table[g * 256 : (g + 1) * 256, :], rows[...], (((1,), (1,)), ((), ())),
            preferred_element_type=F32).astype(BF).reshape(16, 2 * ORD, 512)
        if g == 0:
            pl.semaphore_wait(barrier, 22)

            ring_copy(0).start()
            ring_copy(1).start()
            continue

        if g < 3:
            send_in(g)
        if g == 1:
            send_first(3)
    perm[...] = lane_swap()
    degree = (x * 2 + core) * 64 + lax.broadcasted_iota(jnp.int32, (64, 512), 0)
    loads[1].wait()
    loads[2].wait()
    for odd in range(2):
        entry_rows = order_rows(me, odd)
        for k in range(ORD):
            n = odd * ORD + k
            first, second = legendre[n].astype(F32), legendre[16 + n].astype(F32)
            entry = jnp.broadcast_to(
                jnp.concatenate([entry_rows[k : k + 1, :]] * 4, axis=1), (64, 512))
            swap, low = entry >= 1024, entry % 1024
            leg[n] = jnp.where(degree >= low, jnp.where(swap, second, first), 0.0).astype(BF)
            leg[16 + n] = jnp.where(degree >= 511 - low, jnp.where(swap, first, second), 0.0).astype(BF)
    forward_first()
    arrive(1)
    far_first()
    send_in(3)
    arrive(2)
    arrive_first(3)
    arrive_first(0)
    arrive_first(1)
    forward(1)
    arrive_first(2)
    arrive(3)
    forward(2)
    middle(0)
    forward_far(1)
    add_pair(0)
    middle(1)
    forward(3)
    forward_far(2)
    add_pair(1)
    add_far(0)
    middle(2)
    forward_far(3)
    add_far(1)
    add_pair(2)
    middle(3)
    add_pair(3)
    depart(0)
    last_arrived(0)
    last_far_copy(0).start()
    last_far_copy(1).start()
    add_far(3)
    depart(1)
    last_add(0)
    last_add(1)

    def arrived(g):
        def wait(k, _):
            out_copy(g, k).wait_recv()
            return 0

        lax.fori_loop(1, 16, wait, 0)

    def transform(first, count, n):
        cols = pl.ds(pl.multiple_of(n * 128, 128), 128)
        value = out[first : first + count, :, :, cols].reshape(count * 256, 128)
        return lax.dot_general(
            value, table[first * 256 : (first + count) * 256, :], (((0,), (0,)), ((), ())),
            preferred_element_type=F32)

    arrived(0)
    arrived(1)

    def partial(n, _):
        synth[pl.ds(pl.multiple_of(n * 128, 128), 128), :] = transform(0, 2, n)
        return 0

    lax.fori_loop(0, 4, partial, 0)
    depart(3)
    for n in range(3, 6):
        loads[n].wait()
    last_arrived(3)
    for way in range(2):
        last_line_copy(way).wait_recv()

    def total(j, _):
        out[LAST, j] = (last[3, j].astype(F32) + last_fin[0, j].astype(F32)
                        + last_fin[1, j].astype(F32)).astype(BF)
        return 0

    lax.fori_loop(0, 16, total, 0)

    def partial2(n, _):
        synth[pl.ds(pl.multiple_of(n * 128, 128), 128), :] += transform(2, 1, n)
        return 0

    lax.fori_loop(0, 4, partial2, 0)
    arrived(3)

    def synthesis(n, _):
        block = synth[pl.ds(pl.multiple_of(n * 128, 128), 128), :] + transform(3, 1, n)
        for t in range(4):
            for q in range(8):
                split[pl.ds(q * 512 + n * 4 + t, 32, stride=16), :] = (
                    block[t * 32 : (t + 1) * 32, q * 128 : (q + 1) * 128])
        return 0

    lax.fori_loop(0, 4, synthesis, 0)

    def combine(n, totals):
        r8 = pl.ds(pl.multiple_of(n * 8, 8), 8)
        nn, dp, rp, pp = totals
        for q in range(8):
            cols = slice(q * 128, (q + 1) * 128)
            d, r = direction[r8, cols], residual[r8, cols]
            p = split[pl.ds(pl.multiple_of(q * 512 + n * 8, 8), 8), :] + noise[r8, cols] * d
            product[r8, cols] = p
            nn, dp, rp, pp = nn + r * r, dp + d * p, rp + r * p, pp + p * p
        return nn, dp, rp, pp

    zero = jnp.zeros((8, 128), F32)
    totals = lax.fori_loop(0, 64, combine, (zero, zero, zero, zero), unroll=2)
    for k in range(4):
        stage[0, 2 * k : 2 * k + 2, :] = jnp.broadcast_to(
            jnp.sum(totals[k], axis=0, keepdims=True), (2, 128))
    for k in range(1, 8):
        sum_copy(k).start()
    line[pl.ds(x * 2 + core, 1)] = stage[0:1]
    for k in range(1, 8):
        sum_copy(k).wait_recv()
    stage[1] = jnp.sum(line[...], axis=0)
    for k in range(1, 16):
        all_copy(k).start()
    plane[pl.ds(me, 1)] = stage[1:2]
    for k in range(1, 16):
        all_copy(k).wait_recv()
    sums[...] = jnp.sum(plane[...], axis=0)
    for k in range(1, 8):
        sum_copy(k).wait_send()
    for k in range(1, 16):
        all_copy(k).wait_send()
    for g in range(GROUPS):
        for n in range(4):
            pair_copy(g, n).wait_send()
        for way in range(2):
            if g == 0:
                ring_copy(way).wait_send()
                ring_forward(way).wait_send()
            if g == LAST:
                last_far_copy(way).wait_send()
                last_line_copy(way).wait_send()
            else:
                far_copy(g, way).wait_send()
                line_copy(g, way).wait_send()

    def finish(k, _):
        for g in range(1, GROUPS):
            in_copy(g, k).wait_send()
            if g - 1 != LAST:
                out_copy(g - 1, k).wait_send()
        out_copy(3, k).wait_send()
        for n in range(4):
            in_first(n, k).wait_send()
            out_last(n, k).wait_send()
        return 0

    lax.fori_loop(1, 16, finish, 0)


def step_stage(orders, direction, residual, solution, noise, legendre, temporal):
    dma = pltpu.SemaphoreType.DMA
    two, four, five, blk = dma((GROUPS, 2)), dma((GROUPS, 4)), dma((GROUPS, 5)), dma((GROUPS + 3, 16))
    grid = pltpu.VMEM((512, 1024), F32)
    hbm = pl.BlockSpec(memory_space=pl.ANY)
    shape = jax.ShapeDtypeStruct((512, 1024), F32)
    return pl.pallas_call(
        step_kernel,
        out_shape=(shape, jax.ShapeDtypeStruct((8, 128), F32), shape, shape, shape),
        in_specs=[pl.BlockSpec(memory_space=pltpu.HBM)] + [hbm] * 6,
        out_specs=(VM,) * 5,
        scratch_shapes=[
            pltpu.SMEM((512,), jnp.int32),
            grid,
            pltpu.VMEM((32, 64, 512), BF),
            pltpu.VMEM((64, 128, 128), F32),
            dma((7,)),
            pltpu.VMEM((4096, 128), F32),
            pltpu.VMEM((512, 1024), BF),
            pltpu.VMEM((1024, 1024), BF),
            pltpu.VMEM((GROUPS, 16, 2 * ORD, 512), BF),
            pltpu.VMEM((3, 16, 2 * ORD, 512), BF),
            pltpu.VMEM((32, 2, 128, 512), BF),
            pltpu.VMEM((32, 64, 512), BF),
            pltpu.VMEM((GROUPS + 3, 16, 2 * ORD, 512), BF),
            pltpu.VMEM((GROUPS + 3, 16, 2 * ORD, 512), BF),
            pltpu.VMEM((1024, 128), F32),
            pltpu.VMEM((512, 512), BF),
            pltpu.VMEM((2 * ORD * 64, 128), F32),
            pltpu.VMEM((2 * ORD * 64, 128), F32),
            pltpu.VMEM((GROUPS, 4, ORD, 2, 16, 512), BF),
            pltpu.VMEM((3, 2, ORD // 2, 2, 16, 512), BF),
            pltpu.VMEM((3, 2, ORD, 2, 16, 512), BF),
            pltpu.VMEM((2, 8, 2 * ORD, 512), BF),
            pltpu.VMEM((2, 16, 2 * ORD, 512), BF),
            pltpu.VMEM((4, 16, 2 * ORD, 512), BF),
            pltpu.VMEM((GROUPS, 16, 2 * ORD, 512), BF),
            grid,
            pltpu.VMEM((2, 8, 128), F32),
            pltpu.VMEM((8, 8, 128), F32),
            pltpu.VMEM((16, 8, 128), F32),
            blk, blk, two, two, five, two, two, five, four, four, two, two, two, two, blk, blk,
            dma((8,)), dma((8,)), dma((16,)), dma((16,)),
        ],
        compiler_params=pltpu.CompilerParams(
            collective_id=0, has_side_effects=True, vmem_limit_bytes=45 * 1024 * 1024),
        name="step_stage",
    )(orders, direction, residual, solution, noise, legendre, temporal)


def update_kernel(sums, solution, residual, direction, product, solution_new, residual_new,
                  direction_new, stage, sems):
    def total(k):
        return jnp.sum(sums[2 * k : 2 * k + 1, :], axis=1, keepdims=True)

    norm_now, curvature, cross, square = total(0), total(1), total(2), total(3)
    step = norm_now / curvature
    norm_next = norm_now - 2.0 * step * cross + step * step * square
    ratio = norm_next / norm_now
    outs = (solution_new, residual_new, direction_new)

    def copy(n, k):
        rows = pl.ds(pl.multiple_of(n * 64, 64), 64)
        return pltpu.make_async_copy(stage.at[k, rows, :], outs[k].at[rows, :], sems.at[n, k])

    def block(n, _):
        rows = pl.ds(pl.multiple_of(n * 64, 64), 64)
        d = direction[rows, :]
        r = residual[rows, :] - step * product[rows, :]
        stage[0, rows, :] = solution[rows, :] + step * d
        stage[1, rows, :] = r
        stage[2, rows, :] = r + ratio * d
        for k in range(3):
            copy(n, k).start()
        return 0

    lax.fori_loop(0, 8, block, 0)

    def drain(n, _):
        for k in range(3):
            copy(n, k).wait()
        return 0

    lax.fori_loop(0, 8, drain, 0)


def update(sums, solution, residual, direction, product):
    shape = jax.ShapeDtypeStruct((512, 1024), F32)
    hbm = pl.BlockSpec(memory_space=pl.ANY)
    return pl.pallas_call(
        update_kernel,
        out_shape=(shape, shape, shape),
        in_specs=[VM] * 5,
        out_specs=(hbm, hbm, hbm),
        scratch_shapes=[pltpu.VMEM((3, 512, 1024), F32), pltpu.SemaphoreType.DMA((8, 3))],
        compiler_params=pltpu.CompilerParams(vmem_limit_bytes=24 * 1024 * 1024),
        name="update",
    )(sums, solution, residual, direction, product)


def body(solution, residual, direction, noise_var, legendre, temporal, order_table):
    shape = direction.shape
    flat = lambda v: v.reshape(512, 1024)
    product, sums, direction, residual, solution = step_stage(
        order_table, flat(direction), flat(residual), flat(solution), flat(noise_var), legendre,
        temporal)
    outs = update(sums, solution, residual, direction, product)
    return tuple(o.reshape(shape) for o in outs)


def solution(mesh):
    torus = Mesh(mesh.devices.reshape(4, 4, 4, 2), ("blk_0", "blk_1", "tm_0", "tm_1"))
    return jax.shard_map(
        body,
        mesh=torus,
        in_specs=(
            P(BLK, TM, None),
            P(BLK, TM, None),
            P(BLK, TM, None),
            P(BLK, TM, None),
            P(BLK, TM, None),
            P(TM, None, None),
            P(),
        ),
        out_specs=(P(BLK, TM, None), P(BLK, TM, None), P(BLK, TM, None)),
        check_vma=False,
    )
```

```python
import math

import jax
import jax.numpy as jnp
from jax import lax
from jax.experimental import pallas as pl
from jax.experimental.pallas import tpu as pltpu
from jax.sharding import Mesh
from jax.sharding import PartitionSpec as P

BLK = ("blk_0", "blk_1")
TM = ("tm_0", "tm_1")
BLK_TM = ("blk_0", "blk_1", "tm_0", "tm_1")
BF = jnp.bfloat16
F32 = jnp.float32
MESH = pl.DeviceIdType.MESH
GROUPS = 4
ORD = 8
LAST = 2
SLOT = (0, 1, None, 2)
FIRST = (4, 5, 6, 0)
VM = pl.BlockSpec(memory_space=pltpu.VMEM)


def unit_circle(phase):
    quadrant = (phase + 128) // 256
    x = (phase - quadrant * 256).astype(F32) * (2.0 * math.pi / 1024)
    x2 = x * x
    s = x * (1.0 + x2 * (-1.0 / 6 + x2 * (1.0 / 120 + x2 * (-1.0 / 5040 + x2 / 362880))))
    c = 1.0 + x2 * (-0.5 + x2 * (1.0 / 24 + x2 * (-1.0 / 720 + x2 / 40320)))
    odd = quadrant % 2 == 1
    cos = jnp.where(odd, s, c)
    sin = jnp.where(odd, c, s)
    cos = jnp.where((quadrant == 1) | (quadrant == 2), -cos, cos)
    sin = jnp.where((quadrant == 2) | (quadrant == 3), -sin, sin)
    return cos, sin


def lane_swap():
    row = lax.broadcasted_iota(jnp.int32, (512, 512), 0)
    col = lax.broadcasted_iota(jnp.int32, (512, 512), 1)
    moved = (row // 32 % 4) * 128 + (row // 128) * 32 + row % 32
    return (col == moved).astype(F32).astype(BF)


def step_kernel(orders_in, direction_in, residual_in, solution_in, noise_in, legendre_in, temporal_in,
                product, sums, direction, residual, solution, orders, noise, legendre, temporal, load,
                split, rows, table, spectra, ring, full, leg, recv, blocks, mid, perm, coef, mixed, acc,
                far_in, fin_in, last_far, last_fin, last, out, synth, rhat, nhat, tot, stage, line, plane, in_send, in_recv, own_send, fwd_send, dup_send,
                own_recv, fwd_recv, dup_recv, pair_send, pair_recv, far_send, far_recv, line_send,
                line_recv, out_send, out_recv, sum_send, sum_recv, all_send, all_recv):
    loads = [
        pltpu.make_async_copy(src, dst, load.at[n])
        for n, (src, dst) in enumerate((
            (direction_in, direction), (legendre_in, legendre), (temporal_in.at[pl.ds(0, 4096)], synth),
            (residual_in, residual), (noise_in, noise), (solution_in, solution),
            (orders_in, orders), (temporal_in.at[pl.ds(4096, 4096)], split)))
    ]
    for copy in loads[:7]:
        copy.start()
    y, z = lax.axis_index("blk_0"), lax.axis_index("blk_1")
    x, core = lax.axis_index("tm_0"), lax.axis_index("tm_1")
    me = y * 4 + z
    right, left, far = (x + 1) % 4, (x + 3) % 4, (x + 2) % 4
    half = ORD // 2
    barrier = pltpu.get_barrier_semaphore()

    def greet(k, _):
        pl.semaphore_signal(
            barrier, inc=1, device_id={"blk_0": (y + k // 4) % 4, "blk_1": (z + k % 4) % 4},
            device_id_type=MESH,
        )
        return 0

    lax.fori_loop(1, 16, greet, 0)

    def in_line(k):
        return {"tm_0": (x + k // 2) % 4, "tm_1": (core + k) % 2}

    def greet_line(k, _):
        pl.semaphore_signal(barrier, inc=1, device_id=in_line(k), device_id_type=MESH)
        return 0

    lax.fori_loop(1, 8, greet_line, 0)
    side = ({"tm_0": right}, {"tm_0": left})
    peer = {"tm_1": 1 - core}

    def remote(src, dst, send, recv_sem, device):
        return pltpu.make_async_remote_copy(
            src_ref=src, dst_ref=dst, send_sem=send, recv_sem=recv_sem, device_id=device,
            device_id_type=MESH)

    def in_copy(g, k):
        ty, tz = (y + k // 4) % 4, (z + k % 4) % 4
        return remote(spectra.at[g, ty * 4 + tz], recv.at[g, me], in_send.at[g, k],
                      in_recv.at[g, k], {"blk_0": ty, "blk_1": tz})

    def in_first(slot, k):
        ty, tz = (y + k // 4) % 4, (z + k % 4) % 4
        dest = ty * 4 + tz
        src = spectra.at[0, dest] if slot == 3 else ring.at[slot, dest]
        return remote(src, recv.at[FIRST[slot], me], in_send.at[FIRST[slot], k],
                      in_recv.at[FIRST[slot], k], {"blk_0": ty, "blk_1": tz})

    def ring_copy(way):
        return remote(spectra.at[0], ring.at[way], own_send.at[0, way], own_recv.at[0, way], side[way])

    def ring_forward(way):
        return remote(ring.at[way, pl.ds(way * 8, 8)], ring.at[2, pl.ds(way * 8, 8)],
                      fwd_send.at[0, way], fwd_recv.at[0, way], side[way])

    def dup_first(slot):
        ref = piece(0, (left, right, far, x)[slot], 0, ORD)
        return remote(ref, ref, dup_send.at[0, slot], dup_recv.at[0, slot], peer)

    def out_last(n, k):
        ty, tz = (y + k // 4) % 4, (z + k % 4) % 4
        return remote(blocks.at[3 + n, ty * 4 + tz], last.at[n, me], out_send.at[3 + n, k],
                      out_recv.at[3 + n, k], {"blk_0": ty, "blk_1": tz})

    def last_far_copy(way):
        return remote(last.at[0, pl.ds(way * 8, 8)], last_far.at[way], far_send.at[LAST, way],
                      far_recv.at[LAST, way], side[way])

    def last_line_copy(way):
        return remote(last.at[1 + way], last_fin.at[way], line_send.at[LAST, way],
                      line_recv.at[LAST, way], side[way])

    def out_copy(g, k):
        ty, tz = (y + k // 4) % 4, (z + k % 4) % 4
        return remote(blocks.at[SLOT[g], ty * 4 + tz], out.at[g, me], out_send.at[SLOT[g], k],
                      out_recv.at[SLOT[g], k], {"blk_0": ty, "blk_1": tz})

    def hours(plane, who):
        return pl.ds(pl.multiple_of((plane * 2 + who) * 16, 16), 16)

    def piece(g, plane, first, count):
        return full.at[pl.ds(g * ORD + first, count), :, hours(plane, core), :]

    def own_copy(g, way):
        ref = piece(g, x, 0, ORD)
        return remote(ref, ref, own_send.at[g, way], own_recv.at[g, way], side[way])

    def fwd_copy(g, way):
        ref = piece(g, left if way == 0 else right, way * half, half)
        return remote(ref, ref, fwd_send.at[g, way], fwd_recv.at[g, way], side[way])

    def dup_copy(g, slot):
        plane, first, count = (
            (x, 0, ORD), (left, 0, ORD), (right, 0, ORD), (far, 0, half), (far, half, half))[slot]
        ref = piece(g, plane, first, count)
        return remote(ref, ref, dup_send.at[g, slot], dup_recv.at[g, slot], peer)

    planes = (far, right, left, x)

    def pair_copy(g, n):
        return remote(full.at[pl.ds(g * ORD, ORD), :, hours(planes[n], 1 - core), :], acc.at[g, n],
                      pair_send.at[g, n], pair_recv.at[g, n], peer)

    def far_copy(g, way):
        return remote(acc.at[g, 0, pl.ds(way * half, half)], far_in.at[SLOT[g], way],
                      far_send.at[g, way], far_recv.at[g, way], side[way])

    def line_copy(g, way):
        return remote(acc.at[g, 1 + way], fin_in.at[SLOT[g], way], line_send.at[g, way],
                      line_recv.at[g, way], side[way])

    def regroup_in(n, g, plane_of):
        blocks_in = []
        for sq in range(4):
            for tq in range(4):
                blocks_in.append(jnp.concatenate(
                    [recv[n, sq * 4 + s, :, tq * 128 : (tq + 1) * 128] for s in range(4)], axis=1))
        moved = jnp.dot(jnp.concatenate(blocks_in, axis=0), perm[...], preferred_element_type=F32)
        for sq in range(4):
            for tq in range(4):
                n0 = (sq * 4 + tq) * 16
                for t in range(4):
                    m = sq * 256 + (tq * 4 + t) * 16
                    mid[m : m + 16, :] = moved[n0 : n0 + 16, t * 128 : (t + 1) * 128]
        for c in range(2):
            for i in range(ORD):
                for sq in range(4):
                    full[g * ORD + i, c, hours(plane_of, core), sq * 128 : (sq + 1) * 128] = (
                        mid[pl.ds(sq * 256 + c * ORD + i, 16, stride=16), :].astype(BF))

    def arrive(g):
        def wait(k, _):
            in_copy(g, k).wait_recv()
            return 0

        lax.fori_loop(1, 16, wait, 0)
        regroup_in(g, g, x)
        own_copy(g, 0).start()
        own_copy(g, 1).start()
        dup_copy(g, 0).start()

    def send_first(slot):
        def send(k, _):
            in_first(slot, k).start()
            return 0

        lax.fori_loop(1, 16, send, 0)
        src = spectra if slot == 3 else ring
        recv[FIRST[slot], pl.ds(me, 1)] = src[0 if slot == 3 else slot, pl.ds(me, 1)]

    def arrive_first(slot):
        def wait(k, _):
            in_first(slot, k).wait_recv()
            return 0

        lax.fori_loop(1, 16, wait, 0)
        regroup_in(FIRST[slot], 0, (left, right, far, x)[slot])
        dup_first(slot).start()

    def forward_first():
        for way in range(2):
            ring_copy(way).wait_recv()
            ring_forward(way).start()
        for way in range(2):
            send_first(way)

    def far_first():
        for way in range(2):
            ring_forward(way).wait_recv()
        send_first(2)

    def forward(g):
        for way in range(2):
            own_copy(g, way).wait_recv()
            fwd_copy(g, way).start()
            dup_copy(g, 1 + way).start()

    def forward_far(g):
        for way in range(2):
            fwd_copy(g, way).wait_recv()
            dup_copy(g, 3 + way).start()

    def middle(g):
        if g == 0:
            for slot in range(4):
                dup_first(slot).wait_recv()
        else:
            for slot in range(5):
                dup_copy(g, slot).wait_recv()

        def analyse(i, _):
            value = lax.dot_general(
                leg[g * ORD + i], full[g * ORD + i].reshape(256, 512), (((1,), (1,)), ((), ())),
                preferred_element_type=F32)
            row = pl.multiple_of(i * 64, 64)
            coef[pl.ds(row, 64), :] = value[:, :128]
            coef[pl.ds(ORD * 64 + row, 64), :] = value[:, 128:]
            return 0

        lax.fori_loop(0, ORD, analyse, 0, unroll=4)

        for slot in range(4 if g == 0 else 5):
            (dup_first(slot) if g == 0 else dup_copy(g, slot)).wait_send()
        if g > 0:
            for way in range(2):
                own_copy(g, way).wait_send()
                fwd_copy(g, way).wait_send()

        def mix(n, _):
            for k in range(16):
                l = n * 16 + k
                rows = jnp.concatenate(
                    [coef[pl.ds(c * ORD * 64 + l, ORD, stride=64), :] for c in range(2)], axis=0)
                mixed[pl.ds(pl.multiple_of(l * 16, 16), 16), :] = jnp.dot(
                    rows.astype(BF), temporal[l], preferred_element_type=F32)
            return 0

        lax.fori_loop(0, 4, mix, 0)

        def synthesise(i, _):
            rows = jnp.concatenate(
                [mixed[pl.ds(c * ORD + i, 64, stride=16), :] for c in range(2)], axis=1)
            value = lax.dot_general(
                rows.astype(BF), leg[g * ORD + i], (((0,), (0,)), ((), ())),
                preferred_element_type=F32)
            full[g * ORD + i] = value.astype(BF).reshape(2, 128, 512)
            return 0

        lax.fori_loop(0, ORD, synthesise, 0, unroll=4)
        for n in range(4):
            pair_copy(g, n).start()

    def add_pair(g):
        for n in range(4):
            pair_copy(g, n).wait_recv()

            def step(i, _):
                own = full[g * ORD + i, :, hours(planes[n], core), :]
                acc[g, n, i] = (acc[g, n, i].astype(F32) + own.astype(F32)).astype(BF)
                return 0

            lax.fori_loop(0, ORD, step, 0)
            if g == LAST:
                regroup_out(3 + n, lambda i, c: acc[g, n, i, c].astype(F32))

                def send(k, _):
                    out_last(n, k).start()
                    return 0

                lax.fori_loop(1, 16, send, 0)
                last[n, pl.ds(me, 1)] = blocks[3 + n, pl.ds(me, 1)]
            elif n == 0:
                far_copy(g, 0).start()
                far_copy(g, 1).start()

    def add_far(g):
        for way in range(2):
            far_copy(g, way).wait_recv()

            def step(i, _):
                acc[g, 1 + way, way * half + i] = (
                    acc[g, 1 + way, way * half + i].astype(F32) + far_in[SLOT[g], way, i].astype(F32)
                ).astype(BF)
                return 0

            lax.fori_loop(0, half, step, 0)
            line_copy(g, way).start()

    def regroup_out(n, value):
        for i in range(ORD):
            for c in range(2):
                total = value(i, c)
                for sq in range(4):
                    mid[pl.ds(sq * 256 + c * ORD + i, 16, stride=16), :] = (
                        total[:, sq * 128 : (sq + 1) * 128])
        rows_out = []
        for sq in range(4):
            for tq in range(4):
                m = sq * 256 + tq * 64
                rows_out.append(jnp.concatenate(
                    [mid[m + t * 16 : m + (t + 1) * 16, :].astype(BF) for t in range(4)], axis=1))
        moved = jnp.dot(
            jnp.concatenate(rows_out, axis=0), perm[...], preferred_element_type=F32).astype(BF)
        for sq in range(4):
            for tq in range(4):
                n0 = (sq * 4 + tq) * 16
                for s in range(4):
                    blocks[n, sq * 4 + s, :, tq * 128 : (tq + 1) * 128] = (
                        moved[n0 : n0 + 16, s * 128 : (s + 1) * 128])

    def depart(g):
        line_copy(g, 0).wait_recv()
        line_copy(g, 1).wait_recv()
        regroup_out(SLOT[g], lambda i, c: acc[g, 3, i, c].astype(F32)
                    + fin_in[SLOT[g], 0, i, c].astype(F32) + fin_in[SLOT[g], 1, i, c].astype(F32))

        def send(k, _):
            out_copy(g, k).start()
            return 0

        lax.fori_loop(1, 16, send, 0)
        out[g, pl.ds(me, 1)] = blocks[SLOT[g], pl.ds(me, 1)]

    def last_arrived(n):
        def wait(k, _):
            out_last(n, k).wait_recv()
            return 0

        lax.fori_loop(1, 16, wait, 0)

    def last_add(way):
        last_arrived(1 + way)
        last_far_copy(way).wait_recv()

        def step(j, _):
            last[1 + way, way * 8 + j] = (
                last[1 + way, way * 8 + j].astype(F32) + last_far[way, j].astype(F32)).astype(BF)
            return 0

        lax.fori_loop(0, 8, step, 0)
        last_line_copy(way).start()

    def sum_copy(k):
        return remote(stage.at[0], line.at[x * 2 + core], sum_send.at[k], sum_recv.at[k], in_line(k))

    def all_copy(k):
        return remote(stage.at[1], plane.at[me], all_send.at[k], all_recv.at[k],
                      {"blk_0": (y + k // 4) % 4, "blk_1": (z + k % 4) % 4})

    def order_rows(block, odd):
        sub = lax.broadcasted_iota(jnp.int32, (ORD, 128), 0)
        value = jnp.zeros((ORD, 128), jnp.int32)
        for i in range(ORD):
            value = jnp.where(sub == i, orders[block * 32 + odd * ORD + i], value)
        low = jnp.minimum(value, 511 - value)
        return low + jnp.where(value == low, 0, 1024)

    loads[6].wait()
    lane = lax.broadcasted_iota(jnp.int32, (4 * ORD, 128), 1)
    scale = 1.0 / math.sqrt(512.0)

    def fill_group(g):
        def fill(n, _):
            m = jnp.concatenate([order_rows(n * 4 + k, g % 2) for k in range(4)], axis=0) % 1024
            m = m if g < 2 else 511 - m
            cos, sin = unit_circle((m * lane) % 1024)
            turn_c, turn_s = unit_circle((m * 128) % 1024)
            cos, sin = cos * scale, sin * scale
            for q in range(8):
                both = jnp.concatenate(
                    [v[k * ORD : (k + 1) * ORD] for k in range(4) for v in (cos, sin)], axis=0)
                table[pl.ds(pl.multiple_of(g * 256 + n * 64, 64), 64), q * 128 : (q + 1) * 128] = (
                    both.astype(BF))
                cos, sin = cos * turn_c - sin * turn_s, sin * turn_c + cos * turn_s
            return 0

        lax.fori_loop(0, 4, fill, 0)

    def send_in(g):
        def send(k, _):
            in_copy(g, k).start()
            return 0

        lax.fori_loop(1, 16, send, 0)
        recv[g, pl.ds(me, 1)] = spectra[g, pl.ds(me, 1)]

    fill_group(0)
    fill_group(1)
    loads[0].wait()
    lat, time = 32, 16
    for q in range(8):
        split[q * 512 : (q + 1) * 512, :] = direction[:, q * 128 : (q + 1) * 128]

    def gather(t, _):
        for q in range(8):
            rows[pl.ds(pl.multiple_of(t * lat, lat), lat), q * 128 : (q + 1) * 128] = split[
                pl.ds(q * 512 + t, lat, stride=time), :
            ].astype(BF)
        return 0

    lax.fori_loop(0, time, gather, 0, unroll=2)
    loads[7].start()
    for g in range(GROUPS):
        if g >= 2:
            fill_group(g)
        spectra[g] = lax.dot_general(
            table[g * 256 : (g + 1) * 256, :], rows[...], (((1,), (1,)), ((), ())),
            preferred_element_type=F32).astype(BF).reshape(16, 2 * ORD, 512)
        if g == 0:
            pl.semaphore_wait(barrier, 22)

            ring_copy(0).start()
            ring_copy(1).start()
            continue

        if g < 3:
            send_in(g)
        if g == 1:
            send_first(3)
    perm[...] = lane_swap()
    degree = (x * 2 + core) * 64 + lax.broadcasted_iota(jnp.int32, (64, 512), 0)
    loads[1].wait()
    loads[2].wait()
    loads[7].wait()

    def narrow(l, _):
        part = pl.ds(pl.multiple_of(l * 128, 128), 128)
        temporal[l] = synth[part, :].astype(BF)
        temporal[32 + l] = split[part, :].astype(BF)
        return 0

    lax.fori_loop(0, 32, narrow, 0, unroll=2)
    for odd in range(2):
        entry_rows = order_rows(me, odd)
        for k in range(ORD):
            n = odd * ORD + k
            first, second = legendre[n].astype(F32), legendre[16 + n].astype(F32)
            entry = jnp.broadcast_to(
                jnp.concatenate([entry_rows[k : k + 1, :]] * 4, axis=1), (64, 512))
            swap, low = entry >= 1024, entry % 1024
            leg[n] = jnp.where(degree >= low, jnp.where(swap, second, first), 0.0).astype(BF)
            leg[16 + n] = jnp.where(degree >= 511 - low, jnp.where(swap, first, second), 0.0).astype(BF)
    def project(value, target):
        for q in range(8):
            split[q * 512 : (q + 1) * 512, :] = value(q)
        lax.fori_loop(0, time, gather, 0, unroll=2)

        def one(g, _):
            target[g] = lax.dot_general(
                table[pl.ds(pl.multiple_of(g * 256, 256), 256), :], rows[...],
                (((1,), (1,)), ((), ())), preferred_element_type=F32,
            ).astype(BF).reshape(16, 2 * ORD, 512)
            return 0

        lax.fori_loop(0, GROUPS, one, 0)

    def local_sums():
        def step(n, totals):
            r8 = pl.ds(pl.multiple_of(n * 8, 8), 8)
            nn, dp, rp, pp = totals
            for q in range(8):
                cols = slice(q * 128, (q + 1) * 128)
                d, r = direction[r8, cols], residual[r8, cols]
                e = noise[r8, cols] * d
                nn, dp, rp, pp = nn + r * r, dp + d * e, rp + r * e, pp + e * e
            return nn, dp, rp, pp

        zero = jnp.zeros((8, 128), F32)
        totals = lax.fori_loop(0, 64, step, (zero, zero, zero, zero), unroll=2)
        for k in range(4):
            tot[k] = totals[k]

    def fold(v):
        v = v[:8] + v[8:]
        return (v[:, :128] + v[:, 128:256]) + (v[:, 256:384] + v[:, 384:])

    def spectral_sums(g):
        def step(o, totals):
            dp, rp, pp = totals
            value = out[g, o].astype(F32)
            weighted = value
            if g < 2:
                low = jnp.concatenate([order_rows(o, g) % 1024] * 4, axis=1)
                weighted = jnp.concatenate(
                    [jnp.where(low == 0, 2.0 * value[:ORD], value[:ORD]), value[ORD:]], axis=0)
            dp = dp + fold(spectra[g, o].astype(F32) * value)
            rp = rp + fold(rhat[g, o].astype(F32) * value)
            pp = pp + fold(value * (weighted + 2.0 * nhat[g, o].astype(F32)))
            return dp, rp, pp

        totals = lax.fori_loop(0, 16, step, (tot[1], tot[2], tot[3]))
        for k in range(3):
            tot[1 + k] = totals[k]

    forward_first()
    arrive(1)
    far_first()
    send_in(3)
    arrive(2)
    arrive_first(3)
    arrive_first(0)
    arrive_first(1)
    forward(1)
    arrive_first(2)
    arrive(3)
    forward(2)
    middle(0)
    forward_far(1)
    add_pair(0)
    middle(1)
    forward(3)
    forward_far(2)
    add_pair(1)
    add_far(0)
    middle(2)
    forward_far(3)
    add_far(1)
    add_pair(2)
    middle(3)
    add_pair(3)
    depart(0)
    last_arrived(0)
    last_far_copy(0).start()
    last_far_copy(1).start()
    add_far(3)
    depart(1)
    for n in range(3, 6):
        loads[n].wait()
    project(lambda q: residual[:, q * 128 : (q + 1) * 128], rhat)
    last_add(0)
    last_add(1)
    depart(3)
    project(lambda q: noise[:, q * 128 : (q + 1) * 128] * direction[:, q * 128 : (q + 1) * 128], nhat)
    local_sums()

    def arrived(g):
        def wait(k, _):
            out_copy(g, k).wait_recv()
            return 0

        lax.fori_loop(1, 16, wait, 0)

    def transform(first, count, n):
        cols = pl.ds(pl.multiple_of(n * 128, 128), 128)
        value = out[first : first + count, :, :, cols].reshape(count * 256, 128)
        return lax.dot_general(
            value, table[first * 256 : (first + count) * 256, :], (((0,), (0,)), ((), ())),
            preferred_element_type=F32)

    for g in range(2):
        arrived(g)
        spectral_sums(g)
    last_arrived(3)
    for way in range(2):
        last_line_copy(way).wait_recv()

    def total(j, _):
        out[LAST, j] = (last[3, j].astype(F32) + last_fin[0, j].astype(F32)
                        + last_fin[1, j].astype(F32)).astype(BF)
        return 0

    lax.fori_loop(0, 16, total, 0)
    spectral_sums(LAST)
    arrived(3)
    spectral_sums(3)
    for k in range(4):
        stage[0, 2 * k : 2 * k + 2, :] = jnp.broadcast_to(
            jnp.sum(tot[k], axis=0, keepdims=True), (2, 128))
    for k in range(1, 8):
        sum_copy(k).start()
    line[pl.ds(x * 2 + core, 1)] = stage[0:1]

    def synthesis(n, _):
        block = transform(0, 4, n)
        for t in range(4):
            for q in range(8):
                split[pl.ds(q * 512 + n * 4 + t, 32, stride=16), :] = (
                    block[t * 32 : (t + 1) * 32, q * 128 : (q + 1) * 128])
        return 0

    lax.fori_loop(0, 4, synthesis, 0)
    for k in range(1, 8):
        sum_copy(k).wait_recv()
    stage[1] = jnp.sum(line[...], axis=0)
    for k in range(1, 16):
        all_copy(k).start()
    plane[pl.ds(me, 1)] = stage[1:2]

    def combine(n, _):
        r8 = pl.ds(pl.multiple_of(n * 8, 8), 8)
        for q in range(8):
            cols = slice(q * 128, (q + 1) * 128)
            product[r8, cols] = (
                split[pl.ds(pl.multiple_of(q * 512 + n * 8, 8), 8), :]
                + noise[r8, cols] * direction[r8, cols])
        return 0

    lax.fori_loop(0, 64, combine, 0, unroll=2)
    for k in range(1, 16):
        all_copy(k).wait_recv()
    sums[...] = jnp.sum(plane[...], axis=0)
    for k in range(1, 8):
        sum_copy(k).wait_send()
    for k in range(1, 16):
        all_copy(k).wait_send()
    for g in range(GROUPS):
        for n in range(4):
            pair_copy(g, n).wait_send()
        for way in range(2):
            if g == 0:
                ring_copy(way).wait_send()
                ring_forward(way).wait_send()
            if g == LAST:
                last_far_copy(way).wait_send()
                last_line_copy(way).wait_send()
            else:
                far_copy(g, way).wait_send()
                line_copy(g, way).wait_send()

    def finish(k, _):
        for g in range(1, GROUPS):
            in_copy(g, k).wait_send()
            if g - 1 != LAST:
                out_copy(g - 1, k).wait_send()
        out_copy(3, k).wait_send()
        for n in range(4):
            in_first(n, k).wait_send()
            out_last(n, k).wait_send()
        return 0

    lax.fori_loop(1, 16, finish, 0)


def step_stage(orders, direction, residual, solution, noise, legendre, temporal):
    dma = pltpu.SemaphoreType.DMA
    two, four, five, blk = dma((GROUPS, 2)), dma((GROUPS, 4)), dma((GROUPS, 5)), dma((GROUPS + 3, 16))
    grid = pltpu.VMEM((512, 1024), F32)
    hbm = pl.BlockSpec(memory_space=pl.ANY)
    shape = jax.ShapeDtypeStruct((512, 1024), F32)
    return pl.pallas_call(
        step_kernel,
        out_shape=(shape, jax.ShapeDtypeStruct((8, 128), F32), shape, shape, shape),
        in_specs=[pl.BlockSpec(memory_space=pltpu.HBM)] + [hbm] * 6,
        out_specs=(VM,) * 5,
        scratch_shapes=[
            pltpu.SMEM((512,), jnp.int32),
            grid,
            pltpu.VMEM((32, 64, 512), BF),
            pltpu.VMEM((64, 128, 128), BF),
            dma((8,)),
            pltpu.VMEM((4096, 128), F32),
            pltpu.VMEM((512, 1024), BF),
            pltpu.VMEM((1024, 1024), BF),
            pltpu.VMEM((GROUPS, 16, 2 * ORD, 512), BF),
            pltpu.VMEM((3, 16, 2 * ORD, 512), BF),
            pltpu.VMEM((32, 2, 128, 512), BF),
            pltpu.VMEM((32, 64, 512), BF),
            pltpu.VMEM((GROUPS + 3, 16, 2 * ORD, 512), BF),
            pltpu.VMEM((GROUPS + 3, 16, 2 * ORD, 512), BF),
            pltpu.VMEM((1024, 128), F32),
            pltpu.VMEM((512, 512), BF),
            pltpu.VMEM((2 * ORD * 64, 128), F32),
            pltpu.VMEM((2 * ORD * 64, 128), F32),
            pltpu.VMEM((GROUPS, 4, ORD, 2, 16, 512), BF),
            pltpu.VMEM((3, 2, ORD // 2, 2, 16, 512), BF),
            pltpu.VMEM((3, 2, ORD, 2, 16, 512), BF),
            pltpu.VMEM((2, 8, 2 * ORD, 512), BF),
            pltpu.VMEM((2, 16, 2 * ORD, 512), BF),
            pltpu.VMEM((4, 16, 2 * ORD, 512), BF),
            pltpu.VMEM((GROUPS, 16, 2 * ORD, 512), BF),
            pltpu.VMEM((4096, 128), F32),
            pltpu.VMEM((GROUPS, 16, 2 * ORD, 512), BF),
            pltpu.VMEM((GROUPS, 16, 2 * ORD, 512), BF),
            pltpu.VMEM((4, 8, 128), F32),
            pltpu.VMEM((2, 8, 128), F32),
            pltpu.VMEM((8, 8, 128), F32),
            pltpu.VMEM((16, 8, 128), F32),
            blk, blk, two, two, five, two, two, five, four, four, two, two, two, two, blk, blk,
            dma((8,)), dma((8,)), dma((16,)), dma((16,)),
        ],
        compiler_params=pltpu.CompilerParams(
            collective_id=0, has_side_effects=True, vmem_limit_bytes=45 * 1024 * 1024),
        name="step_stage",
    )(orders, direction, residual, solution, noise, legendre, temporal)


def update_kernel(sums, solution, residual, direction, product, solution_new, residual_new,
                  direction_new, stage, sems):
    def total(k):
        return jnp.sum(sums[2 * k : 2 * k + 1, :], axis=1, keepdims=True)

    norm_now, curvature, cross, square = total(0), total(1), total(2), total(3)
    step = norm_now / curvature
    norm_next = norm_now - 2.0 * step * cross + step * step * square
    ratio = norm_next / norm_now
    outs = (solution_new, residual_new, direction_new)

    def copy(n, k):
        rows = pl.ds(pl.multiple_of(n * 64, 64), 64)
        return pltpu.make_async_copy(stage.at[k, rows, :], outs[k].at[rows, :], sems.at[n, k])

    def block(n, _):
        rows = pl.ds(pl.multiple_of(n * 64, 64), 64)
        d = direction[rows, :]
        r = residual[rows, :] - step * product[rows, :]
        stage[0, rows, :] = solution[rows, :] + step * d
        stage[1, rows, :] = r
        stage[2, rows, :] = r + ratio * d
        for k in range(3):
            copy(n, k).start()
        return 0

    lax.fori_loop(0, 8, block, 0)

    def drain(n, _):
        for k in range(3):
            copy(n, k).wait()
        return 0

    lax.fori_loop(0, 8, drain, 0)


def update(sums, solution, residual, direction, product):
    shape = jax.ShapeDtypeStruct((512, 1024), F32)
    hbm = pl.BlockSpec(memory_space=pl.ANY)
    return pl.pallas_call(
        update_kernel,
        out_shape=(shape, shape, shape),
        in_specs=[VM] * 5,
        out_specs=(hbm, hbm, hbm),
        scratch_shapes=[pltpu.VMEM((3, 512, 1024), F32), pltpu.SemaphoreType.DMA((8, 3))],
        compiler_params=pltpu.CompilerParams(vmem_limit_bytes=24 * 1024 * 1024),
        name="update",
    )(sums, solution, residual, direction, product)


def body(solution, residual, direction, noise_var, legendre, temporal, order_table):
    shape = direction.shape
    flat = lambda v: v.reshape(512, 1024)
    product, sums, direction, residual, solution = step_stage(
        order_table, flat(direction), flat(residual), flat(solution), flat(noise_var), legendre,
        temporal.reshape(8192, 128))
    outs = update(sums, solution, residual, direction, product)
    return tuple(o.reshape(shape) for o in outs)


def solution(mesh):
    torus = Mesh(mesh.devices.reshape(4, 4, 4, 2), ("blk_0", "blk_1", "tm_0", "tm_1"))
    return jax.shard_map(
        body,
        mesh=torus,
        in_specs=(
            P(BLK, TM, None),
            P(BLK, TM, None),
            P(BLK, TM, None),
            P(BLK, TM, None),
            P(BLK, TM, None),
            P(TM, None, None),
            P(),
        ),
        out_specs=(P(BLK, TM, None), P(BLK, TM, None), P(BLK, TM, None)),
        check_vma=False,
    )
```

```python
import math

import jax
import jax.numpy as jnp
from jax import lax
from jax.experimental import pallas as pl
from jax.experimental.pallas import tpu as pltpu
from jax.sharding import Mesh
from jax.sharding import PartitionSpec as P

BLK = ("blk_0", "blk_1")
TM = ("tm_0", "tm_1")
BLK_TM = ("blk_0", "blk_1", "tm_0", "tm_1")
BF = jnp.bfloat16
F32 = jnp.float32
MESH = pl.DeviceIdType.MESH
GROUPS = 4
ORD = 8
LAST = 2
SLOT = (0, 1, None, 2)
FIRST = (4, 5, 6, 0)
VM = pl.BlockSpec(memory_space=pltpu.VMEM)


def unit_circle(phase):
    quadrant = (phase + 128) // 256
    x = (phase - quadrant * 256).astype(F32) * (2.0 * math.pi / 1024)
    x2 = x * x
    s = x * (1.0 + x2 * (-1.0 / 6 + x2 * (1.0 / 120 + x2 * (-1.0 / 5040 + x2 / 362880))))
    c = 1.0 + x2 * (-0.5 + x2 * (1.0 / 24 + x2 * (-1.0 / 720 + x2 / 40320)))
    odd = quadrant % 2 == 1
    cos = jnp.where(odd, s, c)
    sin = jnp.where(odd, c, s)
    cos = jnp.where((quadrant == 1) | (quadrant == 2), -cos, cos)
    sin = jnp.where((quadrant == 2) | (quadrant == 3), -sin, sin)
    return cos, sin


def lane_swap():
    row = lax.broadcasted_iota(jnp.int32, (512, 512), 0)
    col = lax.broadcasted_iota(jnp.int32, (512, 512), 1)
    moved = (row // 32 % 4) * 128 + (row // 128) * 32 + row % 32
    return (col == moved).astype(F32).astype(BF)


def step_kernel(orders_in, direction_in, residual_in, solution_in, noise_in, legendre_in, temporal_in,
                product, sums, direction, residual, solution, orders, noise, legendre, temporal, load,
                split, rows, table, spectra, ring, full, leg, recv, blocks, mid, perm, coef, mixed, acc,
                far_in, fin_in, last_far, last_fin, last, out, synth, rhat, nhat, tot, stage, line, plane, in_send, in_recv, own_send, fwd_send, dup_send,
                own_recv, fwd_recv, dup_recv, pair_send, pair_recv, far_send, far_recv, line_send,
                line_recv, out_send, out_recv, sum_send, sum_recv, all_send, all_recv):
    loads = [
        pltpu.make_async_copy(src, dst, load.at[n])
        for n, (src, dst) in enumerate((
            (direction_in, direction), (legendre_in, legendre), (temporal_in.at[pl.ds(0, 4096)], synth),
            (residual_in, residual), (noise_in, noise), (solution_in, solution),
            (orders_in, orders), (temporal_in.at[pl.ds(4096, 4096)], split)))
    ]
    chunks = [
        pltpu.make_async_copy(
            direction_in.at[:, pl.ds(q * 128, 128)], split.at[pl.ds(q * 512, 512)], load.at[8 + q])
        for q in range(8)
    ]
    loads[6].start()
    for copy in chunks + loads[:6]:
        copy.start()
    y, z = lax.axis_index("blk_0"), lax.axis_index("blk_1")
    x, core = lax.axis_index("tm_0"), lax.axis_index("tm_1")
    me = y * 4 + z
    right, left, far = (x + 1) % 4, (x + 3) % 4, (x + 2) % 4
    half = ORD // 2
    barrier = pltpu.get_barrier_semaphore()

    def greet(k, _):
        pl.semaphore_signal(
            barrier, inc=1, device_id={"blk_0": (y + k // 4) % 4, "blk_1": (z + k % 4) % 4},
            device_id_type=MESH,
        )
        return 0

    lax.fori_loop(1, 16, greet, 0)

    def in_line(k):
        return {"tm_0": (x + k // 2) % 4, "tm_1": (core + k) % 2}

    def greet_line(k, _):
        pl.semaphore_signal(barrier, inc=1, device_id=in_line(k), device_id_type=MESH)
        return 0

    lax.fori_loop(1, 8, greet_line, 0)
    side = ({"tm_0": right}, {"tm_0": left})
    peer = {"tm_1": 1 - core}

    def remote(src, dst, send, recv_sem, device):
        return pltpu.make_async_remote_copy(
            src_ref=src, dst_ref=dst, send_sem=send, recv_sem=recv_sem, device_id=device,
            device_id_type=MESH)

    def in_copy(g, k):
        ty, tz = (y + k // 4) % 4, (z + k % 4) % 4
        return remote(spectra.at[g, ty * 4 + tz], recv.at[g, me], in_send.at[g, k],
                      in_recv.at[g, k], {"blk_0": ty, "blk_1": tz})

    def in_first(slot, k):
        ty, tz = (y + k // 4) % 4, (z + k % 4) % 4
        dest = ty * 4 + tz
        src = spectra.at[0, dest] if slot == 3 else ring.at[slot, dest]
        return remote(src, recv.at[FIRST[slot], me], in_send.at[FIRST[slot], k],
                      in_recv.at[FIRST[slot], k], {"blk_0": ty, "blk_1": tz})

    def ring_copy(way):
        return remote(spectra.at[0], ring.at[way], own_send.at[0, way], own_recv.at[0, way], side[way])

    def ring_forward(way):
        return remote(ring.at[way, pl.ds(way * 8, 8)], ring.at[2, pl.ds(way * 8, 8)],
                      fwd_send.at[0, way], fwd_recv.at[0, way], side[way])

    def dup_first(slot):
        ref = piece(0, (left, right, far, x)[slot], 0, ORD)
        return remote(ref, ref, dup_send.at[0, slot], dup_recv.at[0, slot], peer)

    def out_last(n, k):
        ty, tz = (y + k // 4) % 4, (z + k % 4) % 4
        return remote(blocks.at[3 + n, ty * 4 + tz], last.at[n, me], out_send.at[3 + n, k],
                      out_recv.at[3 + n, k], {"blk_0": ty, "blk_1": tz})

    def last_far_copy(way):
        return remote(last.at[0, pl.ds(way * 8, 8)], last_far.at[way], far_send.at[LAST, way],
                      far_recv.at[LAST, way], side[way])

    def last_line_copy(way):
        return remote(last.at[1 + way], last_fin.at[way], line_send.at[LAST, way],
                      line_recv.at[LAST, way], side[way])

    def out_copy(g, k):
        ty, tz = (y + k // 4) % 4, (z + k % 4) % 4
        return remote(blocks.at[SLOT[g], ty * 4 + tz], out.at[g, me], out_send.at[SLOT[g], k],
                      out_recv.at[SLOT[g], k], {"blk_0": ty, "blk_1": tz})

    def hours(plane, who):
        return pl.ds(pl.multiple_of((plane * 2 + who) * 16, 16), 16)

    def piece(g, plane, first, count):
        return full.at[pl.ds(g * ORD + first, count), :, hours(plane, core), :]

    def own_copy(g, way):
        ref = piece(g, x, 0, ORD)
        return remote(ref, ref, own_send.at[g, way], own_recv.at[g, way], side[way])

    def fwd_copy(g, way):
        ref = piece(g, left if way == 0 else right, way * half, half)
        return remote(ref, ref, fwd_send.at[g, way], fwd_recv.at[g, way], side[way])

    def dup_copy(g, slot):
        plane, first, count = (
            (x, 0, ORD), (left, 0, ORD), (right, 0, ORD), (far, 0, half), (far, half, half))[slot]
        ref = piece(g, plane, first, count)
        return remote(ref, ref, dup_send.at[g, slot], dup_recv.at[g, slot], peer)

    planes = (far, right, left, x)

    def pair_copy(g, n):
        return remote(full.at[pl.ds(g * ORD, ORD), :, hours(planes[n], 1 - core), :], acc.at[g, n],
                      pair_send.at[g, n], pair_recv.at[g, n], peer)

    def far_copy(g, way):
        return remote(acc.at[g, 0, pl.ds(way * half, half)], far_in.at[SLOT[g], way],
                      far_send.at[g, way], far_recv.at[g, way], side[way])

    def line_copy(g, way):
        return remote(acc.at[g, 1 + way], fin_in.at[SLOT[g], way], line_send.at[g, way],
                      line_recv.at[g, way], side[way])

    def regroup_in(n, g, plane_of):
        blocks_in = []
        for sq in range(4):
            for tq in range(4):
                blocks_in.append(jnp.concatenate(
                    [recv[n, sq * 4 + s, :, tq * 128 : (tq + 1) * 128] for s in range(4)], axis=1))
        moved = jnp.dot(jnp.concatenate(blocks_in, axis=0), perm[...], preferred_element_type=F32)
        for sq in range(4):
            for tq in range(4):
                n0 = (sq * 4 + tq) * 16
                for t in range(4):
                    m = sq * 256 + (tq * 4 + t) * 16
                    mid[m : m + 16, :] = moved[n0 : n0 + 16, t * 128 : (t + 1) * 128]
        for c in range(2):
            for i in range(ORD):
                for sq in range(4):
                    full[g * ORD + i, c, hours(plane_of, core), sq * 128 : (sq + 1) * 128] = (
                        mid[pl.ds(sq * 256 + c * ORD + i, 16, stride=16), :].astype(BF))

    def arrive(g):
        def wait(k, _):
            in_copy(g, k).wait_recv()
            return 0

        lax.fori_loop(1, 16, wait, 0)
        regroup_in(g, g, x)
        own_copy(g, 0).start()
        own_copy(g, 1).start()
        dup_copy(g, 0).start()

    def send_first(slot):
        def send(k, _):
            in_first(slot, k).start()
            return 0

        lax.fori_loop(1, 16, send, 0)
        src = spectra if slot == 3 else ring
        recv[FIRST[slot], pl.ds(me, 1)] = src[0 if slot == 3 else slot, pl.ds(me, 1)]

    def arrive_first(slot):
        def wait(k, _):
            in_first(slot, k).wait_recv()
            return 0

        lax.fori_loop(1, 16, wait, 0)
        regroup_in(FIRST[slot], 0, (left, right, far, x)[slot])
        dup_first(slot).start()

    def forward_first():
        for way in range(2):
            ring_copy(way).wait_recv()
            ring_forward(way).start()
        for way in range(2):
            send_first(way)

    def far_first():
        for way in range(2):
            ring_forward(way).wait_recv()
        send_first(2)

    def forward(g):
        for way in range(2):
            own_copy(g, way).wait_recv()
            fwd_copy(g, way).start()
            dup_copy(g, 1 + way).start()

    def forward_far(g):
        for way in range(2):
            fwd_copy(g, way).wait_recv()
            dup_copy(g, 3 + way).start()

    def middle(g):
        if g == 0:
            for slot in range(4):
                dup_first(slot).wait_recv()
        else:
            for slot in range(5):
                dup_copy(g, slot).wait_recv()

        def analyse(i, _):
            value = lax.dot_general(
                leg[g * ORD + i], full[g * ORD + i].reshape(256, 512), (((1,), (1,)), ((), ())),
                preferred_element_type=F32)
            row = pl.multiple_of(i * 64, 64)
            coef[pl.ds(row, 64), :] = value[:, :128]
            coef[pl.ds(ORD * 64 + row, 64), :] = value[:, 128:]
            return 0

        lax.fori_loop(0, ORD, analyse, 0, unroll=4)

        for slot in range(4 if g == 0 else 5):
            (dup_first(slot) if g == 0 else dup_copy(g, slot)).wait_send()
        if g > 0:
            for way in range(2):
                own_copy(g, way).wait_send()
                fwd_copy(g, way).wait_send()

        def mix(n, _):
            for k in range(16):
                l = n * 16 + k
                rows = jnp.concatenate(
                    [coef[pl.ds(c * ORD * 64 + l, ORD, stride=64), :] for c in range(2)], axis=0)
                mixed[pl.ds(pl.multiple_of(l * 16, 16), 16), :] = jnp.dot(
                    rows.astype(BF), temporal[l], preferred_element_type=F32)
            return 0

        lax.fori_loop(0, 4, mix, 0)

        def synthesise(i, _):
            rows = jnp.concatenate(
                [mixed[pl.ds(c * ORD + i, 64, stride=16), :] for c in range(2)], axis=1)
            value = lax.dot_general(
                rows.astype(BF), leg[g * ORD + i], (((0,), (0,)), ((), ())),
                preferred_element_type=F32)
            full[g * ORD + i] = value.astype(BF).reshape(2, 128, 512)
            return 0

        lax.fori_loop(0, ORD, synthesise, 0, unroll=4)
        for n in range(4):
            pair_copy(g, n).start()

    def add_pair(g):
        for n in range(4):
            pair_copy(g, n).wait_recv()

            def step(i, _):
                own = full[g * ORD + i, :, hours(planes[n], core), :]
                acc[g, n, i] = (acc[g, n, i].astype(F32) + own.astype(F32)).astype(BF)
                return 0

            lax.fori_loop(0, ORD, step, 0)
            if g == LAST:
                regroup_out(3 + n, lambda i, c: acc[g, n, i, c].astype(F32))

                def send(k, _):
                    out_last(n, k).start()
                    return 0

                lax.fori_loop(1, 16, send, 0)
                last[n, pl.ds(me, 1)] = blocks[3 + n, pl.ds(me, 1)]
            elif n == 0:
                far_copy(g, 0).start()
                far_copy(g, 1).start()

    def add_far(g):
        for way in range(2):
            far_copy(g, way).wait_recv()

            def step(i, _):
                acc[g, 1 + way, way * half + i] = (
                    acc[g, 1 + way, way * half + i].astype(F32) + far_in[SLOT[g], way, i].astype(F32)
                ).astype(BF)
                return 0

            lax.fori_loop(0, half, step, 0)
            line_copy(g, way).start()

    def regroup_out(n, value):
        for i in range(ORD):
            for c in range(2):
                total = value(i, c)
                for sq in range(4):
                    mid[pl.ds(sq * 256 + c * ORD + i, 16, stride=16), :] = (
                        total[:, sq * 128 : (sq + 1) * 128])
        rows_out = []
        for sq in range(4):
            for tq in range(4):
                m = sq * 256 + tq * 64
                rows_out.append(jnp.concatenate(
                    [mid[m + t * 16 : m + (t + 1) * 16, :].astype(BF) for t in range(4)], axis=1))
        moved = jnp.dot(
            jnp.concatenate(rows_out, axis=0), perm[...], preferred_element_type=F32).astype(BF)
        for sq in range(4):
            for tq in range(4):
                n0 = (sq * 4 + tq) * 16
                for s in range(4):
                    blocks[n, sq * 4 + s, :, tq * 128 : (tq + 1) * 128] = (
                        moved[n0 : n0 + 16, s * 128 : (s + 1) * 128])

    def depart(g):
        line_copy(g, 0).wait_recv()
        line_copy(g, 1).wait_recv()
        regroup_out(SLOT[g], lambda i, c: acc[g, 3, i, c].astype(F32)
                    + fin_in[SLOT[g], 0, i, c].astype(F32) + fin_in[SLOT[g], 1, i, c].astype(F32))

        def send(k, _):
            out_copy(g, k).start()
            return 0

        lax.fori_loop(1, 16, send, 0)
        out[g, pl.ds(me, 1)] = blocks[SLOT[g], pl.ds(me, 1)]

    def last_arrived(n):
        def wait(k, _):
            out_last(n, k).wait_recv()
            return 0

        lax.fori_loop(1, 16, wait, 0)

    def last_add(way):
        last_arrived(1 + way)
        last_far_copy(way).wait_recv()

        def step(j, _):
            last[1 + way, way * 8 + j] = (
                last[1 + way, way * 8 + j].astype(F32) + last_far[way, j].astype(F32)).astype(BF)
            return 0

        lax.fori_loop(0, 8, step, 0)
        last_line_copy(way).start()

    def sum_copy(k):
        return remote(stage.at[0], line.at[x * 2 + core], sum_send.at[k], sum_recv.at[k], in_line(k))

    def all_copy(k):
        return remote(stage.at[1], plane.at[me], all_send.at[k], all_recv.at[k],
                      {"blk_0": (y + k // 4) % 4, "blk_1": (z + k % 4) % 4})

    def order_rows(block, odd):
        sub = lax.broadcasted_iota(jnp.int32, (ORD, 128), 0)
        value = jnp.zeros((ORD, 128), jnp.int32)
        for i in range(ORD):
            value = jnp.where(sub == i, orders[block * 32 + odd * ORD + i], value)
        low = jnp.minimum(value, 511 - value)
        return low + jnp.where(value == low, 0, 1024)

    loads[6].wait()
    lane = lax.broadcasted_iota(jnp.int32, (4 * ORD, 128), 1)
    scale = 1.0 / math.sqrt(512.0)

    def fill_group(g):
        def fill(n, _):
            m = jnp.concatenate([order_rows(n * 4 + k, g % 2) for k in range(4)], axis=0) % 1024
            m = m if g < 2 else 511 - m
            cos, sin = unit_circle((m * lane) % 1024)
            turn_c, turn_s = unit_circle((m * 128) % 1024)
            cos, sin = cos * scale, sin * scale
            for q in range(8):
                both = jnp.concatenate(
                    [v[k * ORD : (k + 1) * ORD] for k in range(4) for v in (cos, sin)], axis=0)
                table[pl.ds(pl.multiple_of(g * 256 + n * 64, 64), 64), q * 128 : (q + 1) * 128] = (
                    both.astype(BF))
                cos, sin = cos * turn_c - sin * turn_s, sin * turn_c + cos * turn_s
            return 0

        lax.fori_loop(0, 4, fill, 0)

    def send_in(g):
        def send(k, _):
            in_copy(g, k).start()
            return 0

        lax.fori_loop(1, 16, send, 0)
        recv[g, pl.ds(me, 1)] = spectra[g, pl.ds(me, 1)]

    fill_group(0)
    fill_group(1)
    lat, time = 32, 16
    for copy in chunks:
        copy.wait()

    def gather(t, _):
        for q in range(8):
            rows[pl.ds(pl.multiple_of(t * lat, lat), lat), q * 128 : (q + 1) * 128] = split[
                pl.ds(q * 512 + t, lat, stride=time), :
            ].astype(BF)
        return 0

    lax.fori_loop(0, time, gather, 0, unroll=2)
    loads[7].start()
    for g in range(GROUPS):
        if g >= 2:
            fill_group(g)
        spectra[g] = lax.dot_general(
            table[g * 256 : (g + 1) * 256, :], rows[...], (((1,), (1,)), ((), ())),
            preferred_element_type=F32).astype(BF).reshape(16, 2 * ORD, 512)
        if g == 0:
            pl.semaphore_wait(barrier, 22)

            ring_copy(0).start()
            ring_copy(1).start()
            continue

        if g < 3:
            send_in(g)
        if g == 1:
            send_first(3)
    perm[...] = lane_swap()
    degree = (x * 2 + core) * 64 + lax.broadcasted_iota(jnp.int32, (64, 512), 0)
    loads[1].wait()
    loads[2].wait()
    loads[7].wait()

    def narrow(l, _):
        part = pl.ds(pl.multiple_of(l * 128, 128), 128)
        temporal[l] = synth[part, :].astype(BF)
        temporal[32 + l] = split[part, :].astype(BF)
        return 0

    lax.fori_loop(0, 32, narrow, 0, unroll=2)
    for odd in range(2):
        entry_rows = order_rows(me, odd)
        for k in range(ORD):
            n = odd * ORD + k
            first, second = legendre[n].astype(F32), legendre[16 + n].astype(F32)
            entry = jnp.broadcast_to(
                jnp.concatenate([entry_rows[k : k + 1, :]] * 4, axis=1), (64, 512))
            swap, low = entry >= 1024, entry % 1024
            leg[n] = jnp.where(degree >= low, jnp.where(swap, second, first), 0.0).astype(BF)
            leg[16 + n] = jnp.where(degree >= 511 - low, jnp.where(swap, first, second), 0.0).astype(BF)
    def project(value, target):
        for q in range(8):
            split[q * 512 : (q + 1) * 512, :] = value(q)
        lax.fori_loop(0, time, gather, 0, unroll=2)

        def one(g, _):
            target[g] = lax.dot_general(
                table[pl.ds(pl.multiple_of(g * 256, 256), 256), :], rows[...],
                (((1,), (1,)), ((), ())), preferred_element_type=F32,
            ).astype(BF).reshape(16, 2 * ORD, 512)
            return 0

        lax.fori_loop(0, GROUPS, one, 0)

    def local_sums():
        def step(n, totals):
            r8 = pl.ds(pl.multiple_of(n * 8, 8), 8)
            nn, dp, rp, pp = totals
            for q in range(8):
                cols = slice(q * 128, (q + 1) * 128)
                d, r = direction[r8, cols], residual[r8, cols]
                e = noise[r8, cols] * d
                nn, dp, rp, pp = nn + r * r, dp + d * e, rp + r * e, pp + e * e
            return nn, dp, rp, pp

        zero = jnp.zeros((8, 128), F32)
        totals = lax.fori_loop(0, 64, step, (zero, zero, zero, zero), unroll=2)
        for k in range(4):
            tot[k] = totals[k]

    def fold(v):
        v = v[:8] + v[8:]
        return (v[:, :128] + v[:, 128:256]) + (v[:, 256:384] + v[:, 384:])

    def spectral_sums(g):
        def step(o, totals):
            dp, rp, pp = totals
            value = out[g, o].astype(F32)
            weighted = value
            if g < 2:
                low = jnp.concatenate([order_rows(o, g) % 1024] * 4, axis=1)
                weighted = jnp.concatenate(
                    [jnp.where(low == 0, 2.0 * value[:ORD], value[:ORD]), value[ORD:]], axis=0)
            dp = dp + fold(spectra[g, o].astype(F32) * value)
            rp = rp + fold(rhat[g, o].astype(F32) * value)
            pp = pp + fold(value * (weighted + 2.0 * nhat[g, o].astype(F32)))
            return dp, rp, pp

        totals = lax.fori_loop(0, 16, step, (tot[1], tot[2], tot[3]))
        for k in range(3):
            tot[1 + k] = totals[k]

    forward_first()
    arrive(1)
    far_first()
    send_in(3)
    arrive(2)
    arrive_first(3)
    for n in (0, 3, 4, 5):
        loads[n].wait()
    project(lambda q: residual[:, q * 128 : (q + 1) * 128], rhat)
    arrive_first(0)
    arrive_first(1)
    forward(1)
    arrive_first(2)
    arrive(3)
    forward(2)
    middle(0)
    forward_far(1)
    add_pair(0)
    middle(1)
    forward(3)
    forward_far(2)
    add_pair(1)
    add_far(0)
    middle(2)
    forward_far(3)
    add_far(1)
    add_pair(2)
    middle(3)
    add_pair(3)
    depart(0)
    last_arrived(0)
    last_far_copy(0).start()
    last_far_copy(1).start()
    add_far(3)
    depart(1)
    project(lambda q: noise[:, q * 128 : (q + 1) * 128] * direction[:, q * 128 : (q + 1) * 128], nhat)
    local_sums()
    last_add(0)
    last_add(1)
    depart(3)

    def arrived(g):
        def wait(k, _):
            out_copy(g, k).wait_recv()
            return 0

        lax.fori_loop(1, 16, wait, 0)

    def transform(first, count, n):
        cols = pl.ds(pl.multiple_of(n * 128, 128), 128)
        value = out[first : first + count, :, :, cols].reshape(count * 256, 128)
        return lax.dot_general(
            value, table[first * 256 : (first + count) * 256, :], (((0,), (0,)), ((), ())),
            preferred_element_type=F32)

    for g in range(2):
        arrived(g)
        spectral_sums(g)
    last_arrived(3)
    for way in range(2):
        last_line_copy(way).wait_recv()

    def total(j, _):
        out[LAST, j] = (last[3, j].astype(F32) + last_fin[0, j].astype(F32)
                        + last_fin[1, j].astype(F32)).astype(BF)
        return 0

    lax.fori_loop(0, 16, total, 0)
    spectral_sums(LAST)
    arrived(3)
    spectral_sums(3)
    for k in range(4):
        stage[0, 2 * k : 2 * k + 2, :] = jnp.broadcast_to(
            jnp.sum(tot[k], axis=0, keepdims=True), (2, 128))
    for k in range(1, 8):
        sum_copy(k).start()
    line[pl.ds(x * 2 + core, 1)] = stage[0:1]

    def synthesis(n, _):
        block = transform(0, 4, n)
        for t in range(4):
            for q in range(8):
                split[pl.ds(q * 512 + n * 4 + t, 32, stride=16), :] = (
                    block[t * 32 : (t + 1) * 32, q * 128 : (q + 1) * 128])
        return 0

    lax.fori_loop(0, 4, synthesis, 0)
    for k in range(1, 8):
        sum_copy(k).wait_recv()
    stage[1] = jnp.sum(line[...], axis=0)
    for k in range(1, 16):
        all_copy(k).start()
    plane[pl.ds(me, 1)] = stage[1:2]

    def combine(n, _):
        r8 = pl.ds(pl.multiple_of(n * 8, 8), 8)
        for q in range(8):
            cols = slice(q * 128, (q + 1) * 128)
            product[r8, cols] = (
                split[pl.ds(pl.multiple_of(q * 512 + n * 8, 8), 8), :]
                + noise[r8, cols] * direction[r8, cols])
        return 0

    lax.fori_loop(0, 64, combine, 0, unroll=2)
    for k in range(1, 16):
        all_copy(k).wait_recv()
    sums[...] = jnp.sum(plane[...], axis=0)
    for k in range(1, 8):
        sum_copy(k).wait_send()
    for k in range(1, 16):
        all_copy(k).wait_send()
    for g in range(GROUPS):
        for n in range(4):
            pair_copy(g, n).wait_send()
        for way in range(2):
            if g == 0:
                ring_copy(way).wait_send()
                ring_forward(way).wait_send()
            if g == LAST:
                last_far_copy(way).wait_send()
                last_line_copy(way).wait_send()
            else:
                far_copy(g, way).wait_send()
                line_copy(g, way).wait_send()

    def finish(k, _):
        for g in range(1, GROUPS):
            in_copy(g, k).wait_send()
            if g - 1 != LAST:
                out_copy(g - 1, k).wait_send()
        out_copy(3, k).wait_send()
        for n in range(4):
            in_first(n, k).wait_send()
            out_last(n, k).wait_send()
        return 0

    lax.fori_loop(1, 16, finish, 0)


def step_stage(orders, direction, residual, solution, noise, legendre, temporal):
    dma = pltpu.SemaphoreType.DMA
    two, four, five, blk = dma((GROUPS, 2)), dma((GROUPS, 4)), dma((GROUPS, 5)), dma((GROUPS + 3, 16))
    grid = pltpu.VMEM((512, 1024), F32)
    hbm = pl.BlockSpec(memory_space=pl.ANY)
    shape = jax.ShapeDtypeStruct((512, 1024), F32)
    return pl.pallas_call(
        step_kernel,
        out_shape=(shape, jax.ShapeDtypeStruct((8, 128), F32), shape, shape, shape),
        in_specs=[pl.BlockSpec(memory_space=pltpu.HBM)] + [hbm] * 6,
        out_specs=(VM,) * 5,
        scratch_shapes=[
            pltpu.SMEM((512,), jnp.int32),
            grid,
            pltpu.VMEM((32, 64, 512), BF),
            pltpu.VMEM((64, 128, 128), BF),
            dma((16,)),
            pltpu.VMEM((4096, 128), F32),
            pltpu.VMEM((512, 1024), BF),
            pltpu.VMEM((1024, 1024), BF),
            pltpu.VMEM((GROUPS, 16, 2 * ORD, 512), BF),
            pltpu.VMEM((3, 16, 2 * ORD, 512), BF),
            pltpu.VMEM((32, 2, 128, 512), BF),
            pltpu.VMEM((32, 64, 512), BF),
            pltpu.VMEM((GROUPS + 3, 16, 2 * ORD, 512), BF),
            pltpu.VMEM((GROUPS + 3, 16, 2 * ORD, 512), BF),
            pltpu.VMEM((1024, 128), F32),
            pltpu.VMEM((512, 512), BF),
            pltpu.VMEM((2 * ORD * 64, 128), F32),
            pltpu.VMEM((2 * ORD * 64, 128), F32),
            pltpu.VMEM((GROUPS, 4, ORD, 2, 16, 512), BF),
            pltpu.VMEM((3, 2, ORD // 2, 2, 16, 512), BF),
            pltpu.VMEM((3, 2, ORD, 2, 16, 512), BF),
            pltpu.VMEM((2, 8, 2 * ORD, 512), BF),
            pltpu.VMEM((2, 16, 2 * ORD, 512), BF),
            pltpu.VMEM((4, 16, 2 * ORD, 512), BF),
            pltpu.VMEM((GROUPS, 16, 2 * ORD, 512), BF),
            pltpu.VMEM((4096, 128), F32),
            pltpu.VMEM((GROUPS, 16, 2 * ORD, 512), BF),
            pltpu.VMEM((GROUPS, 16, 2 * ORD, 512), BF),
            pltpu.VMEM((4, 8, 128), F32),
            pltpu.VMEM((2, 8, 128), F32),
            pltpu.VMEM((8, 8, 128), F32),
            pltpu.VMEM((16, 8, 128), F32),
            blk, blk, two, two, five, two, two, five, four, four, two, two, two, two, blk, blk,
            dma((8,)), dma((8,)), dma((16,)), dma((16,)),
        ],
        compiler_params=pltpu.CompilerParams(
            collective_id=0, has_side_effects=True, vmem_limit_bytes=45 * 1024 * 1024),
        name="step_stage",
    )(orders, direction, residual, solution, noise, legendre, temporal)


def update_kernel(sums, solution, residual, direction, product, solution_new, residual_new,
                  direction_new, stage, sems):
    def total(k):
        return jnp.sum(sums[2 * k : 2 * k + 1, :], axis=1, keepdims=True)

    norm_now, curvature, cross, square = total(0), total(1), total(2), total(3)
    step = norm_now / curvature
    norm_next = norm_now - 2.0 * step * cross + step * step * square
    ratio = norm_next / norm_now
    outs = (solution_new, residual_new, direction_new)

    def copy(n, k):
        rows = pl.ds(pl.multiple_of(n * 64, 64), 64)
        return pltpu.make_async_copy(stage.at[k, rows, :], outs[k].at[rows, :], sems.at[n, k])

    def block(n, _):
        rows = pl.ds(pl.multiple_of(n * 64, 64), 64)
        d = direction[rows, :]
        r = residual[rows, :] - step * product[rows, :]
        stage[0, rows, :] = solution[rows, :] + step * d
        stage[1, rows, :] = r
        stage[2, rows, :] = r + ratio * d
        for k in range(3):
            copy(n, k).start()
        return 0

    lax.fori_loop(0, 8, block, 0)

    def drain(n, _):
        for k in range(3):
            copy(n, k).wait()
        return 0

    lax.fori_loop(0, 8, drain, 0)


def update(sums, solution, residual, direction, product):
    shape = jax.ShapeDtypeStruct((512, 1024), F32)
    hbm = pl.BlockSpec(memory_space=pl.ANY)
    return pl.pallas_call(
        update_kernel,
        out_shape=(shape, shape, shape),
        in_specs=[VM] * 5,
        out_specs=(hbm, hbm, hbm),
        scratch_shapes=[pltpu.VMEM((3, 512, 1024), F32), pltpu.SemaphoreType.DMA((8, 3))],
        compiler_params=pltpu.CompilerParams(vmem_limit_bytes=24 * 1024 * 1024),
        name="update",
    )(sums, solution, residual, direction, product)


def body(solution, residual, direction, noise_var, legendre, temporal, order_table):
    shape = direction.shape
    flat = lambda v: v.reshape(512, 1024)
    product, sums, direction, residual, solution = step_stage(
        order_table, flat(direction), flat(residual), flat(solution), flat(noise_var), legendre,
        temporal.reshape(8192, 128))
    outs = update(sums, solution, residual, direction, product)
    return tuple(o.reshape(shape) for o in outs)


def solution(mesh):
    torus = Mesh(mesh.devices.reshape(4, 4, 4, 2), ("blk_0", "blk_1", "tm_0", "tm_1"))
    return jax.shard_map(
        body,
        mesh=torus,
        in_specs=(
            P(BLK, TM, None),
            P(BLK, TM, None),
            P(BLK, TM, None),
            P(BLK, TM, None),
            P(BLK, TM, None),
            P(TM, None, None),
            P(),
        ),
        out_specs=(P(BLK, TM, None), P(BLK, TM, None), P(BLK, TM, None)),
        check_vma=False,
    )
```
